32 devices in a mesh: parts: 2 (over y), seq: 4 (over z), head: 2 (over x), rep: 2 (over core).
Axes of the slice: x: 2, y: 2, z: 4, core: 2. Of those that a mesh axis runs over, the one named last changes fastest.
Arguments:
- queries: bfloat16 [4, 1024, 2048], P(('parts', 'rep'), 'seq', 'head'), parts along dimension 0, may hold values from -6 to 6
- reflect_keys: bfloat16 [4, 1024, 2, 2048], P(('parts', 'rep'), 'seq', None, 'head'), parts along dimension 0, may hold values from -6 to 6
- reflect_values: bfloat16 [4, 1024, 2, 2048], P(('parts', 'rep'), 'seq', None, 'head'), parts along dimension 0, may hold values from -6 to 6
- reflect_beta: float32 [4, 1024, 2, 16], P(('parts', 'rep'), 'seq', None, 'head'), parts along dimension 0, may hold values from 0.2 to 2
- log_decay: float32 [4, 1024, 16], P(('parts', 'rep'), 'seq', 'head'), parts along dimension 0, may hold values from -2.5 to 0
- prompt_lengths: int32 [4, 6], P(('parts', 'rep')), parts along dimension 0, may hold values from 1 to 512, 1024 in all within a row
- norm_gain: float32 [128], replicated, may hold values from 0.1 to 1.9
- out_weight: bfloat16 [2048, 2048], P('head'), may hold values from -0.125 to 0.125
Outputs:
- layer_out: bfloat16 [4, 1024, 2048], P(('parts', 'rep'), ('seq', 'head')), parts along dimension 0
The draws below stay inside these ranges and needn't reach their ends.
There are 2 independent parts, one for each index of `parts`. The reference program is written for one: setup_inputs(seed, part) draws one part's arguments, and reference() takes and returns one part's arrays. A program takes and returns all parts, laid end to end along the dimension named above; an argument that names none is the same for every part. Nothing has to cross between parts.
Inputs may be any that keep to these rules, and one draw needn't show every extreme that they name: `prompt_lengths`: the 6 prompts of a pack lie end to end from its first token and cover all 1024 tokens; the longest has exactly 512.
All inputs are finite; a program needn't handle non-finite values.
Results may differ from the reference program's by a relative error of at most 0.0095.
Values may be sent and summed in bfloat16 or wider, within the bound.
A program may use at most 64 MiB of HBM per device.

```python
import math
import jax
import jax.numpy as jnp
import numpy as np
from jax import lax

D = 2048
HEADS = 16
DK = 128
REFL = 2
BLOCK = 64
DOCS = 6
TOK_DEV = 256
BUNDLE_COUNT = 2
BUNDLE_SPAN = 1024
MOST_LEN = 512
N_HEAD = 2


def slow_heads(key):
    chances = jax.random.uniform(jax.random.fold_in(key, 11), (HEADS,))
    return chances < 0.5


def draw_log_decay(key, part):
    slow_mask = slow_heads(key)
    slow_rate = jnp.exp(jax.random.uniform(jax.random.fold_in(key, 21), (HEADS,), minval=jnp.log(0.1 / MOST_LEN), maxval=jnp.log(1.0 / MOST_LEN)))
    fast_rate = jnp.exp(jax.random.uniform(jax.random.fold_in(key, 22), (HEADS,), minval=jnp.log(1.0 / 50.0), maxval=jnp.log(1.0 / 20.0)))
    channel_speed = jnp.where(slow_mask, slow_rate, fast_rate)
    uneven_quantity = jax.random.uniform(jax.random.fold_in(key, 23), (BUNDLE_COUNT, BUNDLE_SPAN, HEADS), minval=0.4, maxval=1.6)
    symbol_span = jnp.exp(jax.random.uniform(jax.random.fold_in(key, 24), (BUNDLE_COUNT, BUNDLE_SPAN // TOK_DEV, HEADS), minval=jnp.log(0.5), maxval=jnp.log(2.0)))
    symbol_span = jnp.repeat(symbol_span, TOK_DEV, axis=1)
    spike_position = jax.random.randint(jax.random.fold_in(key, 25), (BUNDLE_COUNT, 3), 0, BUNDLE_SPAN)
    spike_kept = jax.random.uniform(jax.random.fold_in(key, 26), (BUNDLE_COUNT, 3), minval=0.5, maxval=0.8)
    spike_hits = jnp.arange(BUNDLE_SPAN)[None, None, :] == spike_position[:, :, None]
    spike_log_scale = jnp.sum(jnp.where(spike_hits, jnp.log(spike_kept)[:, :, None], 0.0), axis=1)
    return (spike_log_scale[:, :, None] - channel_speed * uneven_quantity * symbol_span).astype(jnp.float32)


def draw_reflect_beta(key, part):
    slow_mask = slow_heads(key)
    margin = jnp.exp(jax.random.uniform(jax.random.fold_in(key, 31), (BUNDLE_COUNT, BUNDLE_SPAN, REFL, HEADS), minval=jnp.log(0.0001), maxval=jnp.log(0.02)))
    spread = jax.random.uniform(jax.random.fold_in(key, 32), (BUNDLE_COUNT, BUNDLE_SPAN, REFL, HEADS), minval=0.2, maxval=1.9)
    return jnp.where(slow_mask, 2.0 - margin, spread).astype(jnp.float32)


def shard_levels(rng, shape, pieces, least, top_value):
    gain, own = 1.0, jax.random.fold_in(rng, 6)
    for position, blocks in pieces:
        draws = jnp.exp(jax.random.uniform(jax.random.fold_in(own, position), (blocks,), jnp.float32, least / len(pieces), top_value / len(pieces)))
        gain = gain * jnp.repeat(draws, shape[position] // blocks).reshape([-1 if axis == position else 1 for axis in range(len(shape))])
    return gain


def profile(amount, total, reach, skew):
    loads = [(1 << 20) // math.isqrt(standing ** skew) + 1 for standing in range(2, amount + 1)]
    rest, holding = total - reach - (amount - 1), [1] * (amount - 1)
    while rest > 0:
        candidates = [i for i in range(amount - 1) if holding[i] < reach]
        pool, budget = sum([loads[i] for i in candidates]), rest
        for i in candidates:
            extra = min(reach - holding[i], max(1, budget * loads[i] // pool), rest)
            holding[i] = holding[i] + extra
            rest = rest - extra
    return np.array([reach] + holding)


def ragged(rng, count, total, limit, lean):
    if count == 2:
        one = jax.random.randint(rng, (), max(1, total - limit), min(limit, total - 1) + 1)
        return jnp.stack([one, total - one])
    tallies = jnp.asarray(profile(count, total, limit, lean), jnp.int32)
    twos = (count - 1) // 2
    donor, taker = tallies[1:1 + 2 * twos:2], tallies[2:2 + 2 * twos:2]
    room = jnp.minimum(donor - 1, limit - taker)
    moved = jax.random.randint(jax.random.fold_in(rng, 1), (twos,), 0, 1 << 20) % (room + 1)
    tallies = tallies.at[1:1 + 2 * twos:2].set(donor - moved).at[2:2 + 2 * twos:2].set(taker + moved)
    return tallies[jax.random.permutation(jax.random.fold_in(rng, 2), count)]


def scatter_about(key, extent, width, most, cuts=(), held_as=jnp.bfloat16):
    factor_of = shard_levels(key, extent, cuts, -0.22, 0.18) if cuts else 1.0
    entries = jax.random.normal(key, extent, jnp.float32) * width * factor_of
    return jnp.minimum(jnp.maximum(entries, -most), most).astype(held_as)


def setup_inputs(seed: int = 0, part: int = 0) -> dict:
    streams_of = jax.random.split(jax.random.key(seed), 9)
    own_keys = jax.random.split(jax.random.fold_in(streams_of[8], part), 9)
    queries = scatter_about(own_keys[0], (BUNDLE_COUNT, BUNDLE_SPAN, HEADS * DK), 1.0, 6.0, ((0, 2), (1, 4), (2, 2)))
    reflect_keys = scatter_about(own_keys[1], (BUNDLE_COUNT, BUNDLE_SPAN, REFL, HEADS * DK), 1.0, 6.0, ((0, 2), (1, 4), (3, 2)))
    reflect_values = scatter_about(own_keys[2], (BUNDLE_COUNT, BUNDLE_SPAN, REFL, HEADS * DK), 1.0, 6.0, ((0, 2), (1, 4), (3, 2)))
    reflect_beta = draw_reflect_beta(jax.random.fold_in(jax.random.fold_in(streams_of[8], part), 71), part)
    log_decay = draw_log_decay(jax.random.fold_in(jax.random.fold_in(streams_of[8], part), 71), part)
    prompt_lengths = jax.vmap(lambda own: ragged(own, DOCS, BUNDLE_SPAN, MOST_LEN, 2))(jax.random.split(own_keys[5], BUNDLE_COUNT)).reshape((BUNDLE_COUNT, DOCS)).astype(jnp.int32)
    norm_gain = jnp.clip(1.0 + 0.18 * jax.random.normal(streams_of[6], (DK,), jnp.float32), 0.1, 1.9)
    out_weight = scatter_about(streams_of[7], (HEADS * DK, D), (HEADS * DK) ** -0.5, 0.125, ((0, 2),))
    return dict(queries=queries, reflect_keys=reflect_keys, reflect_values=reflect_values, reflect_beta=reflect_beta, log_decay=log_decay, prompt_lengths=prompt_lengths, norm_gain=norm_gain, out_weight=out_weight)


highest = lax.Precision.HIGHEST
epsilon = 1e-06

def unit_rows(vectors):
    return vectors * lax.rsqrt(lax.optimization_barrier(jnp.sum(vectors * vectors, axis=-1, keepdims=True)) + epsilon)

def block_parts(key_rows, value_rows, beta_rows, decay_rows, seg_rows, seg_before):
    steps_here = key_rows.shape[-2]
    cum_decay = jnp.cumsum(decay_rows, axis=-1)
    ordinal = jnp.arange(steps_here)
    incl_mask = ordinal[:, None] >= ordinal[None, :]
    strict_mask = ordinal[:, None] > ordinal[None, :]
    same_doc = seg_rows[:, None, :, None] == seg_rows[:, None, None, :]
    decay_gap = cum_decay[..., :, None] - cum_decay[..., None, :]
    decay_ratio = jnp.where(incl_mask & same_doc, jnp.exp(jnp.minimum(decay_gap, 0.0)), 0.0)
    carry_in = jnp.where(seg_rows[:, None, :] == seg_before[:, None, None], jnp.exp(cum_decay), 0.0)
    key_inner = jnp.einsum('bhik,bhjk->bhij', key_rows, key_rows, precision=highest)
    system = jnp.eye(steps_here, dtype=key_rows.dtype) + jnp.where(strict_mask, beta_rows[..., :, None] * decay_ratio * key_inner, 0.0)
    right_side = jnp.concatenate([beta_rows[..., None] * value_rows, (beta_rows * carry_in)[..., None] * key_rows], axis=-1)
    solved = lax.linalg.triangular_solve(system, right_side, left_side=True, lower=True, unit_diagonal=True)
    val_width = value_rows.shape[-1]
    return (decay_ratio, carry_in, solved[..., :val_width], solved[..., val_width:])

def reference(queries, reflect_keys, reflect_values, reflect_beta, log_decay, prompt_lengths, norm_gain, out_weight):
    pack_count = queries.shape[0]
    length = queries.shape[1]
    blocks = length // BLOCK
    sub_steps = REFL * BLOCK
    doc_ends = jnp.cumsum(prompt_lengths, axis=-1).astype(jnp.int32)
    positions = jnp.arange(length, dtype=jnp.int32)
    segment = lax.optimization_barrier(jnp.sum((positions[None, :, None] >= doc_ends[:, None, :]).astype(jnp.int32), axis=-1)).astype(jnp.int32)
    query_rows = unit_rows(queries.astype(jnp.float32).reshape(pack_count, blocks, BLOCK, HEADS, DK)) * DK ** (-0.5)
    query_rows = query_rows.transpose(1, 0, 3, 2, 4)
    key_rows = unit_rows(reflect_keys.astype(jnp.float32).reshape(pack_count, blocks, BLOCK, REFL, HEADS, DK))
    key_rows = key_rows.transpose(1, 0, 4, 2, 3, 5).reshape(blocks, pack_count, HEADS, sub_steps, DK)
    value_rows = reflect_values.astype(jnp.float32).reshape(pack_count, blocks, BLOCK, REFL, HEADS, DK)
    value_rows = value_rows.transpose(1, 0, 4, 2, 3, 5).reshape(blocks, pack_count, HEADS, sub_steps, DK)
    beta_rows = reflect_beta.reshape(pack_count, blocks, BLOCK, REFL, HEADS).transpose(1, 0, 4, 2, 3).reshape(blocks, pack_count, HEADS, sub_steps)
    gate_rows = log_decay.reshape(pack_count, blocks, BLOCK, HEADS).transpose(1, 0, 3, 2)
    decay_rows = jnp.concatenate([gate_rows[..., None], jnp.zeros(gate_rows.shape + (REFL - 1,), jnp.float32)], axis=-1).reshape(blocks, pack_count, HEADS, sub_steps)
    seg_rows = jnp.repeat(segment.reshape(pack_count, blocks, BLOCK), REFL, axis=-1).transpose(1, 0, 2).astype(jnp.int32)
    last_row = REFL - 1

    def one_block(carried, inputs):
        state, seg_before = carried
        query_block, key_block, value_block, beta_block, decay_block, seg_block = inputs
        decay_ratio, carry_in, write_vals, write_keys = block_parts(key_block, value_block, beta_block, decay_block, seg_block, seg_before)
        updates = write_vals - jnp.einsum('bhck,bhkv->bhcv', write_keys, state, precision=highest)
        read_weights = decay_ratio[..., last_row::REFL, :] * jnp.einsum('bhik,bhjk->bhij', query_block, key_block, precision=highest)
        carry_read = carry_in[..., last_row::REFL]
        head_out = carry_read[..., None] * jnp.einsum('bhik,bhkv->bhiv', query_block, state, precision=highest) + jnp.einsum('bhij,bhjv->bhiv', read_weights, updates, precision=highest)
        end_keys = decay_ratio[..., -1, :, None] * key_block
        new_state = carry_in[..., -1, None, None] * state + jnp.einsum('bhjk,bhjl->bhkl', end_keys, updates, precision=highest)
        return ((new_state, seg_block[:, -1].astype(jnp.int32)), head_out)
    initial = (jnp.zeros((pack_count, HEADS, DK, DK), jnp.float32), jnp.full((pack_count,), -1, jnp.int32))
    finished, outputs = lax.scan(one_block, initial, (query_rows, key_rows, value_rows, beta_rows, decay_rows, seg_rows))
    outputs = outputs.transpose(1, 0, 3, 2, 4)
    normed = (outputs * lax.rsqrt(lax.optimization_barrier(jnp.mean(outputs * outputs, axis=-1, keepdims=True)) + epsilon) * norm_gain).astype(jnp.bfloat16)
    flat_rows = normed.reshape(pack_count, length, HEADS * DK)
    group_width = HEADS * DK // N_HEAD
    total_sum = jnp.zeros((pack_count, length, out_weight.shape[1]), jnp.float32)
    for group_index in range(N_HEAD):
        lower_col = group_index * group_width
        upper_col = lower_col + group_width
        partial_sum = jnp.dot(flat_rows[..., lower_col:upper_col].astype(jnp.float32), out_weight[lower_col:upper_col].astype(jnp.float32), preferred_element_type=jnp.float32).astype(jnp.bfloat16)
        partial_sum = lax.optimization_barrier(partial_sum)
        total_sum = total_sum + partial_sum.astype(jnp.float32)
    return total_sum.astype(jnp.bfloat16)
```

```python
import functools

import jax
import jax.numpy as jnp
from jax import lax
from jax.experimental import pallas as pl
from jax.experimental.pallas import tpu as pltpu
from jax.sharding import PartitionSpec as P

BLOCK = 64
HEADS_STEP = 4
FINISH_GROUP = 2
PIECES = 4
MESH = pl.DeviceIdType.MESH

epsilon = 1e-06
f32 = jnp.float32
bf16 = jnp.bfloat16
highest = lax.Precision.HIGHEST


def mm(a, b, precision=None):
    return jnp.dot(a, b, preferred_element_type=f32, precision=precision)


def mm_nt(a, b):
    return lax.dot_general(a, b, (((1,), (1,)), ((), ())), preferred_element_type=f32)


def mm_tn(a, b):
    return lax.dot_general(a, b, (((0,), (0,)), ((), ())), preferred_element_type=f32)


def split(x):
    hi = x.astype(bf16)
    return hi, (x - hi.astype(f32)).astype(bf16)


def split3(x):
    hi = x.astype(bf16).astype(f32)
    mid = (x - hi).astype(bf16).astype(f32)
    return [hi, mid, x - hi - mid]


def sub_rows(x, pattern, blocks):
    rows = x.shape[0]
    zero = jnp.zeros_like(pattern)
    table = jnp.concatenate(
        [jnp.concatenate([pattern if c == r else zero for c in range(blocks)], axis=1) for r in range(blocks)],
        axis=0,
    )
    got = mm(jnp.concatenate(split3(x), axis=0).astype(bf16), table)
    return got[:rows] + got[rows : 2 * rows] + got[2 * rows :]


def mixer_kernel(
    refl, blocks, len_ref, q_hbm, k_hbm, v_hbm, beta_hbm, gate_hbm, gain_ref, weight_hbm, out_ref,
    q_ref, k_ref, v_ref, beta_ref, gate_ref, in_sem,
    rows_ref, scale_ref, kflat_ref, wrote_ref, prefix_ref, oloc_ref, read_ref, add_ref, map_ref,
    weight_ref, weight_sem, state_in, state_out, normed_ref, own_ref, part_out, part_in,
    state_send, state_recv, part_send, part_recv,
):
    heads, width = add_ref.shape[:2]
    steps = heads // HEADS_STEP
    wide = HEADS_STEP * width
    sub = refl * BLOCK
    tokens = blocks * BLOCK
    seq_count, head_count = lax.axis_size("seq"), lax.axis_size("head")
    seq_here, head_here = lax.axis_index("seq"), lax.axis_index("head")
    chunk = out_ref.shape[0]
    first, last = seq_here == 0, seq_here == seq_count - 1
    others = [lax.rem(head_here + d, head_count) for d in range(1, head_count)]

    def load(s, kind):
        span = pl.ds(pl.multiple_of(s * wide, wide), wide)
        src, dst = [
            (k_hbm.at[:, :, span], k_ref), (v_hbm.at[:, :, span], v_ref), (q_hbm.at[:, span], q_ref)
        ][kind]
        return pltpu.make_async_copy(src, dst.at[s], in_sem.at[s, kind])

    load_beta = pltpu.make_async_copy(beta_hbm, beta_ref, weight_sem.at[1])
    load_gate = pltpu.make_async_copy(gate_hbm, gate_ref, weight_sem.at[2])
    load_weight = pltpu.make_async_copy(weight_hbm, weight_ref, weight_sem.at[0])
    load_gate.start()
    load_beta.start()
    for s in range(steps):
        load(s, 0).start()
        load(s, 1).start()
    for s in range(steps):
        load(s, 2).start()
    load_weight.start()

    barrier = pltpu.get_barrier_semaphore()

    @pl.when(seq_here > 0)
    def _():
        pl.semaphore_signal(barrier, inc=1, device_id={"seq": seq_here - 1}, device_id_type=MESH)

    @pl.when(seq_here < seq_count - 1)
    def _():
        pl.semaphore_signal(barrier, inc=1, device_id={"seq": seq_here + 1}, device_id_type=MESH)

    for other in others:
        pl.semaphore_signal(barrier, inc=1, device_id={"head": other}, device_id_type=MESH)

    offset = seq_here * tokens
    ends = []
    running = 0
    for d in range(len_ref.shape[1]):
        running = running + len_ref[0, d]
        ends.append(running)

    def segment(pos):
        total = jnp.zeros(pos.shape, jnp.int32)
        for end in ends:
            total += jnp.where(pos >= end, 1, 0)
        return total

    row_i = lax.broadcasted_iota(jnp.int32, (sub, sub), 0)
    col_i = lax.broadcasted_iota(jnp.int32, (sub, sub), 1)
    eye = row_i == col_i
    eye_f = jnp.where(eye, 1.0, 0.0).astype(f32)
    tok_i = lax.broadcasted_iota(jnp.int32, (BLOCK, sub), 0)
    tok_j = lax.broadcasted_iota(jnp.int32, (BLOCK, sub), 1)
    pick_tok = tok_j == tok_i * refl + refl - 1
    levels = []
    size = refl
    while size < sub:
        big = min(4 * size, sub)
        levels.append((row_i // big == col_i // big) & (row_i // size > col_i // size))
        size = big

    load_gate.wait()
    load_beta.wait()
    table = sub_rows(gate_ref[...], jnp.where(tok_i <= tok_j // refl, 1.0, 0.0).astype(bf16), blocks)
    total = 0.0
    for j in range(refl):
        pick = jnp.where(tok_i * refl + j == tok_j, 1.0, 0.0).astype(bf16)
        total += sub_rows(beta_ref[j], pick, blocks)
    for b in range(blocks):
        rows_ref[b, 0] = table[:, b * sub : (b + 1) * sub]
        rows_ref[b, 1] = total[:, b * sub : (b + 1) * sub]

    def geometry(b):
        start = offset + b * BLOCK
        seg_row = segment(start + lax.broadcasted_iota(jnp.int32, (1, sub), 1) // refl)
        before = jnp.where(start == 0, -1, 0)
        last_seg = 0
        for end in ends:
            before += jnp.where(start - 1 >= end, 1, 0)
            last_seg += jnp.where(start + BLOCK - 1 >= end, 1, 0)
        return start, seg_row, before, last_seg

    pairs = [(h, b) for h in range(HEADS_STEP) for b in range(blocks)]

    def over(stage, *lists):
        return [stage(h, b, *args) for (h, b), *args in zip(pairs, *lists)]

    def cols(h):
        return slice(h * width, (h + 1) * width)

    def toks(b):
        return slice(b * BLOCK, (b + 1) * BLOCK)

    def column(values):
        return jnp.sum(jnp.where(eye, values, 0.0), axis=1, keepdims=True)

    def hop(h):
        return pltpu.make_async_remote_copy(
            src_ref=state_out.at[h],
            dst_ref=state_in.at[h],
            send_sem=state_send.at[h],
            recv_sem=state_recv.at[h],
            device_id={"seq": lax.rem(seq_here + 1, seq_count)},
            device_id_type=MESH,
        )

    def forward(h):
        hop(h).wait_recv()
        state = state_in[h]
        both = jnp.concatenate(split(map_ref[h]), axis=1)
        grown = add_ref[h] + mm(both, jnp.concatenate([state, state], axis=0))
        state_out[h] = grown.astype(bf16)
        hop(h).start()

    def near(s, b):
        def keys(h):
            return kflat_ref[s, b * sub : (b + 1) * sub, cols(h)]

        def row(kind, h):
            return rows_ref[b, kind, pl.ds(s * HEADS_STEP + h, 1), :]

        return keys, row

    def states_step(s, carry):
        load(s, 0).wait()
        load(s, 1).wait()
        keys = lambda h, b: near(s, b)[0](h)
        row = lambda kind, h, b: near(s, b)[1](kind, h)
        geo = []
        for b in range(blocks):
            start, seg_row, before, last_seg = geometry(b)
            seg_col = segment(start + lax.broadcasted_iota(jnp.int32, (sub, 1), 0) // refl)
            incl = (row_i >= col_i) & (seg_col == seg_row)
            geo.append((incl, seg_row == before, seg_col == last_seg, last_seg == before))

        for h, b in pairs:
            kflat_ref[s, b * sub : (b + 1) * sub, cols(h)] = k_ref[s, toks(b), :, cols(h)].reshape(sub, width)

        def scales(h, b):
            gram = mm_nt(keys(h, b), keys(h, b))
            diag = jnp.where(eye, gram, 0.0)
            n_row = lax.rsqrt(jnp.sum(diag, axis=0, keepdims=True) + epsilon)
            n_col = lax.rsqrt(jnp.sum(diag, axis=1, keepdims=True) + epsilon)
            scale_ref[b, pl.ds(s * HEADS_STEP + h, 1), :] = n_row
            c_row = row(0, h, b)
            c_col = column(c_row)
            ratio = jnp.where(geo[b][0], jnp.exp(jnp.minimum(c_col - c_row, 0.0)), 0.0)
            low = jnp.where(eye, 0.0, (column(row(1, h, b)) * n_col) * ratio * gram * n_row)
            return low, n_row, n_col, c_col

        lows, n_rows, n_cols, c_cols = zip(*over(scales))
        invs = [eye_f - jnp.where(row_i // refl == col_i // refl, low, 0.0) for low in lows]
        for mask in levels:
            heads_b = [inv.astype(bf16) for inv in invs]
            nils = [
                mm(inv, jnp.where(mask, low, 0.0).astype(bf16)).astype(bf16)
                for inv, low in zip(heads_b, lows)
            ]
            both = [mm(nil, jnp.concatenate([nil, inv], axis=1)) for nil, inv in zip(nils, heads_b)]
            halves = [inv - pair[:, sub:] for inv, pair in zip(invs, both)]
            invs = [
                half + mm(pair[:, :sub].astype(bf16), half.astype(bf16))
                for half, pair in zip(halves, both)
            ]

        def residual(h, b, inv, low):
            inv_b = inv.astype(bf16)
            low_2 = jnp.concatenate(split(low), axis=1)
            return eye_f - inv_b.astype(f32) - mm(low_2, jnp.concatenate([inv_b, inv_b], axis=0))

        resids = over(residual, invs, lows)

        def refine(h, b, inv, resid):
            inv_b = inv.astype(bf16)
            return inv_b.astype(f32) + mm(inv_b, resid.astype(bf16))

        invs = over(refine, invs, resids)

        def write(h, b, inv, n_row):
            carry_row = jnp.where(geo[b][1], jnp.exp(row(0, h, b)), 0.0)
            by_beta = inv * row(1, h, b)
            tv = jnp.concatenate(split(by_beta), axis=1)
            tk = jnp.concatenate(split(by_beta * (carry_row * n_row)), axis=1)
            vb, kb = v_ref[s, toks(b), :, cols(h)].reshape(sub, width), keys(h, b)
            return jnp.concatenate(
                [mm(tv, jnp.concatenate([vb, vb], axis=0)), mm(tk, jnp.concatenate([kb, kb], axis=0))],
                axis=1,
            )

        writes = over(write, invs, n_rows)

        def block_step(h, b, wrote, n_col, c_col):
            wrote_ref[s * HEADS_STEP + h, b] = wrote.astype(bf16)
            c_end = row(0, h, b)[:, sub - 1 : sub]
            e_col = jnp.where(geo[b][2], jnp.exp(jnp.minimum(c_end - c_col, 0.0)), 0.0) * n_col
            kb = keys(h, b)
            moved = mm_tn(
                jnp.concatenate([kb, kb], axis=0), jnp.concatenate(split(wrote * e_col), axis=0)
            )
            carry_end = jnp.where(geo[b][3], jnp.exp(c_end), 0.0)
            return moved[:, :width], carry_end * eye_f - moved[:, width:]

        made = over(block_step, writes, n_cols, c_cols)
        states = [jnp.concatenate(made[h * blocks], axis=1) for h in range(HEADS_STEP)]
        for b in range(1, blocks):
            for h in range(HEADS_STEP):
                block_add, block_map = made[h * blocks + b]
                s_hi = states[h].astype(bf16)
                prefix_ref[s * HEADS_STEP + h, b - 1] = s_hi
                grown = mm(
                    jnp.concatenate(split(block_map), axis=1), jnp.concatenate([s_hi, s_hi], axis=0)
                )
                states[h] = jnp.concatenate([grown[:, :width] + block_add, grown[:, width:]], axis=1)
        for h in range(HEADS_STEP):
            add_ref[s * HEADS_STEP + h] = states[h][:, :width]
            map_ref[s * HEADS_STEP + h] = states[h][:, width:]
            state_out[s * HEADS_STEP + h] = states[h][:, :width].astype(bf16)

        @pl.when(s == 0)
        def _():
            expected = jnp.where(first, 0, 1) + jnp.where(last, 0, 1) + head_count - 1
            pl.semaphore_wait(pltpu.get_barrier_semaphore(), expected)

        @pl.when(first & (seq_here < seq_count - 1))
        def _():
            for h in range(HEADS_STEP):
                hop(s * HEADS_STEP + h).start()

        @pl.when((s > 0) & (seq_here == 1) & (seq_here < seq_count - 1))
        def _():
            for h in range(HEADS_STEP):
                forward((s - 1) * HEADS_STEP + h)

        return carry

    lax.fori_loop(0, steps, states_step, 0)

    @pl.when(first)
    def _():
        state_in[...] = jnp.zeros_like(state_in)

    if steps > 1:
        @pl.when((seq_here > 1) & (seq_here < seq_count - 1))
        def _():
            for h in range((steps - 1) * HEADS_STEP):
                forward(h)

    def reads_step(s, carry):
        load(s, 2).wait()
        geo = []
        for b in range(blocks):
            start, seg_row, before, _ = geometry(b)
            seg_tok = segment(start + lax.broadcasted_iota(jnp.int32, (BLOCK, 1), 0))
            geo.append(((tok_j // refl <= tok_i) & (seg_tok == seg_row), seg_tok == before))

        def read_weights(h, b):
            keys, row = near(s, b)
            qb, c_row = q_ref[s, toks(b), cols(h)], row(0, h)
            n_row = scale_ref[b, pl.ds(s * HEADS_STEP + h, 1), :]
            qf = qb.astype(f32)
            nq = lax.rsqrt(jnp.sum(qf * qf, axis=1, keepdims=True) + epsilon) * width ** (-0.5)
            ct = jnp.sum(jnp.where(pick_tok, c_row, 0.0), axis=1, keepdims=True)
            ratio = jnp.where(geo[b][0], jnp.exp(jnp.minimum(ct - c_row, 0.0)), 0.0)
            carried = (jnp.where(geo[b][1], jnp.exp(ct), 0.0) * nq) * qf
            return (ratio * mm_nt(qb, keys(h)) * nq * n_row).astype(bf16), carried

        weights = over(read_weights)

        def read(h, b, weight):
            got = mm(weight[0], wrote_ref[s * HEADS_STEP + h, b])
            return got[:, :width], (weight[1] - got[:, width:]).astype(bf16)

        for (h, b), (own, back) in zip(pairs, over(read, weights)):
            if b:
                moved = mm(back, prefix_ref[s * HEADS_STEP + h, b - 1])
                own, back = own + moved[:, :width], moved[:, width:].astype(bf16)
            oloc_ref[s * HEADS_STEP + h, toks(b), :] = own
            read_ref[s * HEADS_STEP + h, toks(b), :] = back
        return carry

    lax.fori_loop(0, steps, reads_step, 0)

    done = (steps - 1) * HEADS_STEP
    for g in range(0, heads, FINISH_GROUP):
        group = range(g, min(g + FINISH_GROUP, heads))

        for h in group:
            if h < done:
                @pl.when(last & (seq_here > 0))
                def _():
                    hop(h).wait_recv()
            else:
                @pl.when(last & (seq_here > 0))
                def _():
                    hop(h).wait_recv()

                @pl.when((seq_here > 0) & (seq_here < seq_count - 1))
                def _():
                    forward(h)

        for h in group:
            out = oloc_ref[h] + mm(read_ref[h], state_in[h])
            scale = lax.rsqrt(jnp.mean(out * out, axis=-1, keepdims=True) + epsilon)
            normed_ref[:, cols(h)] = (out * scale * gain_ref[...]).astype(bf16)

    load_weight.wait()
    piece = weight_ref.shape[1] // PIECES
    copies = []
    for slot, other in enumerate(others):
        rows = normed_ref[pl.ds(pl.multiple_of(other * chunk, chunk), chunk), :]
        for p in range(PIECES):
            part = pl.ds(p * piece, piece)
            part_out[slot, :, part] = mm(rows, weight_ref[:, part]).astype(bf16)
            copies.append(
                pltpu.make_async_remote_copy(
                    src_ref=part_out.at[slot, :, part],
                    dst_ref=part_in.at[slot, :, part],
                    send_sem=part_send.at[slot, p],
                    recv_sem=part_recv.at[slot, p],
                    device_id={"head": other},
                    device_id_type=MESH,
                )
            )
            copies[-1].start()
    rows = normed_ref[pl.ds(pl.multiple_of(head_here * chunk, chunk), chunk), :]
    for p in range(PIECES):
        part = pl.ds(p * piece, piece)
        own_ref[:, part] = mm(rows, weight_ref[:, part])
    for p in range(PIECES):
        part = pl.ds(p * piece, piece)
        total = own_ref[:, part].astype(bf16).astype(f32)
        for slot in range(len(others)):
            copies[slot * PIECES + p].wait_recv()
            total += part_in[slot, :, part].astype(f32)
        out_ref[:, part] = total.astype(bf16)
    for copy in copies:
        copy.wait_send()

    @pl.when(seq_here < seq_count - 1)
    def _():
        for h in range(heads):
            hop(h).wait_send()


def body(queries, reflect_keys, reflect_values, reflect_beta, log_decay, prompt_lengths, norm_gain, out_weight):
    tokens, refl, wide = reflect_keys.shape[1:]
    heads = log_decay.shape[2]
    width = wide // heads
    blocks = tokens // BLOCK
    sub = refl * BLOCK
    head_count = lax.axis_size("head")
    chunk, model = tokens // head_count, out_weight.shape[1]
    steps, slots = heads // HEADS_STEP, max(head_count - 1, 1)
    wide_step = HEADS_STEP * width
    beta, gate = reflect_beta[0].transpose(1, 2, 0), log_decay[0].T
    dma = pltpu.SemaphoreType.DMA
    anywhere, vmem = pl.BlockSpec(memory_space=pl.ANY), pl.BlockSpec(memory_space=pltpu.VMEM)
    out = pl.pallas_call(
        functools.partial(mixer_kernel, refl, blocks),
        in_specs=[
            pl.BlockSpec(memory_space=pltpu.SMEM),
            anywhere, anywhere, anywhere, anywhere, anywhere, vmem, anywhere,
        ],
        out_specs=vmem,
        out_shape=pltpu.VMEM((chunk, model), bf16),
        scratch_shapes=[
            pltpu.VMEM((steps, tokens, wide_step), bf16),
            pltpu.VMEM((steps, tokens, refl, wide_step), bf16),
            pltpu.VMEM((steps, tokens, refl, wide_step), bf16),
            pltpu.VMEM(beta.shape, f32),
            pltpu.VMEM(gate.shape, f32),
            dma((steps, 3)),
            pltpu.VMEM((blocks, 2, heads, sub), f32),
            pltpu.VMEM((blocks, heads, sub), f32),
            pltpu.VMEM((steps, tokens * refl, wide_step), bf16),
            pltpu.VMEM((heads, blocks, sub, 2 * width), bf16),
            pltpu.VMEM((heads, max(blocks - 1, 1), width, 2 * width), bf16),
            pltpu.VMEM((heads, tokens, width), f32),
            pltpu.VMEM((heads, tokens, width), bf16),
            pltpu.VMEM((heads, width, width), f32),
            pltpu.VMEM((heads, width, width), f32),
            pltpu.VMEM(out_weight.shape, bf16),
            dma((3,)),
            pltpu.VMEM((heads, width, width), bf16),
            pltpu.VMEM((heads, width, width), bf16),
            pltpu.VMEM((tokens, wide), bf16),
            pltpu.VMEM((chunk, model), f32),
            pltpu.VMEM((slots, chunk, model), bf16),
            pltpu.VMEM((slots, chunk, model), bf16),
            dma((heads,)), dma((heads,)), dma((slots, PIECES)), dma((slots, PIECES)),
        ],
        compiler_params=pltpu.CompilerParams(
            collective_id=0, has_side_effects=True, vmem_limit_bytes=56 * 2**20
        ),
    )(
        prompt_lengths,
        queries[0],
        reflect_keys[0],
        reflect_values[0],
        beta,
        gate,
        norm_gain[None],
        out_weight,
    )
    return out[None]


def solution(mesh):
    in_specs = (
        P(("parts", "rep"), "seq", "head"),
        P(("parts", "rep"), "seq", None, "head"),
        P(("parts", "rep"), "seq", None, "head"),
        P(("parts", "rep"), "seq", None, "head"),
        P(("parts", "rep"), "seq", "head"),
        P(("parts", "rep"), None),
        P(),
        P("head", None),
    )
    out_specs = P(("parts", "rep"), ("seq", "head"), None)
    return jax.shard_map(body, mesh=mesh, in_specs=in_specs, out_specs=out_specs, check_vma=False)
```

```python
import functools

import jax
import jax.numpy as jnp
from jax import lax
from jax.experimental import pallas as pl
from jax.experimental.pallas import tpu as pltpu
from jax.sharding import PartitionSpec as P

BLOCK = 64
HEADS_STEP = 4
FINISH_GROUP = 2
PIECES = 4
SHARE = 50
SHARE_PARTS = 8
MID_RELAYS = (1, 3)
MESH = pl.DeviceIdType.MESH

epsilon = 1e-06
f32 = jnp.float32
bf16 = jnp.bfloat16
highest = lax.Precision.HIGHEST


def mm(a, b, precision=None):
    return jnp.dot(a, b, preferred_element_type=f32, precision=precision)


def mm_nt(a, b):
    return lax.dot_general(a, b, (((1,), (1,)), ((), ())), preferred_element_type=f32)


def mm_tn(a, b):
    return lax.dot_general(a, b, (((0,), (0,)), ((), ())), preferred_element_type=f32)


def split(x):
    hi = x.astype(bf16)
    return hi, (x - hi.astype(f32)).astype(bf16)


def split3(x):
    hi = x.astype(bf16).astype(f32)
    mid = (x - hi).astype(bf16).astype(f32)
    return [hi, mid, x - hi - mid]


def sub_rows(x, pattern, blocks):
    rows = x.shape[0]
    zero = jnp.zeros_like(pattern)
    table = jnp.concatenate(
        [jnp.concatenate([pattern if c == r else zero for c in range(blocks)], axis=1) for r in range(blocks)],
        axis=0,
    )
    got = mm(jnp.concatenate(split3(x), axis=0).astype(bf16), table)
    return got[:rows] + got[rows : 2 * rows] + got[2 * rows :]


def sharing():
    return all(lax.axis_size(name) == 2 for name in ("head", "parts", "rep"))


def mixer_kernel(
    refl, blocks, len_ref, q_hbm, k_hbm, v_hbm, beta_hbm, gate_hbm, gain_ref, weight_hbm, out_ref,
    q_ref, k_ref, v_ref, beta_ref, gate_ref, in_sem,
    rows_ref, scale_ref, kflat_ref, wrote_ref, prefix_ref, oloc_ref, read_ref, add_ref, map_ref,
    weight_ref, weight_sem, state_in, state_out, normed_ref, own_ref, part_out, part_in,
    state_send, state_recv, part_send, part_recv,
    peer_ref, rows_in, x_send, x_recv, y_send, y_recv, core_send, core_recv, norm_send, norm_recv,
):
    heads, width = add_ref.shape[:2]
    steps = heads // HEADS_STEP
    wide = HEADS_STEP * width
    sub = refl * BLOCK
    tokens = blocks * BLOCK
    seq_count, head_count = lax.axis_size("seq"), lax.axis_size("head")
    seq_here, head_here = lax.axis_index("seq"), lax.axis_index("head")
    chunk = out_ref.shape[0]
    first, last = seq_here == 0, seq_here == seq_count - 1
    others = [lax.rem(head_here + d, head_count) for d in range(1, head_count)]
    shared = peer_ref.shape[1] if sharing() else 0
    parts_here, rep_here = lax.axis_index("parts"), lax.axis_index("rep")
    quarter = peer_ref.shape[0] // 4
    slab = quarter // SHARE_PARTS

    def slab_rows(rep, parts, j, count=1):
        at = (rep * 2 + parts) * quarter + j * slab
        return pl.ds(pl.multiple_of(at, slab), count * slab)

    def remote(src, dst, send, recv, device):
        return pltpu.make_async_remote_copy(
            src_ref=src, dst_ref=dst, send_sem=send, recv_sem=recv, device_id=device, device_id_type=MESH
        )

    def from_head(j):
        rows = slab_rows(rep_here, parts_here, j)
        return remote(
            weight_hbm.at[rows, pl.ds(0, shared)], peer_ref.at[rows],
            x_send.at[j], x_recv.at[j], {"head": 1 - head_here},
        )

    def over_parts(j, parts):
        rows = slab_rows(rep_here, parts, j)
        return remote(
            peer_ref.at[rows], peer_ref.at[rows], y_send.at[j], y_recv.at[j], {"parts": 1 - parts_here}
        )

    def over_cores(j, rep):
        count = 1 if j < SHARE_PARTS else SHARE_PARTS
        parts, at = (parts_here, j) if j < SHARE_PARTS else (1 - parts_here, 0)
        rows = slab_rows(rep, parts, at, count)
        return remote(
            peer_ref.at[rows], peer_ref.at[rows], core_send.at[j], core_recv.at[j], {"rep": 1 - rep_here}
        )

    def relay(j):
        from_head(j).wait_recv()
        over_parts(j, parts_here).start()
        over_cores(j, rep_here).start()

    def send_normed(h):
        span = cols(h)
        rows = pl.ds(pl.multiple_of(others[0] * chunk, chunk), chunk)
        return remote(
            normed_ref.at[rows, span], rows_in.at[:, span],
            norm_send.at[h], norm_recv.at[h], {"head": 1 - head_here},
        )

    def load(s, kind):
        span = pl.ds(pl.multiple_of(s * wide, wide), wide)
        src, dst = [
            (k_hbm.at[:, :, span], k_ref), (v_hbm.at[:, :, span], v_ref), (q_hbm.at[:, span], q_ref)
        ][kind]
        return pltpu.make_async_copy(src, dst.at[s], in_sem.at[s, kind])

    load_beta = pltpu.make_async_copy(beta_hbm, beta_ref, weight_sem.at[1])
    load_gate = pltpu.make_async_copy(gate_hbm, gate_ref, weight_sem.at[2])
    load_weight = pltpu.make_async_copy(weight_hbm, weight_ref, weight_sem.at[0])
    load_gate.start()
    load_beta.start()
    for s in range(steps):
        load(s, 0).start()
        load(s, 1).start()
    for s in range(steps):
        load(s, 2).start()
    load_weight.start()

    barrier = pltpu.get_barrier_semaphore()

    @pl.when(seq_here > 0)
    def _():
        pl.semaphore_signal(barrier, inc=1, device_id={"seq": seq_here - 1}, device_id_type=MESH)

    @pl.when(seq_here < seq_count - 1)
    def _():
        pl.semaphore_signal(barrier, inc=1, device_id={"seq": seq_here + 1}, device_id_type=MESH)

    for other in others:
        pl.semaphore_signal(barrier, inc=1, device_id={"head": other}, device_id_type=MESH)
    if shared:
        pl.semaphore_signal(barrier, inc=1, device_id={"parts": 1 - parts_here}, device_id_type=MESH)
        pl.semaphore_signal(barrier, inc=1, device_id={"rep": 1 - rep_here}, device_id_type=MESH)

    offset = seq_here * tokens
    ends = []
    running = 0
    for d in range(len_ref.shape[1]):
        running = running + len_ref[0, d]
        ends.append(running)

    def segment(pos):
        total = jnp.zeros(pos.shape, jnp.int32)
        for end in ends:
            total += jnp.where(pos >= end, 1, 0)
        return total

    row_i = lax.broadcasted_iota(jnp.int32, (sub, sub), 0)
    col_i = lax.broadcasted_iota(jnp.int32, (sub, sub), 1)
    eye = row_i == col_i
    eye_f = jnp.where(eye, 1.0, 0.0).astype(f32)
    tok_i = lax.broadcasted_iota(jnp.int32, (BLOCK, sub), 0)
    tok_j = lax.broadcasted_iota(jnp.int32, (BLOCK, sub), 1)
    pick_tok = tok_j == tok_i * refl + refl - 1
    levels = []
    size = refl
    while size < sub:
        big = min(4 * size, sub)
        levels.append((row_i // big == col_i // big) & (row_i // size > col_i // size))
        size = big

    expected = jnp.where(first, 0, 1) + jnp.where(last, 0, 1) + head_count - 1 + (2 if shared else 0)
    pl.semaphore_wait(barrier, expected)
    if shared:
        for j in range(SHARE_PARTS):
            from_head(j).start()

    load_gate.wait()
    load_beta.wait()
    table = sub_rows(gate_ref[...], jnp.where(tok_i <= tok_j // refl, 1.0, 0.0).astype(bf16), blocks)
    total = 0.0
    for j in range(refl):
        pick = jnp.where(tok_i * refl + j == tok_j, 1.0, 0.0).astype(bf16)
        total += sub_rows(beta_ref[j], pick, blocks)
    for b in range(blocks):
        rows_ref[b, 0] = table[:, b * sub : (b + 1) * sub]
        rows_ref[b, 1] = total[:, b * sub : (b + 1) * sub]

    def geometry(b):
        start = offset + b * BLOCK
        seg_row = segment(start + lax.broadcasted_iota(jnp.int32, (1, sub), 1) // refl)
        before = jnp.where(start == 0, -1, 0)
        last_seg = 0
        for end in ends:
            before += jnp.where(start - 1 >= end, 1, 0)
            last_seg += jnp.where(start + BLOCK - 1 >= end, 1, 0)
        return start, seg_row, before, last_seg

    pairs = [(h, b) for h in range(HEADS_STEP) for b in range(blocks)]

    def over(stage, *lists):
        return [stage(h, b, *args) for (h, b), *args in zip(pairs, *lists)]

    def cols(h):
        return slice(h * width, (h + 1) * width)

    def toks(b):
        return slice(b * BLOCK, (b + 1) * BLOCK)

    def column(values):
        return jnp.sum(jnp.where(eye, values, 0.0), axis=1, keepdims=True)

    def hop(h):
        return pltpu.make_async_remote_copy(
            src_ref=state_out.at[h],
            dst_ref=state_in.at[h],
            send_sem=state_send.at[h],
            recv_sem=state_recv.at[h],
            device_id={"seq": lax.rem(seq_here + 1, seq_count)},
            device_id_type=MESH,
        )

    def forward(h):
        hop(h).wait_recv()
        state = state_in[h]
        both = jnp.concatenate(split(map_ref[h]), axis=1)
        grown = add_ref[h] + mm(both, jnp.concatenate([state, state], axis=0))
        state_out[h] = grown.astype(bf16)
        hop(h).start()

    def near(s, b):
        def keys(h):
            return kflat_ref[s, b * sub : (b + 1) * sub, cols(h)]

        def row(kind, h):
            return rows_ref[b, kind, pl.ds(s * HEADS_STEP + h, 1), :]

        return keys, row

    def states_step(s, carry):
        load(s, 0).wait()
        load(s, 1).wait()
        keys = lambda h, b: near(s, b)[0](h)
        row = lambda kind, h, b: near(s, b)[1](kind, h)
        geo = []
        for b in range(blocks):
            start, seg_row, before, last_seg = geometry(b)
            seg_col = segment(start + lax.broadcasted_iota(jnp.int32, (sub, 1), 0) // refl)
            incl = (row_i >= col_i) & (seg_col == seg_row)
            geo.append((incl, seg_row == before, seg_col == last_seg, last_seg == before))

        for h, b in pairs:
            kflat_ref[s, b * sub : (b + 1) * sub, cols(h)] = k_ref[s, toks(b), :, cols(h)].reshape(sub, width)

        def scales(h, b):
            gram = mm_nt(keys(h, b), keys(h, b))
            diag = jnp.where(eye, gram, 0.0)
            n_row = lax.rsqrt(jnp.sum(diag, axis=0, keepdims=True) + epsilon)
            n_col = lax.rsqrt(jnp.sum(diag, axis=1, keepdims=True) + epsilon)
            scale_ref[b, pl.ds(s * HEADS_STEP + h, 1), :] = n_row
            c_row = row(0, h, b)
            c_col = column(c_row)
            ratio = jnp.where(geo[b][0], jnp.exp(jnp.minimum(c_col - c_row, 0.0)), 0.0)
            low = jnp.where(eye, 0.0, (column(row(1, h, b)) * n_col) * ratio * gram * n_row)
            return low, n_row, n_col, c_col

        lows, n_rows, n_cols, c_cols = zip(*over(scales))
        invs = [eye_f - jnp.where(row_i // refl == col_i // refl, low, 0.0) for low in lows]
        for mask in levels:
            heads_b = [inv.astype(bf16) for inv in invs]
            nils = [
                mm(inv, jnp.where(mask, low, 0.0).astype(bf16)).astype(bf16)
                for inv, low in zip(heads_b, lows)
            ]
            both = [mm(nil, jnp.concatenate([nil, inv], axis=1)) for nil, inv in zip(nils, heads_b)]
            halves = [inv - pair[:, sub:] for inv, pair in zip(invs, both)]
            invs = [
                half + mm(pair[:, :sub].astype(bf16), half.astype(bf16))
                for half, pair in zip(halves, both)
            ]

        if shared:
            @pl.when(s > 0)
            def _():
                for j in range(*MID_RELAYS):
                    relay(j)

        def residual(h, b, inv, low):
            inv_b = inv.astype(bf16)
            low_2 = jnp.concatenate(split(low), axis=1)
            return eye_f - inv_b.astype(f32) - mm(low_2, jnp.concatenate([inv_b, inv_b], axis=0))

        resids = over(residual, invs, lows)

        def refine(h, b, inv, resid):
            inv_b = inv.astype(bf16)
            return inv_b.astype(f32) + mm(inv_b, resid.astype(bf16))

        invs = over(refine, invs, resids)

        def write(h, b, inv, n_row):
            carry_row = jnp.where(geo[b][1], jnp.exp(row(0, h, b)), 0.0)
            by_beta = inv * row(1, h, b)
            tv = jnp.concatenate(split(by_beta), axis=1)
            tk = jnp.concatenate(split(by_beta * (carry_row * n_row)), axis=1)
            vb, kb = v_ref[s, toks(b), :, cols(h)].reshape(sub, width), keys(h, b)
            return jnp.concatenate(
                [mm(tv, jnp.concatenate([vb, vb], axis=0)), mm(tk, jnp.concatenate([kb, kb], axis=0))],
                axis=1,
            )

        writes = over(write, invs, n_rows)

        def block_step(h, b, wrote, n_col, c_col):
            wrote_ref[s * HEADS_STEP + h, b] = wrote.astype(bf16)
            c_end = row(0, h, b)[:, sub - 1 : sub]
            e_col = jnp.where(geo[b][2], jnp.exp(jnp.minimum(c_end - c_col, 0.0)), 0.0) * n_col
            kb = keys(h, b)
            moved = mm_tn(
                jnp.concatenate([kb, kb], axis=0), jnp.concatenate(split(wrote * e_col), axis=0)
            )
            carry_end = jnp.where(geo[b][3], jnp.exp(c_end), 0.0)
            return moved[:, :width], carry_end * eye_f - moved[:, width:]

        made = over(block_step, writes, n_cols, c_cols)
        states = [jnp.concatenate(made[h * blocks], axis=1) for h in range(HEADS_STEP)]
        for b in range(1, blocks):
            for h in range(HEADS_STEP):
                block_add, block_map = made[h * blocks + b]
                s_hi = states[h].astype(bf16)
                prefix_ref[s * HEADS_STEP + h, b - 1] = s_hi
                grown = mm(
                    jnp.concatenate(split(block_map), axis=1), jnp.concatenate([s_hi, s_hi], axis=0)
                )
                states[h] = jnp.concatenate([grown[:, :width] + block_add, grown[:, width:]], axis=1)
        for h in range(HEADS_STEP):
            add_ref[s * HEADS_STEP + h] = states[h][:, :width]
            map_ref[s * HEADS_STEP + h] = states[h][:, width:]
            state_out[s * HEADS_STEP + h] = states[h][:, :width].astype(bf16)

        @pl.when(first & (seq_here < seq_count - 1))
        def _():
            for h in range(HEADS_STEP):
                hop(s * HEADS_STEP + h).start()

        @pl.when((s > 0) & (seq_here == 1) & (seq_here < seq_count - 1))
        def _():
            for h in range(HEADS_STEP):
                forward((s - 1) * HEADS_STEP + h)

        if shared:
            @pl.when(s == 0)
            def _():
                for j in range(MID_RELAYS[0]):
                    relay(j)

        return carry

    lax.fori_loop(0, steps, states_step, 0)
    relayed = MID_RELAYS[1] if steps > 1 else MID_RELAYS[0]
    if shared:
        relay(relayed)
        relayed += 1

    @pl.when(first)
    def _():
        state_in[...] = jnp.zeros_like(state_in)

    if steps > 1:
        @pl.when((seq_here > 1) & (seq_here < seq_count - 1))
        def _():
            for h in range((steps - 1) * HEADS_STEP):
                forward(h)

    def reads_step(s, carry):
        load(s, 2).wait()
        geo = []
        for b in range(blocks):
            start, seg_row, before, _ = geometry(b)
            seg_tok = segment(start + lax.broadcasted_iota(jnp.int32, (BLOCK, 1), 0))
            geo.append(((tok_j // refl <= tok_i) & (seg_tok == seg_row), seg_tok == before))

        def read_weights(h, b):
            keys, row = near(s, b)
            qb, c_row = q_ref[s, toks(b), cols(h)], row(0, h)
            n_row = scale_ref[b, pl.ds(s * HEADS_STEP + h, 1), :]
            qf = qb.astype(f32)
            nq = lax.rsqrt(jnp.sum(qf * qf, axis=1, keepdims=True) + epsilon) * width ** (-0.5)
            ct = jnp.sum(jnp.where(pick_tok, c_row, 0.0), axis=1, keepdims=True)
            ratio = jnp.where(geo[b][0], jnp.exp(jnp.minimum(ct - c_row, 0.0)), 0.0)
            carried = (jnp.where(geo[b][1], jnp.exp(ct), 0.0) * nq) * qf
            return (ratio * mm_nt(qb, keys(h)) * nq * n_row).astype(bf16), carried

        weights = over(read_weights)

        def read(h, b, weight):
            got = mm(weight[0], wrote_ref[s * HEADS_STEP + h, b])
            return got[:, :width], (weight[1] - got[:, width:]).astype(bf16)

        for (h, b), (own, back) in zip(pairs, over(read, weights)):
            if b:
                moved = mm(back, prefix_ref[s * HEADS_STEP + h, b - 1])
                own, back = own + moved[:, :width], moved[:, width:].astype(bf16)
            oloc_ref[s * HEADS_STEP + h, toks(b), :] = own
            read_ref[s * HEADS_STEP + h, toks(b), :] = back
        if shared:
            @pl.when(s == 0)
            def _():
                relay(relayed)
        return carry

    lax.fori_loop(0, steps, reads_step, 0)
    relayed += 1

    done = (steps - 1) * HEADS_STEP
    for g in range(0, heads, FINISH_GROUP):
        group = range(g, min(g + FINISH_GROUP, heads))

        for h in group:
            if h < done:
                @pl.when(last & (seq_here > 0))
                def _():
                    hop(h).wait_recv()
            else:
                @pl.when(last & (seq_here > 0))
                def _():
                    hop(h).wait_recv()

                @pl.when((seq_here > 0) & (seq_here < seq_count - 1))
                def _():
                    forward(h)

        for h in group:
            out = oloc_ref[h] + mm(read_ref[h], state_in[h])
            scale = lax.rsqrt(jnp.mean(out * out, axis=-1, keepdims=True) + epsilon)
            normed_ref[:, cols(h)] = (out * scale * gain_ref[...]).astype(bf16)

        if shared:
            for h in group:
                send_normed(h).start()
            if relayed < SHARE_PARTS:
                relay(relayed)
                relayed += 1

    load_weight.wait()
    if shared:
        for j in range(relayed, SHARE_PARTS):
            relay(j)
    piece = (weight_ref.shape[1] - shared) // PIECES
    copies = []
    for slot, other in enumerate(others):
        rows = normed_ref[pl.ds(pl.multiple_of(other * chunk, chunk), chunk), :]
        for p in range(PIECES):
            part = pl.ds(p * piece, piece)
            part_out[slot, :, part] = mm(rows, weight_ref[:, pl.ds(shared + p * piece, piece)]).astype(bf16)
            copies.append(
                pltpu.make_async_remote_copy(
                    src_ref=part_out.at[slot, :, part],
                    dst_ref=part_in.at[slot, :, part],
                    send_sem=part_send.at[slot, p],
                    recv_sem=part_recv.at[slot, p],
                    device_id={"head": other},
                    device_id_type=MESH,
                )
            )
            copies[-1].start()
    rows = normed_ref[pl.ds(pl.multiple_of(head_here * chunk, chunk), chunk), :]
    if shared:
        for j in range(SHARE_PARTS):
            over_parts(j, 1 - parts_here).wait_recv()
        over_cores(SHARE_PARTS, rep_here).start()
    for p in range(PIECES):
        part = pl.ds(shared + p * piece, piece)
        own_ref[:, part] = mm(rows, weight_ref[:, part])
    if shared:
        portion = shared // PIECES
        for p in range(PIECES):
            part = pl.ds(p * portion, portion)
            own_ref[:, part] = mm(rows, weight_ref[:, part])
        for j in range(SHARE_PARTS + 1):
            over_cores(j, 1 - rep_here).wait_recv()
        for h in range(heads):
            send_normed(h).wait_recv()
        for p in range(PIECES):
            part = pl.ds(p * portion, portion)
            peer = mm(rows_in[...], peer_ref[:, part])
            total = own_ref[:, part].astype(bf16).astype(f32) + peer.astype(bf16).astype(f32)
            out_ref[:, part] = total.astype(bf16)
    for p in range(PIECES):
        part = pl.ds(p * piece, piece)
        spot = pl.ds(shared + p * piece, piece)
        total = own_ref[:, spot].astype(bf16).astype(f32)
        for slot in range(len(others)):
            copies[slot * PIECES + p].wait_recv()
            total += part_in[slot, :, part].astype(f32)
        out_ref[:, spot] = total.astype(bf16)
    for copy in copies:
        copy.wait_send()
    if shared:
        for j in range(SHARE_PARTS):
            from_head(j).wait_send()
            over_parts(j, parts_here).wait_send()
        for j in range(SHARE_PARTS + 1):
            over_cores(j, rep_here).wait_send()
        for h in range(heads):
            send_normed(h).wait_send()

    @pl.when(seq_here < seq_count - 1)
    def _():
        for h in range(heads):
            hop(h).wait_send()


def body(queries, reflect_keys, reflect_values, reflect_beta, log_decay, prompt_lengths, norm_gain, out_weight):
    tokens, refl, wide = reflect_keys.shape[1:]
    heads = log_decay.shape[2]
    width = wide // heads
    blocks = tokens // BLOCK
    sub = refl * BLOCK
    head_count = lax.axis_size("head")
    chunk, model = tokens // head_count, out_weight.shape[1]
    steps, slots = heads // HEADS_STEP, max(head_count - 1, 1)
    wide_step = HEADS_STEP * width
    shared = model * SHARE // 128 // 100 * 128 if sharing() else 0
    peer_shape = (out_weight.shape[0], shared) if shared else (32, 128)
    rest = model - shared
    beta, gate = reflect_beta[0].transpose(1, 2, 0), log_decay[0].T
    dma = pltpu.SemaphoreType.DMA
    anywhere, vmem = pl.BlockSpec(memory_space=pl.ANY), pl.BlockSpec(memory_space=pltpu.VMEM)
    out = pl.pallas_call(
        functools.partial(mixer_kernel, refl, blocks),
        in_specs=[
            pl.BlockSpec(memory_space=pltpu.SMEM),
            anywhere, anywhere, anywhere, anywhere, anywhere, vmem, anywhere,
        ],
        out_specs=vmem,
        out_shape=pltpu.VMEM((chunk, model), bf16),
        scratch_shapes=[
            pltpu.VMEM((steps, tokens, wide_step), bf16),
            pltpu.VMEM((steps, tokens, refl, wide_step), bf16),
            pltpu.VMEM((steps, tokens, refl, wide_step), bf16),
            pltpu.VMEM(beta.shape, f32),
            pltpu.VMEM(gate.shape, f32),
            dma((steps, 3)),
            pltpu.VMEM((blocks, 2, heads, sub), f32),
            pltpu.VMEM((blocks, heads, sub), f32),
            pltpu.VMEM((steps, tokens * refl, wide_step), bf16),
            pltpu.VMEM((heads, blocks, sub, 2 * width), bf16),
            pltpu.VMEM((heads, max(blocks - 1, 1), width, 2 * width), bf16),
            pltpu.VMEM((heads, tokens, width), f32),
            pltpu.VMEM((heads, tokens, width), bf16),
            pltpu.VMEM((heads, width, width), f32),
            pltpu.VMEM((heads, width, width), f32),
            pltpu.VMEM(out_weight.shape, bf16),
            dma((3,)),
            pltpu.VMEM((heads, width, width), bf16),
            pltpu.VMEM((heads, width, width), bf16),
            pltpu.VMEM((tokens, wide), bf16),
            pltpu.VMEM((chunk, model), f32),
            pltpu.VMEM((slots, chunk, rest), bf16),
            pltpu.VMEM((slots, chunk, rest), bf16),
            dma((heads,)), dma((heads,)), dma((slots, PIECES)), dma((slots, PIECES)),
            pltpu.VMEM(peer_shape, bf16),
            pltpu.VMEM((chunk, wide), bf16),
            dma((SHARE_PARTS,)), dma((SHARE_PARTS,)), dma((SHARE_PARTS,)), dma((SHARE_PARTS,)),
            dma((SHARE_PARTS + 1,)), dma((SHARE_PARTS + 1,)), dma((heads,)), dma((heads,)),
        ],
        compiler_params=pltpu.CompilerParams(
            collective_id=0, has_side_effects=True, vmem_limit_bytes=56 * 2**20
        ),
    )(
        prompt_lengths,
        queries[0],
        reflect_keys[0],
        reflect_values[0],
        beta,
        gate,
        norm_gain[None],
        out_weight,
    )
    return out[None]


def solution(mesh):
    in_specs = (
        P(("parts", "rep"), "seq", "head"),
        P(("parts", "rep"), "seq", None, "head"),
        P(("parts", "rep"), "seq", None, "head"),
        P(("parts", "rep"), "seq", None, "head"),
        P(("parts", "rep"), "seq", "head"),
        P(("parts", "rep"), None),
        P(),
        P("head", None),
    )
    out_specs = P(("parts", "rep"), ("seq", "head"), None)
    return jax.shard_map(body, mesh=mesh, in_specs=in_specs, out_specs=out_specs, check_vma=False)
```

```python
import functools

import jax
import jax.numpy as jnp
from jax import lax
from jax.experimental import pallas as pl
from jax.experimental.pallas import tpu as pltpu
from jax.sharding import PartitionSpec as P

BLOCK = 64
HEADS_STEP = 4
FINISH_GROUP = 2
PIECES = 4
SHARE = 50
SHARE_PARTS = 8
MID_RELAYS = (2, 4)
TEAM = 2
MESH = pl.DeviceIdType.MESH

epsilon = 1e-06
f32 = jnp.float32
bf16 = jnp.bfloat16
highest = lax.Precision.HIGHEST


def mm(a, b, precision=None):
    return jnp.dot(a, b, preferred_element_type=f32, precision=precision)


def mm_nt(a, b):
    return lax.dot_general(a, b, (((1,), (1,)), ((), ())), preferred_element_type=f32)


def mm_tn(a, b):
    return lax.dot_general(a, b, (((0,), (0,)), ((), ())), preferred_element_type=f32)


def split(x):
    hi = x.astype(bf16)
    return hi, (x - hi.astype(f32)).astype(bf16)


def split3(x):
    hi = x.astype(bf16).astype(f32)
    mid = (x - hi).astype(bf16).astype(f32)
    return [hi, mid, x - hi - mid]


def sub_rows(x, pattern, blocks):
    rows = x.shape[0]
    zero = jnp.zeros_like(pattern)
    table = jnp.concatenate(
        [jnp.concatenate([pattern if c == r else zero for c in range(blocks)], axis=1) for r in range(blocks)],
        axis=0,
    )
    got = mm(jnp.concatenate(split3(x), axis=0).astype(bf16), table)
    return got[:rows] + got[rows : 2 * rows] + got[2 * rows :]


def sharing():
    return all(lax.axis_size(name) == 2 for name in ("head", "parts", "rep"))


def mixer_kernel(
    refl, blocks, len_ref, q_hbm, k_hbm, v_hbm, beta_hbm, gate_hbm, gain_ref, weight_hbm, out_ref,
    q_ref, k_ref, v_ref, beta_ref, gate_ref, in_sem,
    rows_ref, scale_ref, kflat_ref, wrote_ref, prefix_ref, oloc_ref, read_ref, add_ref, map_ref,
    weight_ref, weight_sem, state_in, own_out, full_out, own_in, full_in, normed_ref, own_ref, part_out, part_in,
    own_send, own_recv, full_send, full_recv, part_send, part_recv,
    peer_ref, rows_in, x_send, x_recv, y_send, y_recv, core_send, core_recv, norm_send, norm_recv,
):
    heads, width = add_ref.shape[:2]
    steps = heads // HEADS_STEP
    wide = HEADS_STEP * width
    sub = refl * BLOCK
    tokens = blocks * BLOCK
    seq_count, head_count = lax.axis_size("seq"), lax.axis_size("head")
    seq_here, head_here = lax.axis_index("seq"), lax.axis_index("head")
    chunk = out_ref.shape[0]
    first, last = seq_here == 0, seq_here == seq_count - 1
    others = [lax.rem(head_here + d, head_count) for d in range(1, head_count)]
    shared = peer_ref.shape[1] if sharing() else 0
    parts_here, rep_here = lax.axis_index("parts"), lax.axis_index("rep")
    quarter = peer_ref.shape[0] // 4
    slab = quarter // SHARE_PARTS

    def slab_rows(rep, parts, j, count=1):
        at = (rep * 2 + parts) * quarter + j * slab
        return pl.ds(pl.multiple_of(at, slab), count * slab)

    def remote(src, dst, send, recv, device):
        return pltpu.make_async_remote_copy(
            src_ref=src, dst_ref=dst, send_sem=send, recv_sem=recv, device_id=device, device_id_type=MESH
        )

    def from_head(j):
        rows = slab_rows(rep_here, parts_here, j)
        return remote(
            weight_hbm.at[rows, pl.ds(0, shared)], peer_ref.at[rows],
            x_send.at[j], x_recv.at[j], {"head": 1 - head_here},
        )

    def over_parts(j, parts):
        rows = slab_rows(rep_here, parts, j)
        return remote(
            peer_ref.at[rows], peer_ref.at[rows], y_send.at[j], y_recv.at[j], {"parts": 1 - parts_here}
        )

    def over_cores(j, rep):
        count = 1 if j < SHARE_PARTS else SHARE_PARTS
        parts, at = (parts_here, j) if j < SHARE_PARTS else (1 - parts_here, 0)
        rows = slab_rows(rep, parts, at, count)
        return remote(
            peer_ref.at[rows], peer_ref.at[rows], core_send.at[j], core_recv.at[j], {"rep": 1 - rep_here}
        )

    def relay(j):
        from_head(j).wait_recv()
        over_parts(j, parts_here).start()
        over_cores(j, rep_here).start()

    def send_normed(h):
        span = cols(h)
        rows = pl.ds(pl.multiple_of(others[0] * chunk, chunk), chunk)
        return remote(
            normed_ref.at[rows, span], rows_in.at[:, span],
            norm_send.at[h], norm_recv.at[h], {"head": 1 - head_here},
        )

    def load(s, kind):
        span = pl.ds(pl.multiple_of(s * wide, wide), wide)
        src, dst = [
            (k_hbm.at[:, :, span], k_ref), (v_hbm.at[:, :, span], v_ref), (q_hbm.at[:, span], q_ref)
        ][kind]
        return pltpu.make_async_copy(src, dst.at[s], in_sem.at[s, kind])

    load_beta = pltpu.make_async_copy(beta_hbm, beta_ref, weight_sem.at[1])
    load_gate = pltpu.make_async_copy(gate_hbm, gate_ref, weight_sem.at[2])
    load_weight = pltpu.make_async_copy(weight_hbm, weight_ref, weight_sem.at[0])
    load_gate.start()
    load_beta.start()
    for s in range(steps):
        load(s, 0).start()
        load(s, 1).start()
    for s in range(steps):
        load(s, 2).start()
    load_weight.start()

    barrier = pltpu.get_barrier_semaphore()

    for move in (1, seq_count - 1):
        other = lax.rem(seq_here + move, seq_count)
        pl.semaphore_signal(barrier, inc=1, device_id={"seq": other}, device_id_type=MESH)

    for other in others:
        pl.semaphore_signal(barrier, inc=1, device_id={"head": other}, device_id_type=MESH)
    if shared:
        pl.semaphore_signal(barrier, inc=1, device_id={"parts": 1 - parts_here}, device_id_type=MESH)
        pl.semaphore_signal(barrier, inc=1, device_id={"rep": 1 - rep_here}, device_id_type=MESH)

    offset = seq_here * tokens
    ends = []
    running = 0
    for d in range(len_ref.shape[1]):
        running = running + len_ref[0, d]
        ends.append(running)

    def segment(pos):
        total = jnp.zeros(pos.shape, jnp.int32)
        for end in ends:
            total += jnp.where(pos >= end, 1, 0)
        return total

    row_i = lax.broadcasted_iota(jnp.int32, (sub, sub), 0)
    col_i = lax.broadcasted_iota(jnp.int32, (sub, sub), 1)
    eye = row_i == col_i
    eye_f = jnp.where(eye, 1.0, 0.0).astype(f32)
    tok_i = lax.broadcasted_iota(jnp.int32, (BLOCK, sub), 0)
    tok_j = lax.broadcasted_iota(jnp.int32, (BLOCK, sub), 1)
    pick_tok = tok_j == tok_i * refl + refl - 1
    levels = []
    size = refl
    while size < sub:
        big = min(4 * size, sub)
        levels.append((row_i // big == col_i // big) & (row_i // size > col_i // size))
        size = big

    pl.semaphore_wait(barrier, 2 + head_count - 1 + (2 if shared else 0))
    if shared:
        for j in range(SHARE_PARTS):
            from_head(j).start()

    load_gate.wait()
    load_beta.wait()
    table = sub_rows(gate_ref[...], jnp.where(tok_i <= tok_j // refl, 1.0, 0.0).astype(bf16), blocks)
    total = 0.0
    for j in range(refl):
        pick = jnp.where(tok_i * refl + j == tok_j, 1.0, 0.0).astype(bf16)
        total += sub_rows(beta_ref[j], pick, blocks)
    for b in range(blocks):
        rows_ref[b, 0] = table[:, b * sub : (b + 1) * sub]
        rows_ref[b, 1] = total[:, b * sub : (b + 1) * sub]

    def geometry(b):
        start = offset + b * BLOCK
        seg_row = segment(start + lax.broadcasted_iota(jnp.int32, (1, sub), 1) // refl)
        before = jnp.where(start == 0, -1, 0)
        last_seg = 0
        for end in ends:
            before += jnp.where(start - 1 >= end, 1, 0)
            last_seg += jnp.where(start + BLOCK - 1 >= end, 1, 0)
        return start, seg_row, before, last_seg

    pairs = [(h, b) for h in range(HEADS_STEP) for b in range(blocks)]

    def over(stage, *lists):
        return [stage(h, b, *args) for (h, b), *args in zip(pairs, *lists)]

    def cols(h):
        return slice(h * width, (h + 1) * width)

    def toks(b):
        return slice(b * BLOCK, (b + 1) * BLOCK)

    def column(values):
        return jnp.sum(jnp.where(eye, values, 0.0), axis=1, keepdims=True)

    reach = (seq_count * tokens // 2 - 2) // tokens
    direct = reach <= 1
    inner = (seq_here > 0) & (seq_here < seq_count - 1)
    following = {"seq": lax.rem(seq_here + 1, seq_count)}

    def send_own(h):
        return remote(own_out.at[h], own_in.at[h], own_send.at[h], own_recv.at[h], following)

    def send_full(h):
        return remote(full_out.at[h], full_in.at[h], full_send.at[h], full_recv.at[h], following)

    def pass_on(h, state):
        both = jnp.concatenate(split(map_ref[h]), axis=1)
        grown = add_ref[h] + mm(both, jnp.concatenate([state, state], axis=0))
        full_out[h] = grown.astype(bf16)
        send_full(h).start()

    def forward(h):
        if direct:
            send_own(h).wait_recv()
            pass_on(h, own_in[h])
        else:
            @pl.when(seq_here == 1)
            def _():
                send_own(h).wait_recv()
                pass_on(h, own_in[h])

            @pl.when(seq_here > 1)
            def _():
                send_full(h).wait_recv()
                pass_on(h, full_in[h])

    def near(s, b):
        def keys(h):
            return kflat_ref[s, b * sub : (b + 1) * sub, cols(h)]

        def row(kind, h):
            return rows_ref[b, kind, pl.ds(s * HEADS_STEP + h, 1), :]

        return keys, row

    def states_step(s, carry):
        load(s, 0).wait()
        load(s, 1).wait()
        keys = lambda h, b: near(s, b)[0](h)
        row = lambda kind, h, b: near(s, b)[1](kind, h)
        geo = []
        for b in range(blocks):
            start, seg_row, before, last_seg = geometry(b)
            seg_col = segment(start + lax.broadcasted_iota(jnp.int32, (sub, 1), 0) // refl)
            incl = (row_i >= col_i) & (seg_col == seg_row)
            geo.append((incl, seg_row == before, seg_col == last_seg, last_seg == before))

        for h, b in pairs:
            kflat_ref[s, b * sub : (b + 1) * sub, cols(h)] = k_ref[s, toks(b), :, cols(h)].reshape(sub, width)

        def scales(h, b):
            gram = mm_nt(keys(h, b), keys(h, b))
            diag = jnp.where(eye, gram, 0.0)
            n_row = lax.rsqrt(jnp.sum(diag, axis=0, keepdims=True) + epsilon)
            n_col = lax.rsqrt(jnp.sum(diag, axis=1, keepdims=True) + epsilon)
            scale_ref[b, pl.ds(s * HEADS_STEP + h, 1), :] = n_row
            c_row = row(0, h, b)
            c_col = column(c_row)
            ratio = jnp.where(geo[b][0], jnp.exp(jnp.minimum(c_col - c_row, 0.0)), 0.0)
            low = jnp.where(eye, 0.0, (column(row(1, h, b)) * n_col) * ratio * gram * n_row)
            return low, n_row, n_col, c_col

        lows, n_rows, n_cols, c_cols = zip(*over(scales))
        invs = [eye_f - jnp.where(row_i // refl == col_i // refl, low, 0.0) for low in lows]
        for mask in levels:
            heads_b = [inv.astype(bf16) for inv in invs]
            nils = [
                mm(inv, jnp.where(mask, low, 0.0).astype(bf16)).astype(bf16)
                for inv, low in zip(heads_b, lows)
            ]
            both = [mm(nil, jnp.concatenate([nil, inv], axis=1)) for nil, inv in zip(nils, heads_b)]
            halves = [inv - pair[:, sub:] for inv, pair in zip(invs, both)]
            invs = [
                half + mm(pair[:, :sub].astype(bf16), half.astype(bf16))
                for half, pair in zip(halves, both)
            ]

        if shared:
            @pl.when(s > 0)
            def _():
                for j in range(*MID_RELAYS):
                    relay(j)

        @pl.when((s > 0) & inner & (direct | (seq_here == 1)))
        def _():
            for h in range(HEADS_STEP):
                forward((s - 1) * HEADS_STEP + h)

        def residual(h, b, inv, low):
            inv_b = inv.astype(bf16)
            low_2 = jnp.concatenate(split(low), axis=1)
            return eye_f - inv_b.astype(f32) - mm(low_2, jnp.concatenate([inv_b, inv_b], axis=0))

        def refine(h, b, inv, resid):
            inv_b = inv.astype(bf16)
            return inv_b.astype(f32) + mm(inv_b, resid.astype(bf16))

        def write(h, b, inv, n_row):
            carry_row = jnp.where(geo[b][1], jnp.exp(row(0, h, b)), 0.0)
            by_beta = inv * row(1, h, b)
            tv = jnp.concatenate(split(by_beta), axis=1)
            tk = jnp.concatenate(split(by_beta * (carry_row * n_row)), axis=1)
            vb, kb = v_ref[s, toks(b), :, cols(h)].reshape(sub, width), keys(h, b)
            return jnp.concatenate(
                [mm(tv, jnp.concatenate([vb, vb], axis=0)), mm(tk, jnp.concatenate([kb, kb], axis=0))],
                axis=1,
            )

        def block_step(h, b, wrote, n_col, c_col):
            wrote_ref[s * HEADS_STEP + h, b] = wrote.astype(bf16)
            c_end = row(0, h, b)[:, sub - 1 : sub]
            e_col = jnp.where(geo[b][2], jnp.exp(jnp.minimum(c_end - c_col, 0.0)), 0.0) * n_col
            kb = keys(h, b)
            moved = mm_tn(
                jnp.concatenate([kb, kb], axis=0), jnp.concatenate(split(wrote * e_col), axis=0)
            )
            carry_end = jnp.where(geo[b][3], jnp.exp(c_end), 0.0)
            return moved[:, :width], carry_end * eye_f - moved[:, width:]

        made, states = {}, {}

        def some(heads_now, stage, *lists):
            return {(h, b): stage(h, b, *[l[h, b] for l in lists]) for h in heads_now for b in range(blocks)}

        def scan(heads_now, b):
            for h in heads_now:
                if b == 0:
                    states[h] = jnp.concatenate(made[h, 0], axis=1)
                    continue
                block_add, block_map = made[h, b]
                s_hi = states[h].astype(bf16)
                prefix_ref[s * HEADS_STEP + h, b - 1] = s_hi
                grown = mm(
                    jnp.concatenate(split(block_map), axis=1), jnp.concatenate([s_hi, s_hi], axis=0)
                )
                states[h] = jnp.concatenate([grown[:, :width] + block_add, grown[:, width:]], axis=1)

        def finish(heads_now):
            for h in heads_now:
                at = s * HEADS_STEP + h
                own_out[at] = states[h][:, :width].astype(bf16)
                send_own(at).start()
                add_ref[at] = states[h][:, :width]
                map_ref[at] = states[h][:, width:]

        named = lambda values: dict(zip(pairs, values))
        lows, invs, n_rows, n_cols, c_cols = map(named, (lows, invs, n_rows, n_cols, c_cols))
        teams = [list(range(h, min(h + TEAM, HEADS_STEP))) for h in range(0, HEADS_STEP, TEAM)]
        pending = []

        def catch_up(count):
            for _ in range(count):
                if pending:
                    pending.pop(0)()

        for team in teams:
            resids = some(team, residual, invs, lows)
            catch_up(2)
            better = some(team, refine, invs, resids)
            catch_up(1)
            writes = some(team, write, better, n_rows)
            catch_up(1)
            made.update(some(team, block_step, writes, n_cols, c_cols))
            catch_up(len(pending))
            pending = [functools.partial(scan, team, b) for b in range(blocks)]
            pending.append(functools.partial(finish, team))
        catch_up(len(pending))

        if shared:
            @pl.when(s == 0)
            def _():
                for j in range(MID_RELAYS[0]):
                    relay(j)

        return carry

    lax.fori_loop(0, steps, states_step, 0)
    relayed = MID_RELAYS[1] if steps > 1 else MID_RELAYS[0]
    if shared:
        for _ in range(2):
            relay(relayed)
            relayed += 1

    @pl.when(first)
    def _():
        state_in[...] = jnp.zeros_like(state_in)

    done = (steps - 1) * HEADS_STEP
    if done and not direct:
        @pl.when(inner & (seq_here > 1))
        def _():
            for h in range(done):
                forward(h)

    def reads_step(s, carry):
        load(s, 2).wait()
        geo = []
        for b in range(blocks):
            start, seg_row, before, _ = geometry(b)
            seg_tok = segment(start + lax.broadcasted_iota(jnp.int32, (BLOCK, 1), 0))
            geo.append(((tok_j // refl <= tok_i) & (seg_tok == seg_row), seg_tok == before))

        def read_weights(h, b):
            keys, row = near(s, b)
            qb, c_row = q_ref[s, toks(b), cols(h)], row(0, h)
            n_row = scale_ref[b, pl.ds(s * HEADS_STEP + h, 1), :]
            qf = qb.astype(f32)
            nq = lax.rsqrt(jnp.sum(qf * qf, axis=1, keepdims=True) + epsilon) * width ** (-0.5)
            ct = jnp.sum(jnp.where(pick_tok, c_row, 0.0), axis=1, keepdims=True)
            ratio = jnp.where(geo[b][0], jnp.exp(jnp.minimum(ct - c_row, 0.0)), 0.0)
            carried = (jnp.where(geo[b][1], jnp.exp(ct), 0.0) * nq) * qf
            return (ratio * mm_nt(qb, keys(h)) * nq * n_row).astype(bf16), carried

        weights = over(read_weights)

        def read(h, b, weight):
            got = mm(weight[0], wrote_ref[s * HEADS_STEP + h, b])
            return got[:, :width], (weight[1] - got[:, width:]).astype(bf16)

        for (h, b), (own, back) in zip(pairs, over(read, weights)):
            if b:
                moved = mm(back, prefix_ref[s * HEADS_STEP + h, b - 1])
                own, back = own + moved[:, :width], moved[:, width:].astype(bf16)
            oloc_ref[s * HEADS_STEP + h, toks(b), :] = own
            read_ref[s * HEADS_STEP + h, toks(b), :] = back
        if shared:
            @pl.when(s == 0)
            def _():
                relay(relayed)
        return carry

    lax.fori_loop(0, steps, reads_step, 0)
    relayed += 1

    for g in range(0, heads, FINISH_GROUP):
        group = range(g, min(g + FINISH_GROUP, heads))

        for h in group:
            if h >= done:
                @pl.when(inner)
                def _():
                    forward(h)

            @pl.when(last & (seq_here == 1))
            def _():
                send_own(h).wait_recv()

            @pl.when((seq_here > 1) & (direct | last))
            def _():
                send_full(h).wait_recv()

            @pl.when(seq_here == 1)
            def _():
                state_in[h] = own_in[h]

            @pl.when(seq_here > 1)
            def _():
                state_in[h] = full_in[h]

        for h in group:
            out = oloc_ref[h] + mm(read_ref[h], state_in[h])
            scale = lax.rsqrt(jnp.mean(out * out, axis=-1, keepdims=True) + epsilon)
            normed_ref[:, cols(h)] = (out * scale * gain_ref[...]).astype(bf16)

        if shared:
            for h in group:
                send_normed(h).start()
            if relayed < SHARE_PARTS:
                relay(relayed)
                relayed += 1

    load_weight.wait()
    if shared:
        for j in range(relayed, SHARE_PARTS):
            relay(j)
    piece = (weight_ref.shape[1] - shared) // PIECES
    copies = []
    for slot, other in enumerate(others):
        rows = normed_ref[pl.ds(pl.multiple_of(other * chunk, chunk), chunk), :]
        for p in range(PIECES):
            part = pl.ds(p * piece, piece)
            part_out[slot, :, part] = mm(rows, weight_ref[:, pl.ds(shared + p * piece, piece)]).astype(bf16)
            copies.append(
                pltpu.make_async_remote_copy(
                    src_ref=part_out.at[slot, :, part],
                    dst_ref=part_in.at[slot, :, part],
                    send_sem=part_send.at[slot, p],
                    recv_sem=part_recv.at[slot, p],
                    device_id={"head": other},
                    device_id_type=MESH,
                )
            )
            copies[-1].start()
    rows = normed_ref[pl.ds(pl.multiple_of(head_here * chunk, chunk), chunk), :]
    if shared:
        for j in range(SHARE_PARTS):
            over_parts(j, 1 - parts_here).wait_recv()
        over_cores(SHARE_PARTS, rep_here).start()
    for p in range(PIECES):
        part = pl.ds(shared + p * piece, piece)
        own_ref[:, part] = mm(rows, weight_ref[:, part])
    if shared:
        portion = shared // PIECES
        for p in range(PIECES):
            part = pl.ds(p * portion, portion)
            own_ref[:, part] = mm(rows, weight_ref[:, part])
        for j in range(SHARE_PARTS + 1):
            over_cores(j, 1 - rep_here).wait_recv()
        for h in range(heads):
            send_normed(h).wait_recv()
        for p in range(PIECES):
            part = pl.ds(p * portion, portion)
            peer = mm(rows_in[...], peer_ref[:, part])
            total = own_ref[:, part].astype(bf16).astype(f32) + peer.astype(bf16).astype(f32)
            out_ref[:, part] = total.astype(bf16)
    for p in range(PIECES):
        part = pl.ds(p * piece, piece)
        spot = pl.ds(shared + p * piece, piece)
        total = own_ref[:, spot].astype(bf16).astype(f32)
        for slot in range(len(others)):
            copies[slot * PIECES + p].wait_recv()
            total += part_in[slot, :, part].astype(f32)
        out_ref[:, spot] = total.astype(bf16)
    for copy in copies:
        copy.wait_send()
    if shared:
        for j in range(SHARE_PARTS):
            from_head(j).wait_send()
            over_parts(j, parts_here).wait_send()
        for j in range(SHARE_PARTS + 1):
            over_cores(j, rep_here).wait_send()
        for h in range(heads):
            send_normed(h).wait_send()

    @pl.when(first | ((seq_here > 1) & (last | (not direct))))
    def _():
        for h in range(heads):
            send_own(h).wait_recv()

    for h in range(heads):
        send_own(h).wait_send()

    @pl.when(inner)
    def _():
        for h in range(heads):
            send_full(h).wait_send()


def body(queries, reflect_keys, reflect_values, reflect_beta, log_decay, prompt_lengths, norm_gain, out_weight):
    tokens, refl, wide = reflect_keys.shape[1:]
    heads = log_decay.shape[2]
    width = wide // heads
    blocks = tokens // BLOCK
    sub = refl * BLOCK
    head_count = lax.axis_size("head")
    chunk, model = tokens // head_count, out_weight.shape[1]
    steps, slots = heads // HEADS_STEP, max(head_count - 1, 1)
    wide_step = HEADS_STEP * width
    shared = model * SHARE // 128 // 100 * 128 if sharing() else 0
    peer_shape = (out_weight.shape[0], shared) if shared else (32, 128)
    rest = model - shared
    beta, gate = reflect_beta[0].transpose(1, 2, 0), log_decay[0].T
    dma = pltpu.SemaphoreType.DMA
    anywhere, vmem = pl.BlockSpec(memory_space=pl.ANY), pl.BlockSpec(memory_space=pltpu.VMEM)
    out = pl.pallas_call(
        functools.partial(mixer_kernel, refl, blocks),
        in_specs=[
            pl.BlockSpec(memory_space=pltpu.SMEM),
            anywhere, anywhere, anywhere, anywhere, anywhere, vmem, anywhere,
        ],
        out_specs=vmem,
        out_shape=pltpu.VMEM((chunk, model), bf16),
        scratch_shapes=[
            pltpu.VMEM((steps, tokens, wide_step), bf16),
            pltpu.VMEM((steps, tokens, refl, wide_step), bf16),
            pltpu.VMEM((steps, tokens, refl, wide_step), bf16),
            pltpu.VMEM(beta.shape, f32),
            pltpu.VMEM(gate.shape, f32),
            dma((steps, 3)),
            pltpu.VMEM((blocks, 2, heads, sub), f32),
            pltpu.VMEM((blocks, heads, sub), f32),
            pltpu.VMEM((steps, tokens * refl, wide_step), bf16),
            pltpu.VMEM((heads, blocks, sub, 2 * width), bf16),
            pltpu.VMEM((heads, max(blocks - 1, 1), width, 2 * width), bf16),
            pltpu.VMEM((heads, tokens, width), f32),
            pltpu.VMEM((heads, tokens, width), bf16),
            pltpu.VMEM((heads, width, width), f32),
            pltpu.VMEM((heads, width, width), f32),
            pltpu.VMEM(out_weight.shape, bf16),
            dma((3,)),
            *[pltpu.VMEM((heads, width, width), bf16)] * 5,
            pltpu.VMEM((tokens, wide), bf16),
            pltpu.VMEM((chunk, model), f32),
            pltpu.VMEM((slots, chunk, rest), bf16),
            pltpu.VMEM((slots, chunk, rest), bf16),
            *[dma((heads,))] * 4, dma((slots, PIECES)), dma((slots, PIECES)),
            pltpu.VMEM(peer_shape, bf16),
            pltpu.VMEM((chunk, wide), bf16),
            dma((SHARE_PARTS,)), dma((SHARE_PARTS,)), dma((SHARE_PARTS,)), dma((SHARE_PARTS,)),
            dma((SHARE_PARTS + 1,)), dma((SHARE_PARTS + 1,)), dma((heads,)), dma((heads,)),
        ],
        compiler_params=pltpu.CompilerParams(
            collective_id=0, has_side_effects=True, vmem_limit_bytes=56 * 2**20
        ),
    )(
        prompt_lengths,
        queries[0],
        reflect_keys[0],
        reflect_values[0],
        beta,
        gate,
        norm_gain[None],
        out_weight,
    )
    return out[None]


def solution(mesh):
    in_specs = (
        P(("parts", "rep"), "seq", "head"),
        P(("parts", "rep"), "seq", None, "head"),
        P(("parts", "rep"), "seq", None, "head"),
        P(("parts", "rep"), "seq", None, "head"),
        P(("parts", "rep"), "seq", "head"),
        P(("parts", "rep"), None),
        P(),
        P("head", None),
    )
    out_specs = P(("parts", "rep"), ("seq", "head"), None)
    return jax.shard_map(body, mesh=mesh, in_specs=in_specs, out_specs=out_specs, check_vma=False)
```

```python
import functools

import jax
import jax.numpy as jnp
from jax import lax
from jax.experimental import pallas as pl
from jax.experimental.pallas import tpu as pltpu
from jax.sharding import PartitionSpec as P

BLOCK = 64
HEADS_STEP = 4
FINISH_GROUP = 2
PIECE = 256
SHARE = 63
SHARE_PARTS = 8
RELAYS = (1, 3, 5, 6, 7)
TEAM = 2
MESH = pl.DeviceIdType.MESH

epsilon = 1e-06
f32 = jnp.float32
bf16 = jnp.bfloat16
highest = lax.Precision.HIGHEST


def mm(a, b, precision=None):
    return jnp.dot(a, b, preferred_element_type=f32, precision=precision)


def mm_nt(a, b):
    return lax.dot_general(a, b, (((1,), (1,)), ((), ())), preferred_element_type=f32)


def mm_tn(a, b):
    return lax.dot_general(a, b, (((0,), (0,)), ((), ())), preferred_element_type=f32)


def split(x):
    hi = x.astype(bf16)
    return hi, (x - hi.astype(f32)).astype(bf16)


def split3(x):
    hi = x.astype(bf16).astype(f32)
    mid = (x - hi).astype(bf16).astype(f32)
    return [hi, mid, x - hi - mid]


def sub_rows(x, pattern, blocks):
    rows = x.shape[0]
    zero = jnp.zeros_like(pattern)
    table = jnp.concatenate(
        [jnp.concatenate([pattern if c == r else zero for c in range(blocks)], axis=1) for r in range(blocks)],
        axis=0,
    )
    got = mm(jnp.concatenate(split3(x), axis=0).astype(bf16), table)
    return got[:rows] + got[rows : 2 * rows] + got[2 * rows :]


def sharing():
    return all(lax.axis_size(name) == 2 for name in ("head", "parts", "rep"))


def mixer_kernel(
    refl, blocks, len_ref, q_hbm, k_hbm, v_hbm, beta_hbm, gate_hbm, gain_ref, weight_hbm, out_ref,
    q_ref, k_ref, v_ref, beta_ref, gate_ref, in_sem,
    rows_ref, scale_ref, kflat_ref, wrote_ref, prefix_ref, oloc_ref, read_ref, add_ref, map_ref,
    weight_ref, weight_sem, state_in, own_out, full_out, own_in, full_in, normed_ref, own_ref, part_out, part_in,
    own_send, own_recv, full_send, full_recv, part_send, part_recv,
    peer_ref, rows_in, x_send, x_recv, y_send, y_recv, core_send, core_recv, norm_send, norm_recv,
):
    heads, width = add_ref.shape[:2]
    steps = heads // HEADS_STEP
    wide = HEADS_STEP * width
    sub = refl * BLOCK
    tokens = blocks * BLOCK
    seq_count, head_count = lax.axis_size("seq"), lax.axis_size("head")
    seq_here, head_here = lax.axis_index("seq"), lax.axis_index("head")
    chunk = out_ref.shape[0]
    first, last = seq_here == 0, seq_here == seq_count - 1
    others = [lax.rem(head_here + d, head_count) for d in range(1, head_count)]
    shared = peer_ref.shape[1] if sharing() else 0
    parts_here, rep_here = lax.axis_index("parts"), lax.axis_index("rep")
    quarter = peer_ref.shape[0] // 4
    slab = quarter // SHARE_PARTS

    def slab_rows(rep, parts, j):
        return pl.ds(pl.multiple_of((rep * 2 + parts) * quarter + j * slab, slab), slab)

    def remote(src, dst, send, recv, device):
        return pltpu.make_async_remote_copy(
            src_ref=src, dst_ref=dst, send_sem=send, recv_sem=recv, device_id=device, device_id_type=MESH
        )

    def from_head(j):
        rows = slab_rows(rep_here, parts_here, j)
        return remote(
            weight_hbm.at[rows, pl.ds(0, shared)], peer_ref.at[rows],
            x_send.at[j], x_recv.at[j], {"head": 1 - head_here},
        )

    def over_parts(j, parts):
        rows = slab_rows(rep_here, parts, j)
        return remote(
            peer_ref.at[rows], peer_ref.at[rows], y_send.at[j], y_recv.at[j], {"parts": 1 - parts_here}
        )

    def over_cores(j, rep):
        parts = parts_here if j < SHARE_PARTS else 1 - parts_here
        rows = slab_rows(rep, parts, j % SHARE_PARTS)
        return remote(
            peer_ref.at[rows], peer_ref.at[rows], core_send.at[j], core_recv.at[j], {"rep": 1 - rep_here}
        )

    def relay(j):
        from_head(j).wait_recv()
        over_parts(j, parts_here).start()
        over_cores(j, rep_here).start()

    def send_normed(h):
        span = cols(h)
        rows = pl.ds(pl.multiple_of(others[0] * chunk, chunk), chunk)
        return remote(
            normed_ref.at[rows, span], rows_in.at[:, span],
            norm_send.at[h], norm_recv.at[h], {"head": 1 - head_here},
        )

    def load(s, kind):
        span = pl.ds(pl.multiple_of(s * wide, wide), wide)
        src, dst = [
            (k_hbm.at[:, :, span], k_ref), (v_hbm.at[:, :, span], v_ref), (q_hbm.at[:, span], q_ref)
        ][kind]
        return pltpu.make_async_copy(src, dst.at[s], in_sem.at[s, kind])

    load_beta = pltpu.make_async_copy(beta_hbm, beta_ref, weight_sem.at[1])
    load_gate = pltpu.make_async_copy(gate_hbm, gate_ref, weight_sem.at[2])
    load_weight = pltpu.make_async_copy(weight_hbm, weight_ref, weight_sem.at[0])
    load_gate.start()
    load_beta.start()
    for s in range(steps):
        load(s, 0).start()
        load(s, 1).start()
    for s in range(steps):
        load(s, 2).start()
    load_weight.start()

    barrier = pltpu.get_barrier_semaphore()

    @pl.when(seq_here > 0)
    def _():
        pl.semaphore_signal(barrier, inc=1, device_id={"seq": seq_here - 1}, device_id_type=MESH)

    @pl.when(seq_here < seq_count - 1)
    def _():
        pl.semaphore_signal(barrier, inc=1, device_id={"seq": seq_here + 1}, device_id_type=MESH)

    for other in others:
        pl.semaphore_signal(barrier, inc=1, device_id={"head": other}, device_id_type=MESH)
    if shared:
        pl.semaphore_signal(barrier, inc=1, device_id={"parts": 1 - parts_here}, device_id_type=MESH)
        pl.semaphore_signal(barrier, inc=1, device_id={"rep": 1 - rep_here}, device_id_type=MESH)

    offset = seq_here * tokens
    ends = []
    running = 0
    for d in range(len_ref.shape[1]):
        running = running + len_ref[0, d]
        ends.append(running)

    def segment(pos):
        total = jnp.zeros(pos.shape, jnp.int32)
        for end in ends:
            total += jnp.where(pos >= end, 1, 0)
        return total

    row_i = lax.broadcasted_iota(jnp.int32, (sub, sub), 0)
    col_i = lax.broadcasted_iota(jnp.int32, (sub, sub), 1)
    eye = row_i == col_i
    eye_f = jnp.where(eye, 1.0, 0.0).astype(f32)
    tok_i = lax.broadcasted_iota(jnp.int32, (BLOCK, sub), 0)
    tok_j = lax.broadcasted_iota(jnp.int32, (BLOCK, sub), 1)
    pick_tok = tok_j == tok_i * refl + refl - 1
    levels = []
    size = refl
    while size < sub:
        big = min(4 * size, sub)
        levels.append((row_i // big == col_i // big) & (row_i // size > col_i // size))
        size = big

    expected = jnp.where(first, 0, 1) + jnp.where(last, 0, 1) + head_count - 1 + (2 if shared else 0)
    pl.semaphore_wait(barrier, expected)
    if shared:
        for j in range(SHARE_PARTS):
            from_head(j).start()

    load_gate.wait()
    load_beta.wait()
    table = sub_rows(gate_ref[...], jnp.where(tok_i <= tok_j // refl, 1.0, 0.0).astype(bf16), blocks)
    total = 0.0
    for j in range(refl):
        pick = jnp.where(tok_i * refl + j == tok_j, 1.0, 0.0).astype(bf16)
        total += sub_rows(beta_ref[j], pick, blocks)
    for b in range(blocks):
        rows_ref[b, 0] = table[:, b * sub : (b + 1) * sub]
        rows_ref[b, 1] = total[:, b * sub : (b + 1) * sub]

    def geometry(b):
        start = offset + b * BLOCK
        seg_row = segment(start + lax.broadcasted_iota(jnp.int32, (1, sub), 1) // refl)
        before = jnp.where(start == 0, -1, 0)
        last_seg = 0
        for end in ends:
            before += jnp.where(start - 1 >= end, 1, 0)
            last_seg += jnp.where(start + BLOCK - 1 >= end, 1, 0)
        return start, seg_row, before, last_seg

    pairs = [(h, b) for h in range(HEADS_STEP) for b in range(blocks)]

    def over(stage, *lists):
        return [stage(h, b, *args) for (h, b), *args in zip(pairs, *lists)]

    def cols(h):
        return slice(h * width, (h + 1) * width)

    def toks(b):
        return slice(b * BLOCK, (b + 1) * BLOCK)

    def column(values):
        return jnp.sum(jnp.where(eye, values, 0.0), axis=1, keepdims=True)

    reach = (seq_count * tokens // 2 - 2) // tokens
    direct = reach <= 1
    inner = (seq_here > 0) & (seq_here < seq_count - 1)
    following = {"seq": lax.rem(seq_here + 1, seq_count)}
    beside = {"seq": jnp.where(last, seq_count - 2, seq_here + 1)}
    spare = jnp.where(last, heads, 0)

    def send_own(h):
        return remote(own_out.at[h], own_in.at[h + spare], own_send.at[h], own_recv.at[h + spare], beside)

    def take_own(h):
        return remote(own_out.at[h], own_in.at[h], own_send.at[h], own_recv.at[h], following)

    def take_spare(h):
        return remote(own_out.at[h], own_in.at[heads + h], own_send.at[h], own_recv.at[heads + h], following)

    def send_full(h):
        return remote(full_out.at[h], full_in.at[h], full_send.at[h], full_recv.at[h], following)

    def pass_on(h, state):
        both = jnp.concatenate(split(map_ref[h]), axis=1)
        grown = add_ref[h] + mm(both, jnp.concatenate([state, state], axis=0))
        full_out[h] = grown.astype(bf16)
        send_full(h).start()

    def forward(h):
        if direct:
            take_own(h).wait_recv()
            pass_on(h, own_in[h])
        else:
            @pl.when(seq_here == 1)
            def _():
                take_own(h).wait_recv()
                pass_on(h, own_in[h])

            @pl.when(seq_here > 1)
            def _():
                send_full(h).wait_recv()
                pass_on(h, full_in[h])

    def near(s, b):
        def keys(h):
            return kflat_ref[s, b * sub : (b + 1) * sub, cols(h)]

        def row(kind, h):
            return rows_ref[b, kind, pl.ds(s * HEADS_STEP + h, 1), :]

        return keys, row

    def states_step(s, carry):
        load(s, 0).wait()
        load(s, 1).wait()
        keys = lambda h, b: near(s, b)[0](h)
        row = lambda kind, h, b: near(s, b)[1](kind, h)
        geo = []
        for b in range(blocks):
            start, seg_row, before, last_seg = geometry(b)
            seg_col = segment(start + lax.broadcasted_iota(jnp.int32, (sub, 1), 0) // refl)
            incl = (row_i >= col_i) & (seg_col == seg_row)
            geo.append((incl, seg_row == before, seg_col == last_seg, last_seg == before))

        for h, b in pairs:
            kflat_ref[s, b * sub : (b + 1) * sub, cols(h)] = k_ref[s, toks(b), :, cols(h)].reshape(sub, width)

        def scales(h, b):
            gram = mm_nt(keys(h, b), keys(h, b))
            diag = jnp.where(eye, gram, 0.0)
            n_row = lax.rsqrt(jnp.sum(diag, axis=0, keepdims=True) + epsilon)
            n_col = lax.rsqrt(jnp.sum(diag, axis=1, keepdims=True) + epsilon)
            scale_ref[b, pl.ds(s * HEADS_STEP + h, 1), :] = n_row
            c_row = row(0, h, b)
            c_col = column(c_row)
            ratio = jnp.where(geo[b][0], jnp.exp(jnp.minimum(c_col - c_row, 0.0)), 0.0)
            low = jnp.where(eye, 0.0, (column(row(1, h, b)) * n_col) * ratio * gram * n_row)
            return low, n_row, n_col, c_col

        lows, n_rows, n_cols, c_cols = zip(*over(scales))
        invs = [eye_f - jnp.where(row_i // refl == col_i // refl, low, 0.0) for low in lows]
        for mask in levels:
            heads_b = [inv.astype(bf16) for inv in invs]
            nils = [
                mm(inv, jnp.where(mask, low, 0.0).astype(bf16)).astype(bf16)
                for inv, low in zip(heads_b, lows)
            ]
            both = [mm(nil, jnp.concatenate([nil, inv], axis=1)) for nil, inv in zip(nils, heads_b)]
            halves = [inv - pair[:, sub:] for inv, pair in zip(invs, both)]
            invs = [
                half + mm(pair[:, :sub].astype(bf16), half.astype(bf16))
                for half, pair in zip(halves, both)
            ]

        if shared:
            @pl.when(s > 0)
            def _():
                for j in range(RELAYS[0], RELAYS[1]):
                    relay(j)

        @pl.when((s > 0) & inner & (direct | (seq_here == 1)))
        def _():
            for h in range(HEADS_STEP):
                forward((s - 1) * HEADS_STEP + h)

        def residual(h, b, inv, low):
            inv_b = inv.astype(bf16)
            low_2 = jnp.concatenate(split(low), axis=1)
            return eye_f - inv_b.astype(f32) - mm(low_2, jnp.concatenate([inv_b, inv_b], axis=0))

        def refine(h, b, inv, resid):
            inv_b = inv.astype(bf16)
            return inv_b.astype(f32) + mm(inv_b, resid.astype(bf16))

        def write(h, b, inv, n_row):
            carry_row = jnp.where(geo[b][1], jnp.exp(row(0, h, b)), 0.0)
            by_beta = inv * row(1, h, b)
            tv = jnp.concatenate(split(by_beta), axis=1)
            tk = jnp.concatenate(split(by_beta * (carry_row * n_row)), axis=1)
            vb, kb = v_ref[s, toks(b), :, cols(h)].reshape(sub, width), keys(h, b)
            return jnp.concatenate(
                [mm(tv, jnp.concatenate([vb, vb], axis=0)), mm(tk, jnp.concatenate([kb, kb], axis=0))],
                axis=1,
            )

        def block_step(h, b, wrote, n_col, c_col):
            wrote_ref[s * HEADS_STEP + h, b] = wrote.astype(bf16)
            c_end = row(0, h, b)[:, sub - 1 : sub]
            e_col = jnp.where(geo[b][2], jnp.exp(jnp.minimum(c_end - c_col, 0.0)), 0.0) * n_col
            kb = keys(h, b)
            moved = mm_tn(
                jnp.concatenate([kb, kb], axis=0), jnp.concatenate(split(wrote * e_col), axis=0)
            )
            carry_end = jnp.where(geo[b][3], jnp.exp(c_end), 0.0)
            return moved[:, :width], carry_end * eye_f - moved[:, width:]

        made, states = {}, {}

        def some(heads_now, stage, *lists):
            return {(h, b): stage(h, b, *[l[h, b] for l in lists]) for h in heads_now for b in range(blocks)}

        def scan(heads_now, b):
            for h in heads_now:
                if b == 0:
                    states[h] = jnp.concatenate(made[h, 0], axis=1)
                    continue
                block_add, block_map = made[h, b]
                s_hi = states[h].astype(bf16)
                prefix_ref[s * HEADS_STEP + h, b - 1] = s_hi
                grown = mm(
                    jnp.concatenate(split(block_map), axis=1), jnp.concatenate([s_hi, s_hi], axis=0)
                )
                states[h] = jnp.concatenate([grown[:, :width] + block_add, grown[:, width:]], axis=1)

        def finish(heads_now):
            for h in heads_now:
                at = s * HEADS_STEP + h
                own_out[at] = states[h][:, :width].astype(bf16)
                send_own(at).start()
                add_ref[at] = states[h][:, :width]
                map_ref[at] = states[h][:, width:]

        named = lambda values: dict(zip(pairs, values))
        lows, invs, n_rows, n_cols, c_cols = map(named, (lows, invs, n_rows, n_cols, c_cols))
        teams = [list(range(h, min(h + TEAM, HEADS_STEP))) for h in range(0, HEADS_STEP, TEAM)]
        pending = []

        def catch_up(count):
            for _ in range(count):
                if pending:
                    pending.pop(0)()

        for team in teams:
            resids = some(team, residual, invs, lows)
            catch_up(2)
            better = some(team, refine, invs, resids)
            catch_up(1)
            writes = some(team, write, better, n_rows)
            catch_up(1)
            made.update(some(team, block_step, writes, n_cols, c_cols))
            catch_up(len(pending))
            pending = [functools.partial(scan, team, b) for b in range(blocks)]
            pending.append(functools.partial(finish, team))
        catch_up(len(pending))

        if shared:
            @pl.when(s == 0)
            def _():
                for j in range(RELAYS[0]):
                    relay(j)

        return carry

    lax.fori_loop(0, steps, states_step, 0)
    relayed = RELAYS[1] if steps > 1 else RELAYS[0]
    if shared:
        while relayed < RELAYS[2]:
            relay(relayed)
            relayed += 1

    @pl.when(first)
    def _():
        state_in[...] = jnp.zeros_like(state_in)

    done = (steps - 1) * HEADS_STEP
    if done and not direct:
        @pl.when(inner & (seq_here > 1))
        def _():
            for h in range(done):
                forward(h)

    def reads_step(s, carry):
        load(s, 2).wait()
        geo = []
        for b in range(blocks):
            start, seg_row, before, _ = geometry(b)
            seg_tok = segment(start + lax.broadcasted_iota(jnp.int32, (BLOCK, 1), 0))
            geo.append(((tok_j // refl <= tok_i) & (seg_tok == seg_row), seg_tok == before))

        def read_weights(h, b):
            keys, row = near(s, b)
            qb, c_row = q_ref[s, toks(b), cols(h)], row(0, h)
            n_row = scale_ref[b, pl.ds(s * HEADS_STEP + h, 1), :]
            qf = qb.astype(f32)
            nq = lax.rsqrt(jnp.sum(qf * qf, axis=1, keepdims=True) + epsilon) * width ** (-0.5)
            ct = jnp.sum(jnp.where(pick_tok, c_row, 0.0), axis=1, keepdims=True)
            ratio = jnp.where(geo[b][0], jnp.exp(jnp.minimum(ct - c_row, 0.0)), 0.0)
            carried = (jnp.where(geo[b][1], jnp.exp(ct), 0.0) * nq) * qf
            return (ratio * mm_nt(qb, keys(h)) * nq * n_row).astype(bf16), carried

        weights = over(read_weights)

        def read(h, b, weight):
            got = mm(weight[0], wrote_ref[s * HEADS_STEP + h, b])
            return got[:, :width], (weight[1] - got[:, width:]).astype(bf16)

        for (h, b), (own, back) in zip(pairs, over(read, weights)):
            if b:
                moved = mm(back, prefix_ref[s * HEADS_STEP + h, b - 1])
                own, back = own + moved[:, :width], moved[:, width:].astype(bf16)
            oloc_ref[s * HEADS_STEP + h, toks(b), :] = own
            read_ref[s * HEADS_STEP + h, toks(b), :] = back
        return carry

    lax.fori_loop(0, steps, reads_step, 0)
    if shared:
        while relayed < RELAYS[3]:
            relay(relayed)
            relayed += 1

    @pl.when(inner)
    def _():
        for h in range(done, heads):
            forward(h)

    if shared:
        while relayed < RELAYS[4]:
            relay(relayed)
            relayed += 1

    for g in range(0, heads, FINISH_GROUP):
        if shared and g >= done:
            while relayed < SHARE_PARTS:
                relay(relayed)
                relayed += 1
        group = range(g, min(g + FINISH_GROUP, heads))

        for h in group:
            @pl.when(last & (seq_here == 1))
            def _():
                take_own(h).wait_recv()

            @pl.when((seq_here > 1) & (direct | last))
            def _():
                send_full(h).wait_recv()

            @pl.when(seq_here == 1)
            def _():
                state_in[h] = own_in[h]

            @pl.when(seq_here > 1)
            def _():
                state_in[h] = full_in[h]

        for h in group:
            out = oloc_ref[h] + mm(read_ref[h], state_in[h])
            scale = lax.rsqrt(jnp.mean(out * out, axis=-1, keepdims=True) + epsilon)
            normed_ref[:, cols(h)] = (out * scale * gain_ref[...]).astype(bf16)

        if shared:
            for h in group:
                send_normed(h).start()

    load_weight.wait()
    piece, pieces = PIECE, (weight_ref.shape[1] - shared) // PIECE
    copies = []
    for slot, other in enumerate(others):
        rows = normed_ref[pl.ds(pl.multiple_of(other * chunk, chunk), chunk), :]
        for p in range(pieces):
            part = pl.ds(p * piece, piece)
            part_out[slot, :, part] = mm(rows, weight_ref[:, pl.ds(shared + p * piece, piece)]).astype(bf16)
            copies.append(
                pltpu.make_async_remote_copy(
                    src_ref=part_out.at[slot, :, part],
                    dst_ref=part_in.at[slot, :, part],
                    send_sem=part_send.at[slot, p],
                    recv_sem=part_recv.at[slot, p],
                    device_id={"head": other},
                    device_id_type=MESH,
                )
            )
            copies[-1].start()
    rows = normed_ref[pl.ds(pl.multiple_of(head_here * chunk, chunk), chunk), :]
    if shared:
        for j in range(SHARE_PARTS):
            over_parts(j, 1 - parts_here).wait_recv()
            over_cores(SHARE_PARTS + j, rep_here).start()
    for p in range(pieces):
        part = pl.ds(shared + p * piece, piece)
        own_ref[:, part] = mm(rows, weight_ref[:, part])
    if shared:
        for p in range(shared // piece):
            part = pl.ds(p * piece, piece)
            own_ref[:, part] = mm(rows, weight_ref[:, part])
        for j in range(2 * SHARE_PARTS):
            over_cores(j, 1 - rep_here).wait_recv()
        for h in range(heads):
            send_normed(h).wait_recv()
        for p in range(shared // piece):
            part = pl.ds(p * piece, piece)
            peer = mm(rows_in[...], peer_ref[:, part])
            total = own_ref[:, part].astype(bf16).astype(f32) + peer.astype(bf16).astype(f32)
            out_ref[:, part] = total.astype(bf16)
    for p in range(pieces):
        part = pl.ds(p * piece, piece)
        spot = pl.ds(shared + p * piece, piece)
        total = own_ref[:, spot].astype(bf16).astype(f32)
        for slot in range(len(others)):
            copies[slot * pieces + p].wait_recv()
            total += part_in[slot, :, part].astype(f32)
        out_ref[:, spot] = total.astype(bf16)
    for copy in copies:
        copy.wait_send()
    if shared:
        for j in range(SHARE_PARTS):
            from_head(j).wait_send()
            over_parts(j, parts_here).wait_send()
        for j in range(2 * SHARE_PARTS):
            over_cores(j, rep_here).wait_send()
        for h in range(heads):
            send_normed(h).wait_send()

    @pl.when((seq_here > 1) & (last | (not direct)))
    def _():
        for h in range(heads):
            take_own(h).wait_recv()

    @pl.when(seq_here == seq_count - 2)
    def _():
        for h in range(heads):
            take_spare(h).wait_recv()

    for h in range(heads):
        send_own(h).wait_send()

    @pl.when(inner)
    def _():
        for h in range(heads):
            send_full(h).wait_send()


def body(queries, reflect_keys, reflect_values, reflect_beta, log_decay, prompt_lengths, norm_gain, out_weight):
    tokens, refl, wide = reflect_keys.shape[1:]
    heads = log_decay.shape[2]
    width = wide // heads
    blocks = tokens // BLOCK
    sub = refl * BLOCK
    head_count = lax.axis_size("head")
    chunk, model = tokens // head_count, out_weight.shape[1]
    steps, slots = heads // HEADS_STEP, max(head_count - 1, 1)
    wide_step = HEADS_STEP * width
    shared = model * SHARE // PIECE // 100 * PIECE if sharing() else 0
    peer_shape = (out_weight.shape[0], shared) if shared else (32, 128)
    rest = model - shared
    pieces = rest // PIECE
    beta, gate = reflect_beta[0].transpose(1, 2, 0), log_decay[0].T
    dma = pltpu.SemaphoreType.DMA
    anywhere, vmem = pl.BlockSpec(memory_space=pl.ANY), pl.BlockSpec(memory_space=pltpu.VMEM)
    out = pl.pallas_call(
        functools.partial(mixer_kernel, refl, blocks),
        in_specs=[
            pl.BlockSpec(memory_space=pltpu.SMEM),
            anywhere, anywhere, anywhere, anywhere, anywhere, vmem, anywhere,
        ],
        out_specs=vmem,
        out_shape=pltpu.VMEM((chunk, model), bf16),
        scratch_shapes=[
            pltpu.VMEM((steps, tokens, wide_step), bf16),
            pltpu.VMEM((steps, tokens, refl, wide_step), bf16),
            pltpu.VMEM((steps, tokens, refl, wide_step), bf16),
            pltpu.VMEM(beta.shape, f32),
            pltpu.VMEM(gate.shape, f32),
            dma((steps, 3)),
            pltpu.VMEM((blocks, 2, heads, sub), f32),
            pltpu.VMEM((blocks, heads, sub), f32),
            pltpu.VMEM((steps, tokens * refl, wide_step), bf16),
            pltpu.VMEM((heads, blocks, sub, 2 * width), bf16),
            pltpu.VMEM((heads, max(blocks - 1, 1), width, 2 * width), bf16),
            pltpu.VMEM((heads, tokens, width), f32),
            pltpu.VMEM((heads, tokens, width), bf16),
            pltpu.VMEM((heads, width, width), f32),
            pltpu.VMEM((heads, width, width), f32),
            pltpu.VMEM(out_weight.shape, bf16),
            dma((3,)),
            *[pltpu.VMEM((heads, width, width), bf16)] * 3,
            pltpu.VMEM((2 * heads, width, width), bf16),
            pltpu.VMEM((heads, width, width), bf16),
            pltpu.VMEM((tokens, wide), bf16),
            pltpu.VMEM((chunk, model), f32),
            pltpu.VMEM((slots, chunk, rest), bf16),
            pltpu.VMEM((slots, chunk, rest), bf16),
            dma((heads,)), dma((2 * heads,)), dma((heads,)), dma((heads,)), dma((slots, pieces)), dma((slots, pieces)),
            pltpu.VMEM(peer_shape, bf16),
            pltpu.VMEM((chunk, wide), bf16),
            dma((SHARE_PARTS,)), dma((SHARE_PARTS,)), dma((SHARE_PARTS,)), dma((SHARE_PARTS,)),
            dma((2 * SHARE_PARTS,)), dma((2 * SHARE_PARTS,)), dma((heads,)), dma((heads,)),
        ],
        compiler_params=pltpu.CompilerParams(
            collective_id=0, has_side_effects=True, vmem_limit_bytes=56 * 2**20
        ),
    )(
        prompt_lengths,
        queries[0],
        reflect_keys[0],
        reflect_values[0],
        beta,
        gate,
        norm_gain[None],
        out_weight,
    )
    return out[None]


def solution(mesh):
    in_specs = (
        P(("parts", "rep"), "seq", "head"),
        P(("parts", "rep"), "seq", None, "head"),
        P(("parts", "rep"), "seq", None, "head"),
        P(("parts", "rep"), "seq", None, "head"),
        P(("parts", "rep"), "seq", "head"),
        P(("parts", "rep"), None),
        P(),
        P("head", None),
    )
    out_specs = P(("parts", "rep"), ("seq", "head"), None)
    return jax.shard_map(body, mesh=mesh, in_specs=in_specs, out_specs=out_specs, check_vma=False)
```

```python
import functools
import math

import jax
import jax.numpy as jnp
from jax import lax
from jax.experimental import pallas as pl
from jax.experimental.pallas import tpu as pltpu
from jax.sharding import PartitionSpec as P

BLOCK = 64
HEADS_STEP = 4
FINISH_GROUP = 2
PIECE = 256
SHARE = 63
SHARE_PARTS = 8
RELAYS = (1, 3, 5, 6, 7)
TEAM = 2
MESH = pl.DeviceIdType.MESH

epsilon = 1e-06
f32 = jnp.float32
bf16 = jnp.bfloat16
highest = lax.Precision.HIGHEST


def mm(a, b, precision=None):
    return jnp.dot(a, b, preferred_element_type=f32, precision=precision)


def mm_nt(a, b):
    return lax.dot_general(a, b, (((1,), (1,)), ((), ())), preferred_element_type=f32)


def mm_tn(a, b):
    return lax.dot_general(a, b, (((0,), (0,)), ((), ())), preferred_element_type=f32)


def split(x):
    hi = x.astype(bf16)
    return hi, (x - hi.astype(f32)).astype(bf16)


def split3(x):
    hi = x.astype(bf16).astype(f32)
    mid = (x - hi).astype(bf16).astype(f32)
    return [hi, mid, x - hi - mid]


def sub_rows(x, pattern, blocks):
    rows = x.shape[0]
    zero = jnp.zeros_like(pattern)
    table = jnp.concatenate(
        [jnp.concatenate([pattern if c == r else zero for c in range(blocks)], axis=1) for r in range(blocks)],
        axis=0,
    )
    got = mm(jnp.concatenate(split3(x), axis=0).astype(bf16), table)
    return got[:rows] + got[rows : 2 * rows] + got[2 * rows :]


def sharing():
    return all(lax.axis_size(name) == 2 for name in ("head", "parts", "rep"))


def mixer_kernel(
    refl, blocks, len_hbm, q_hbm, k_hbm, v_hbm, beta_hbm, gate_hbm, gain_hbm, weight_hbm, out_ref,
    len_ref, q_ref, k_ref, v_ref, beta_ref, gate_ref, gain_ref, in_sem, ready_sem,
    rows_ref, scale_ref, kflat_ref, wrote_ref, prefix_ref, oloc_ref, read_ref, add_ref, map_ref,
    weight_ref, weight_sem, state_in, own_out, full_out, own_in, full_in, normed_ref, own_ref, part_out, part_in,
    own_send, own_recv, full_send, full_recv, part_send, part_recv,
    peer_ref, rows_in, x_send, x_recv, y_send, y_recv, core_send, core_recv, norm_send, norm_recv,
):
    heads, width = add_ref.shape[:2]
    steps = heads // HEADS_STEP
    wide = HEADS_STEP * width
    sub = refl * BLOCK
    tokens = blocks * BLOCK
    seq_count, head_count = lax.axis_size("seq"), lax.axis_size("head")
    seq_here, head_here = lax.axis_index("seq"), lax.axis_index("head")
    chunk = out_ref.shape[0]
    first, last = seq_here == 0, seq_here == seq_count - 1
    others = [lax.rem(head_here + d, head_count) for d in range(1, head_count)]
    shared = peer_ref.shape[1] if sharing() else 0
    parts_here, rep_here = lax.axis_index("parts"), lax.axis_index("rep")
    quarter = peer_ref.shape[0] // 4
    slab = quarter // SHARE_PARTS

    def slab_rows(rep, parts, j):
        return pl.ds(pl.multiple_of((rep * 2 + parts) * quarter + j * slab, slab), slab)

    def remote(src, dst, send, recv, device):
        return pltpu.make_async_remote_copy(
            src_ref=src, dst_ref=dst, send_sem=send, recv_sem=recv, device_id=device, device_id_type=MESH
        )

    def from_head(j):
        rows = slab_rows(rep_here, parts_here, j)
        return remote(
            weight_hbm.at[rows, pl.ds(0, shared)], peer_ref.at[rows],
            x_send.at[j], x_recv.at[j], {"head": 1 - head_here},
        )

    def over_parts(j, parts):
        rows = slab_rows(rep_here, parts, j)
        return remote(
            peer_ref.at[rows], peer_ref.at[rows], y_send.at[j], y_recv.at[j], {"parts": 1 - parts_here}
        )

    def over_cores(j, rep):
        parts = parts_here if j < SHARE_PARTS else 1 - parts_here
        rows = slab_rows(rep, parts, j % SHARE_PARTS)
        return remote(
            peer_ref.at[rows], peer_ref.at[rows], core_send.at[j], core_recv.at[j], {"rep": 1 - rep_here}
        )

    def relay(j):
        from_head(j).wait_recv()
        over_parts(j, parts_here).start()
        over_cores(j, rep_here).start()

    def send_normed(h):
        span = cols(h)
        rows = pl.ds(pl.multiple_of(others[0] * chunk, chunk), chunk)
        return remote(
            normed_ref.at[rows, span], rows_in.at[:, span],
            norm_send.at[h], norm_recv.at[h], {"head": 1 - head_here},
        )

    barrier = pltpu.get_barrier_semaphore()

    @pl.when(seq_here < seq_count - 1)
    def _():
        pl.semaphore_signal(barrier, inc=1, device_id={"seq": seq_here + 1}, device_id_type=MESH)

    for other in others:
        pl.semaphore_signal(barrier, inc=1, device_id={"head": other}, device_id_type=MESH)
    if shared:
        pl.semaphore_signal(barrier, inc=1, device_id={"parts": 1 - parts_here}, device_id_type=MESH)
        pl.semaphore_signal(barrier, inc=1, device_id={"rep": 1 - rep_here}, device_id_type=MESH)

    def load(s, kind):
        span = pl.ds(pl.multiple_of(s * wide, wide), wide)
        src, dst = [
            (k_hbm.at[:, :, span], k_ref), (v_hbm.at[:, :, span], v_ref), (q_hbm.at[:, span], q_ref)
        ][kind]
        return pltpu.make_async_copy(src, dst.at[s], in_sem.at[s, kind])

    load_beta = pltpu.make_async_copy(beta_hbm, beta_ref, weight_sem.at[1])
    load_gate = pltpu.make_async_copy(gate_hbm, gate_ref, weight_sem.at[2])
    load_weight = pltpu.make_async_copy(weight_hbm, weight_ref, weight_sem.at[0])
    load_len = pltpu.make_async_copy(len_hbm, len_ref, weight_sem.at[3])
    load_gain = pltpu.make_async_copy(gain_hbm, gain_ref, weight_sem.at[4])
    load_len.start()
    load_gate.start()
    load_beta.start()
    for s in range(steps):
        load(s, 0).start()
        load(s, 1).start()
    for s in range(steps):
        load(s, 2).start()
    load_gain.start()
    load_weight.start()
    pl.semaphore_wait(barrier, jnp.where(first, 0, 1) + head_count - 1 + (2 if shared else 0))
    if shared:
        for j in range(SHARE_PARTS):
            from_head(j).start()

    @pl.when(seq_here > 0)
    def _():
        pl.semaphore_signal(ready_sem, inc=1, device_id={"seq": seq_here - 1}, device_id_type=MESH)

    load_len.wait()

    offset = seq_here * tokens
    ends = []
    running = 0
    for d in range(len_ref.shape[1]):
        running = running + len_ref[0, d]
        ends.append(running)

    def segment(pos):
        total = jnp.zeros(pos.shape, jnp.int32)
        for end in ends:
            total += jnp.where(pos >= end, 1, 0)
        return total

    row_i = lax.broadcasted_iota(jnp.int32, (sub, sub), 0)
    col_i = lax.broadcasted_iota(jnp.int32, (sub, sub), 1)
    eye = row_i == col_i
    eye_f = jnp.where(eye, 1.0, 0.0).astype(f32)
    tok_i = lax.broadcasted_iota(jnp.int32, (BLOCK, sub), 0)
    tok_j = lax.broadcasted_iota(jnp.int32, (BLOCK, sub), 1)
    pick_tok = tok_j == tok_i * refl + refl - 1
    levels = []
    size = refl
    while size < sub:
        big = min(4 * size, sub)
        levels.append((row_i // big == col_i // big) & (row_i // size > col_i // size))
        size = big

    load_gate.wait()
    load_beta.wait()
    table = sub_rows(gate_ref[...], jnp.where(tok_i <= tok_j // refl, 1.0, 0.0).astype(bf16), blocks)
    total = 0.0
    for j in range(refl):
        pick = jnp.where(tok_i * refl + j == tok_j, 1.0, 0.0).astype(bf16)
        total += sub_rows(beta_ref[j], pick, blocks)
    for b in range(blocks):
        rows_ref[b, 0] = table[:, b * sub : (b + 1) * sub] * math.log2(math.e)
        rows_ref[b, 1] = total[:, b * sub : (b + 1) * sub]
        rows_ref[b, 2] = rows_ref[b, 0] + jnp.log2(rows_ref[b, 1])

    def geometry(b):
        start = offset + b * BLOCK
        seg_row = segment(start + lax.broadcasted_iota(jnp.int32, (1, sub), 1) // refl)
        before = jnp.where(start == 0, -1, 0)
        last_seg = 0
        for end in ends:
            before += jnp.where(start - 1 >= end, 1, 0)
            last_seg += jnp.where(start + BLOCK - 1 >= end, 1, 0)
        return start, seg_row, before, last_seg

    pairs = [(h, b) for h in range(HEADS_STEP) for b in range(blocks)]

    def over(stage, *lists):
        return [stage(h, b, *args) for (h, b), *args in zip(pairs, *lists)]

    def cols(h):
        return slice(h * width, (h + 1) * width)

    def toks(b):
        return slice(b * BLOCK, (b + 1) * BLOCK)

    def column(values):
        return jnp.sum(jnp.where(eye, values, 0.0), axis=1, keepdims=True)

    reach = (seq_count * tokens // 2 - 2) // tokens
    direct = reach <= 1
    inner = (seq_here > 0) & (seq_here < seq_count - 1)
    following = {"seq": lax.rem(seq_here + 1, seq_count)}
    beside = {"seq": jnp.where(last, seq_count - 2, seq_here + 1)}
    spare = jnp.where(last, heads, 0)

    def send_own(h):
        return remote(own_out.at[h], own_in.at[h + spare], own_send.at[h], own_recv.at[h + spare], beside)

    def take_own(h):
        return remote(own_out.at[h], own_in.at[h], own_send.at[h], own_recv.at[h], following)

    def take_spare(h):
        return remote(own_out.at[h], own_in.at[heads + h], own_send.at[h], own_recv.at[heads + h], following)

    def send_full(h):
        return remote(full_out.at[h], full_in.at[h], full_send.at[h], full_recv.at[h], following)

    def pass_on(h, state):
        both = jnp.concatenate(split(map_ref[h]), axis=1)
        grown = add_ref[h] + mm(both, jnp.concatenate([state, state], axis=0))
        full_out[h] = grown.astype(bf16)
        send_full(h).start()

    def forward(h):
        if direct:
            take_own(h).wait_recv()
            pass_on(h, own_in[h])
        else:
            @pl.when(seq_here == 1)
            def _():
                take_own(h).wait_recv()
                pass_on(h, own_in[h])

            @pl.when(seq_here > 1)
            def _():
                send_full(h).wait_recv()
                pass_on(h, full_in[h])

    def near(s, b):
        def keys(h):
            return kflat_ref[s, b * sub : (b + 1) * sub, cols(h)]

        def row(kind, h):
            return rows_ref[b, kind, pl.ds(s * HEADS_STEP + h, 1), :]

        return keys, row

    def states_step(s, carry):
        load(s, 0).wait()
        load(s, 1).wait()
        keys = lambda h, b: near(s, b)[0](h)
        row = lambda kind, h, b: near(s, b)[1](kind, h)
        geo = []
        for b in range(blocks):
            start, seg_row, before, last_seg = geometry(b)
            seg_col = segment(start + lax.broadcasted_iota(jnp.int32, (sub, 1), 0) // refl)
            incl = (row_i > col_i) & (seg_col == seg_row)
            geo.append((incl, seg_row == before, seg_row == last_seg, last_seg == before))

        for h, b in pairs:
            kflat_ref[s, b * sub : (b + 1) * sub, cols(h)] = k_ref[s, toks(b), :, cols(h)].reshape(sub, width)

        def scales(h, b):
            gram = mm_nt(keys(h, b), keys(h, b))
            square = jnp.sum(jnp.where(eye, gram, 0.0), axis=0, keepdims=True) + epsilon
            n_log, n_row = -0.5 * jnp.log2(square), lax.rsqrt(square)
            scale_ref[b, pl.ds(s * HEADS_STEP + h, 1), :] = n_row
            factor = jnp.exp2(column(row(2, h, b) + n_log) + (n_log - row(0, h, b)))
            return jnp.where(geo[b][0], factor * gram, 0.0), n_row

        lows, n_rows = zip(*over(scales))
        invs = [eye_f - jnp.where(row_i // refl == col_i // refl, low, 0.0) for low in lows]
        for mask in levels:
            heads_b = [inv.astype(bf16) for inv in invs]
            nils = [
                mm(inv, jnp.where(mask, low, 0.0).astype(bf16)).astype(bf16)
                for inv, low in zip(heads_b, lows)
            ]
            both = [mm(nil, jnp.concatenate([nil, inv], axis=1)) for nil, inv in zip(nils, heads_b)]
            halves = [inv - pair[:, sub:] for inv, pair in zip(invs, both)]
            invs = [
                half + mm(pair[:, :sub].astype(bf16), half.astype(bf16))
                for half, pair in zip(halves, both)
            ]

        if shared:
            @pl.when(s > 0)
            def _():
                for j in range(RELAYS[0], RELAYS[1]):
                    relay(j)

        @pl.when((s == 0) & (seq_here < seq_count - 1))
        def _():
            pl.semaphore_wait(ready_sem, 1)

        @pl.when((s > 0) & inner & (direct | (seq_here == 1)))
        def _():
            for h in range(HEADS_STEP):
                forward((s - 1) * HEADS_STEP + h)

        def residual(h, b, inv, low):
            inv_b = inv.astype(bf16)
            low_2 = jnp.concatenate(split(low), axis=1)
            return eye_f - inv_b.astype(f32) - mm(low_2, jnp.concatenate([inv_b, inv_b], axis=0))

        def refine(h, b, inv, resid):
            inv_b = inv.astype(bf16)
            return inv_b.astype(f32) + mm(inv_b, resid.astype(bf16))

        def write(h, b, inv, n_row):
            carry_row = jnp.where(geo[b][1], jnp.exp2(row(0, h, b)), 0.0)
            by_beta = inv * row(1, h, b)
            tv = jnp.concatenate(split(by_beta), axis=1)
            tk = jnp.concatenate(split(by_beta * (carry_row * n_row)), axis=1)
            vb, kb = v_ref[s, toks(b), :, cols(h)].reshape(sub, width), keys(h, b)
            return jnp.concatenate(
                [mm(tv, jnp.concatenate([vb, vb], axis=0)), mm(tk, jnp.concatenate([kb, kb], axis=0))],
                axis=1,
            )

        def block_step(h, b, wrote, n_row):
            wrote_ref[s * HEADS_STEP + h, b] = wrote.astype(bf16)
            c_row = row(0, h, b)
            c_end = c_row[:, sub - 1 : sub]
            e_row = jnp.where(geo[b][2], jnp.exp2(jnp.minimum(c_end - c_row, 0.0)), 0.0) * n_row
            kb = keys(h, b)
            moved = mm_tn(
                jnp.concatenate([kb, kb], axis=0), jnp.concatenate(split(wrote * column(e_row)), axis=0)
            )
            carry_end = jnp.where(geo[b][3], jnp.exp2(c_end), 0.0)
            return moved[:, :width], carry_end * eye_f - moved[:, width:]

        made, states = {}, {}

        def some(heads_now, stage, *lists):
            return {(h, b): stage(h, b, *[l[h, b] for l in lists]) for h in heads_now for b in range(blocks)}

        def scan(heads_now, b):
            for h in heads_now:
                if b == 0:
                    states[h] = jnp.concatenate(made[h, 0], axis=1)
                    continue
                block_add, block_map = made[h, b]
                s_hi = states[h].astype(bf16)
                prefix_ref[s * HEADS_STEP + h, b - 1] = s_hi
                grown = mm(
                    jnp.concatenate(split(block_map), axis=1), jnp.concatenate([s_hi, s_hi], axis=0)
                )
                states[h] = jnp.concatenate([grown[:, :width] + block_add, grown[:, width:]], axis=1)

        def finish(heads_now):
            for h in heads_now:
                at = s * HEADS_STEP + h
                own_out[at] = states[h][:, :width].astype(bf16)
                send_own(at).start()
                add_ref[at] = states[h][:, :width]
                map_ref[at] = states[h][:, width:]

        named = lambda values: dict(zip(pairs, values))
        lows, invs, n_rows = map(named, (lows, invs, n_rows))
        teams = [list(range(h, min(h + TEAM, HEADS_STEP))) for h in range(0, HEADS_STEP, TEAM)]
        pending = []

        def catch_up(count):
            for _ in range(count):
                if pending:
                    pending.pop(0)()

        for team in teams:
            resids = some(team, residual, invs, lows)
            catch_up(2)
            better = some(team, refine, invs, resids)
            catch_up(1)
            writes = some(team, write, better, n_rows)
            catch_up(1)
            made.update(some(team, block_step, writes, n_rows))
            catch_up(len(pending))
            pending = [functools.partial(scan, team, b) for b in range(blocks)]
            pending.append(functools.partial(finish, team))
        catch_up(len(pending))

        if shared:
            @pl.when(s == 0)
            def _():
                for j in range(RELAYS[0]):
                    relay(j)

        return carry

    lax.fori_loop(0, steps, states_step, 0)
    relayed = RELAYS[1] if steps > 1 else RELAYS[0]
    if shared:
        while relayed < RELAYS[2]:
            relay(relayed)
            relayed += 1

    @pl.when(first)
    def _():
        state_in[...] = jnp.zeros_like(state_in)

    done = (steps - 1) * HEADS_STEP
    if done and not direct:
        @pl.when(inner & (seq_here > 1))
        def _():
            for h in range(done):
                forward(h)

    def reads_step(s, carry):
        load(s, 2).wait()
        geo = []
        for b in range(blocks):
            start, seg_row, before, _ = geometry(b)
            seg_tok = segment(start + lax.broadcasted_iota(jnp.int32, (BLOCK, 1), 0))
            geo.append(((tok_j // refl <= tok_i) & (seg_tok == seg_row), seg_tok == before))

        def read_weights(h, b):
            keys, row = near(s, b)
            qb, c_row = q_ref[s, toks(b), cols(h)], row(0, h)
            n_row = scale_ref[b, pl.ds(s * HEADS_STEP + h, 1), :]
            qf = qb.astype(f32)
            nq = lax.rsqrt(jnp.sum(qf * qf, axis=1, keepdims=True) + epsilon) * width ** (-0.5)
            ct = jnp.sum(jnp.where(pick_tok, c_row, 0.0), axis=1, keepdims=True)
            ratio = jnp.where(geo[b][0], jnp.exp2(jnp.minimum(ct - c_row, 0.0)), 0.0)
            carried = (jnp.where(geo[b][1], jnp.exp2(ct), 0.0) * nq) * qf
            return (ratio * mm_nt(qb, keys(h)) * nq * n_row).astype(bf16), carried

        weights = over(read_weights)

        def read(h, b, weight):
            got = mm(weight[0], wrote_ref[s * HEADS_STEP + h, b])
            return got[:, :width], (weight[1] - got[:, width:]).astype(bf16)

        for (h, b), (own, back) in zip(pairs, over(read, weights)):
            if b:
                moved = mm(back, prefix_ref[s * HEADS_STEP + h, b - 1])
                own, back = own + moved[:, :width], moved[:, width:].astype(bf16)
            oloc_ref[s * HEADS_STEP + h, toks(b), :] = own
            read_ref[s * HEADS_STEP + h, toks(b), :] = back
        return carry

    lax.fori_loop(0, steps, reads_step, 0)
    if shared:
        while relayed < RELAYS[3]:
            relay(relayed)
            relayed += 1

    @pl.when(inner)
    def _():
        for h in range(done, heads):
            forward(h)

    if shared:
        while relayed < RELAYS[4]:
            relay(relayed)
            relayed += 1

    load_gain.wait()
    for g in range(0, heads, FINISH_GROUP):
        if shared and g >= done:
            while relayed < SHARE_PARTS:
                relay(relayed)
                relayed += 1
        group = range(g, min(g + FINISH_GROUP, heads))

        for h in group:
            @pl.when(last & (seq_here == 1))
            def _():
                take_own(h).wait_recv()

            @pl.when((seq_here > 1) & (direct | last))
            def _():
                send_full(h).wait_recv()

            @pl.when(seq_here == 1)
            def _():
                state_in[h] = own_in[h]

            @pl.when(seq_here > 1)
            def _():
                state_in[h] = full_in[h]

        for h in group:
            out = oloc_ref[h] + mm(read_ref[h], state_in[h])
            scale = lax.rsqrt(jnp.mean(out * out, axis=-1, keepdims=True) + epsilon)
            normed_ref[:, cols(h)] = (out * scale * gain_ref[...]).astype(bf16)

        if shared:
            for h in group:
                send_normed(h).start()

    load_weight.wait()
    piece, pieces = PIECE, (weight_ref.shape[1] - shared) // PIECE
    copies = []
    for slot, other in enumerate(others):
        rows = normed_ref[pl.ds(pl.multiple_of(other * chunk, chunk), chunk), :]
        for p in range(pieces):
            part = pl.ds(p * piece, piece)
            part_out[slot, :, part] = mm(rows, weight_ref[:, pl.ds(shared + p * piece, piece)]).astype(bf16)
            copies.append(
                pltpu.make_async_remote_copy(
                    src_ref=part_out.at[slot, :, part],
                    dst_ref=part_in.at[slot, :, part],
                    send_sem=part_send.at[slot, p],
                    recv_sem=part_recv.at[slot, p],
                    device_id={"head": other},
                    device_id_type=MESH,
                )
            )
            copies[-1].start()
    rows = normed_ref[pl.ds(pl.multiple_of(head_here * chunk, chunk), chunk), :]
    if shared:
        for j in range(SHARE_PARTS):
            over_parts(j, 1 - parts_here).wait_recv()
            over_cores(SHARE_PARTS + j, rep_here).start()
    for p in range(pieces):
        part = pl.ds(shared + p * piece, piece)
        own_ref[:, part] = mm(rows, weight_ref[:, part])
    if shared:
        for p in range(shared // piece):
            part = pl.ds(p * piece, piece)
            own_ref[:, part] = mm(rows, weight_ref[:, part])
        for j in range(2 * SHARE_PARTS):
            over_cores(j, 1 - rep_here).wait_recv()
        for h in range(heads):
            send_normed(h).wait_recv()
        for p in range(shared // piece):
            part = pl.ds(p * piece, piece)
            peer = mm(rows_in[...], peer_ref[:, part])
            total = own_ref[:, part].astype(bf16).astype(f32) + peer.astype(bf16).astype(f32)
            out_ref[:, part] = total.astype(bf16)
    for p in range(pieces):
        part = pl.ds(p * piece, piece)
        spot = pl.ds(shared + p * piece, piece)
        total = own_ref[:, spot].astype(bf16).astype(f32)
        for slot in range(len(others)):
            copies[slot * pieces + p].wait_recv()
            total += part_in[slot, :, part].astype(f32)
        out_ref[:, spot] = total.astype(bf16)
    for copy in copies:
        copy.wait_send()
    if shared:
        for j in range(SHARE_PARTS):
            from_head(j).wait_send()
            over_parts(j, parts_here).wait_send()
        for j in range(2 * SHARE_PARTS):
            over_cores(j, rep_here).wait_send()
        for h in range(heads):
            send_normed(h).wait_send()

    @pl.when((seq_here > 1) & (last | (not direct)))
    def _():
        for h in range(heads):
            take_own(h).wait_recv()

    @pl.when(seq_here == seq_count - 2)
    def _():
        for h in range(heads):
            take_spare(h).wait_recv()

    for h in range(heads):
        send_own(h).wait_send()

    @pl.when(inner)
    def _():
        for h in range(heads):
            send_full(h).wait_send()


def body(queries, reflect_keys, reflect_values, reflect_beta, log_decay, prompt_lengths, norm_gain, out_weight):
    tokens, refl, wide = reflect_keys.shape[1:]
    heads = log_decay.shape[2]
    width = wide // heads
    blocks = tokens // BLOCK
    sub = refl * BLOCK
    head_count = lax.axis_size("head")
    chunk, model = tokens // head_count, out_weight.shape[1]
    steps, slots = heads // HEADS_STEP, max(head_count - 1, 1)
    wide_step = HEADS_STEP * width
    shared = model * SHARE // PIECE // 100 * PIECE if sharing() else 0
    peer_shape = (out_weight.shape[0], shared) if shared else (32, 128)
    rest = model - shared
    pieces = rest // PIECE
    beta, gate = reflect_beta[0].transpose(1, 2, 0), log_decay[0].T
    dma = pltpu.SemaphoreType.DMA
    anywhere, vmem = pl.BlockSpec(memory_space=pl.ANY), pl.BlockSpec(memory_space=pltpu.VMEM)
    out = pl.pallas_call(
        functools.partial(mixer_kernel, refl, blocks),
        in_specs=[anywhere] * 8,
        out_specs=vmem,
        out_shape=pltpu.VMEM((chunk, model), bf16),
        scratch_shapes=[
            pltpu.SMEM(prompt_lengths.shape, jnp.int32),
            pltpu.VMEM((steps, tokens, wide_step), bf16),
            pltpu.VMEM((steps, tokens, refl, wide_step), bf16),
            pltpu.VMEM((steps, tokens, refl, wide_step), bf16),
            pltpu.VMEM(beta.shape, f32),
            pltpu.VMEM(gate.shape, f32),
            pltpu.VMEM((1, width), f32),
            dma((steps, 3)),
            pltpu.SemaphoreType.REGULAR,
            pltpu.VMEM((blocks, 3, heads, sub), f32),
            pltpu.VMEM((blocks, heads, sub), f32),
            pltpu.VMEM((steps, tokens * refl, wide_step), bf16),
            pltpu.VMEM((heads, blocks, sub, 2 * width), bf16),
            pltpu.VMEM((heads, max(blocks - 1, 1), width, 2 * width), bf16),
            pltpu.VMEM((heads, tokens, width), f32),
            pltpu.VMEM((heads, tokens, width), bf16),
            pltpu.VMEM((heads, width, width), f32),
            pltpu.VMEM((heads, width, width), f32),
            pltpu.VMEM(out_weight.shape, bf16),
            dma((5,)),
            *[pltpu.VMEM((heads, width, width), bf16)] * 3,
            pltpu.VMEM((2 * heads, width, width), bf16),
            pltpu.VMEM((heads, width, width), bf16),
            pltpu.VMEM((tokens, wide), bf16),
            pltpu.VMEM((chunk, model), f32),
            pltpu.VMEM((slots, chunk, rest), bf16),
            pltpu.VMEM((slots, chunk, rest), bf16),
            dma((heads,)), dma((2 * heads,)), dma((heads,)), dma((heads,)), dma((slots, pieces)), dma((slots, pieces)),
            pltpu.VMEM(peer_shape, bf16),
            pltpu.VMEM((chunk, wide), bf16),
            dma((SHARE_PARTS,)), dma((SHARE_PARTS,)), dma((SHARE_PARTS,)), dma((SHARE_PARTS,)),
            dma((2 * SHARE_PARTS,)), dma((2 * SHARE_PARTS,)), dma((heads,)), dma((heads,)),
        ],
        compiler_params=pltpu.CompilerParams(
            collective_id=0, has_side_effects=True, vmem_limit_bytes=56 * 2**20
        ),
    )(
        prompt_lengths,
        queries[0],
        reflect_keys[0],
        reflect_values[0],
        beta,
        gate,
        norm_gain[None],
        out_weight,
    )
    return out[None]


def solution(mesh):
    in_specs = (
        P(("parts", "rep"), "seq", "head"),
        P(("parts", "rep"), "seq", None, "head"),
        P(("parts", "rep"), "seq", None, "head"),
        P(("parts", "rep"), "seq", None, "head"),
        P(("parts", "rep"), "seq", "head"),
        P(("parts", "rep"), None),
        P(),
        P("head", None),
    )
    out_specs = P(("parts", "rep"), ("seq", "head"), None)
    return jax.shard_map(body, mesh=mesh, in_specs=in_specs, out_specs=out_specs, check_vma=False)
```

```python
import functools
import math

import jax
import jax.numpy as jnp
from jax import lax
from jax.experimental import pallas as pl
from jax.experimental.pallas import tpu as pltpu
from jax.sharding import PartitionSpec as P

BLOCK = 64
HEADS_STEP = 4
FINISH_GROUP = 2
PIECE = 256
SHARE = 63
SHARE_PARTS = 8
RELAYS = (1, 3, 5, 6, 7)
TEAM = 2
MESH = pl.DeviceIdType.MESH

epsilon = 1e-06
f32 = jnp.float32
bf16 = jnp.bfloat16
highest = lax.Precision.HIGHEST


def mm(a, b, precision=None):
    return jnp.dot(a, b, preferred_element_type=f32, precision=precision)


def mm_nt(a, b):
    return lax.dot_general(a, b, (((1,), (1,)), ((), ())), preferred_element_type=f32)


def mm_tn(a, b):
    return lax.dot_general(a, b, (((0,), (0,)), ((), ())), preferred_element_type=f32)


def split(x):
    hi = x.astype(bf16)
    return hi, (x - hi.astype(f32)).astype(bf16)


def split3(x):
    hi = x.astype(bf16).astype(f32)
    mid = (x - hi).astype(bf16).astype(f32)
    return [hi, mid, x - hi - mid]


def sub_rows(x, pattern, blocks):
    rows = x.shape[0]
    zero = jnp.zeros_like(pattern)
    table = jnp.concatenate(
        [jnp.concatenate([pattern if c == r else zero for c in range(blocks)], axis=1) for r in range(blocks)],
        axis=0,
    )
    got = mm(jnp.concatenate(split3(x), axis=0).astype(bf16), table)
    return got[:rows] + got[rows : 2 * rows] + got[2 * rows :]


def sharing():
    return all(lax.axis_size(name) == 2 for name in ("head", "parts", "rep"))


def mixer_kernel(
    refl, blocks, len_hbm, q_hbm, k_hbm, v_hbm, beta_hbm, gate_hbm, gain_hbm, weight_hbm, out_ref,
    len_ref, q_ref, k_ref, v_ref, beta_ref, gate_ref, gain_ref, in_sem, ready_sem,
    rows_ref, scale_ref, kflat_ref, wrote_ref, prefix_ref, oloc_ref, read_ref, add_ref, map_ref,
    weight_ref, weight_sem, state_in, own_out, full_out, own_in, full_in, normed_ref, own_ref, part_out, part_in,
    own_send, own_recv, full_send, full_recv, part_send, part_recv,
    peer_ref, rows_in, x_send, x_recv, y_send, y_recv, core_send, core_recv, norm_send, norm_recv,
):
    heads, width = add_ref.shape[:2]
    steps = heads // HEADS_STEP
    wide = HEADS_STEP * width
    sub = refl * BLOCK
    tokens = blocks * BLOCK
    seq_count, head_count = lax.axis_size("seq"), lax.axis_size("head")
    seq_here, head_here = lax.axis_index("seq"), lax.axis_index("head")
    chunk = out_ref.shape[0]
    first, last = seq_here == 0, seq_here == seq_count - 1
    others = [lax.rem(head_here + d, head_count) for d in range(1, head_count)]
    shared = peer_ref.shape[1] if sharing() else 0
    parts_here, rep_here = lax.axis_index("parts"), lax.axis_index("rep")
    quarter = peer_ref.shape[0] // 4
    slab = quarter // SHARE_PARTS

    def slab_rows(rep, parts, j):
        return pl.ds(pl.multiple_of((rep * 2 + parts) * quarter + j * slab, slab), slab)

    def remote(src, dst, send, recv, device):
        return pltpu.make_async_remote_copy(
            src_ref=src, dst_ref=dst, send_sem=send, recv_sem=recv, device_id=device, device_id_type=MESH
        )

    def from_head(j):
        rows = slab_rows(rep_here, parts_here, j)
        return remote(
            weight_hbm.at[rows, pl.ds(0, shared)], peer_ref.at[rows],
            x_send, x_recv.at[j], {"head": 1 - head_here},
        )

    def over_parts(j, parts):
        rows = slab_rows(rep_here, parts, j)
        return remote(
            peer_ref.at[rows], peer_ref.at[rows], y_send, y_recv.at[j], {"parts": 1 - parts_here}
        )

    def over_cores(j, rep):
        parts = parts_here if j < SHARE_PARTS else 1 - parts_here
        rows = slab_rows(rep, parts, j % SHARE_PARTS)
        return remote(
            peer_ref.at[rows], peer_ref.at[rows], core_send, core_recv, {"rep": 1 - rep_here}
        )

    def quarter_rows(rep, parts, count=1):
        return pl.ds(pl.multiple_of((rep * 2 + parts) * quarter, quarter), count * quarter)

    def all_x():
        rows = quarter_rows(rep_here, parts_here)
        return remote(
            weight_hbm.at[rows, pl.ds(0, shared)], peer_ref.at[rows],
            x_send, x_recv.at[0], {"head": 1 - head_here},
        )

    def all_y():
        rows = quarter_rows(rep_here, parts_here)
        return remote(peer_ref.at[rows], peer_ref.at[rows], y_send, y_recv.at[0], {"parts": 1 - parts_here})

    def all_cores(rep):
        rows = quarter_rows(rep, 0, 2)
        return remote(peer_ref.at[rows], peer_ref.at[rows], core_send, core_recv, {"rep": 1 - rep_here})

    def all_normed():
        rows = pl.ds(pl.multiple_of(others[0] * chunk, chunk), chunk)
        return remote(normed_ref.at[rows], rows_in, norm_send, norm_recv, {"head": 1 - head_here})

    def relay(j):
        from_head(j).wait_recv()
        over_parts(j, parts_here).start()
        over_cores(j, rep_here).start()

    def send_normed(h):
        span = cols(h)
        rows = pl.ds(pl.multiple_of(others[0] * chunk, chunk), chunk)
        return remote(
            normed_ref.at[rows, span], rows_in.at[:, span],
            norm_send, norm_recv, {"head": 1 - head_here},
        )

    barrier = pltpu.get_barrier_semaphore()

    @pl.when(seq_here < seq_count - 1)
    def _():
        pl.semaphore_signal(barrier, inc=1, device_id={"seq": seq_here + 1}, device_id_type=MESH)

    for other in others:
        pl.semaphore_signal(barrier, inc=1, device_id={"head": other}, device_id_type=MESH)
    if shared:
        pl.semaphore_signal(barrier, inc=1, device_id={"parts": 1 - parts_here}, device_id_type=MESH)
        pl.semaphore_signal(barrier, inc=1, device_id={"rep": 1 - rep_here}, device_id_type=MESH)

    def load(s, kind):
        span = pl.ds(pl.multiple_of(s * wide, wide), wide)
        src, dst = [
            (k_hbm.at[:, :, span], k_ref), (v_hbm.at[:, :, span], v_ref), (q_hbm.at[:, span], q_ref)
        ][kind]
        return pltpu.make_async_copy(src, dst.at[s], in_sem.at[s, kind])

    load_beta = pltpu.make_async_copy(beta_hbm, beta_ref, weight_sem.at[1])
    load_gate = pltpu.make_async_copy(gate_hbm, gate_ref, weight_sem.at[2])
    load_weight = pltpu.make_async_copy(weight_hbm, weight_ref, weight_sem.at[0])
    load_len = pltpu.make_async_copy(len_hbm, len_ref, weight_sem.at[3])
    load_gain = pltpu.make_async_copy(gain_hbm, gain_ref, weight_sem.at[4])
    load_len.start()
    load_gate.start()
    load_beta.start()
    for s in range(steps):
        load(s, 0).start()
        load(s, 1).start()
    for s in range(steps):
        load(s, 2).start()
    load_gain.start()
    load_weight.start()
    pl.semaphore_wait(barrier, jnp.where(first, 0, 1) + head_count - 1 + (2 if shared else 0))
    if shared:
        for j in range(SHARE_PARTS):
            from_head(j).start()

    @pl.when(seq_here > 0)
    def _():
        pl.semaphore_signal(ready_sem, inc=1, device_id={"seq": seq_here - 1}, device_id_type=MESH)

    load_len.wait()

    offset = seq_here * tokens
    ends = []
    running = 0
    for d in range(len_ref.shape[1]):
        running = running + len_ref[0, d]
        ends.append(running)

    def segment(pos):
        total = jnp.zeros(pos.shape, jnp.int32)
        for end in ends:
            total += jnp.where(pos >= end, 1, 0)
        return total

    row_i = lax.broadcasted_iota(jnp.int32, (sub, sub), 0)
    col_i = lax.broadcasted_iota(jnp.int32, (sub, sub), 1)
    eye = row_i == col_i
    eye_f = jnp.where(eye, 1.0, 0.0).astype(f32)
    tok_i = lax.broadcasted_iota(jnp.int32, (BLOCK, sub), 0)
    tok_j = lax.broadcasted_iota(jnp.int32, (BLOCK, sub), 1)
    pick_tok = tok_j == tok_i * refl + refl - 1
    levels = []
    size = refl
    while size < sub:
        big = min(4 * size, sub)
        levels.append((row_i // big == col_i // big) & (row_i // size > col_i // size))
        size = big

    load_gate.wait()
    load_beta.wait()
    table = sub_rows(gate_ref[...], jnp.where(tok_i <= tok_j // refl, 1.0, 0.0).astype(bf16), blocks)
    total = 0.0
    for j in range(refl):
        pick = jnp.where(tok_i * refl + j == tok_j, 1.0, 0.0).astype(bf16)
        total += sub_rows(beta_ref[j], pick, blocks)
    for b in range(blocks):
        rows_ref[b, 0] = table[:, b * sub : (b + 1) * sub] * math.log2(math.e)
        rows_ref[b, 1] = total[:, b * sub : (b + 1) * sub]
        rows_ref[b, 2] = rows_ref[b, 0] + jnp.log2(rows_ref[b, 1])

    def geometry(b):
        start = offset + b * BLOCK
        seg_row = segment(start + lax.broadcasted_iota(jnp.int32, (1, sub), 1) // refl)
        before = jnp.where(start == 0, -1, 0)
        last_seg = 0
        for end in ends:
            before += jnp.where(start - 1 >= end, 1, 0)
            last_seg += jnp.where(start + BLOCK - 1 >= end, 1, 0)
        return start, seg_row, before, last_seg

    pairs = [(h, b) for h in range(HEADS_STEP) for b in range(blocks)]

    def over(stage, *lists):
        return [stage(h, b, *args) for (h, b), *args in zip(pairs, *lists)]

    def cols(h):
        return slice(h * width, (h + 1) * width)

    def toks(b):
        return slice(b * BLOCK, (b + 1) * BLOCK)

    def column(values):
        return jnp.sum(jnp.where(eye, values, 0.0), axis=1, keepdims=True)

    reach = (seq_count * tokens // 2 - 2) // tokens
    direct = reach <= 1
    inner = (seq_here > 0) & (seq_here < seq_count - 1)
    following = {"seq": lax.rem(seq_here + 1, seq_count)}
    beside = {"seq": jnp.where(last, seq_count - 2, seq_here + 1)}
    spare = jnp.where(last, heads, 0)
    arrival = lambda h: jnp.where(last, heads, h)

    def send_own(h):
        return remote(own_out.at[h], own_in.at[h + spare], own_send, own_recv.at[arrival(h)], beside)

    def take_own(h):
        return remote(own_out.at[h], own_in.at[h], own_send, own_recv.at[h], following)

    def send_full(h):
        return remote(full_out.at[h], full_in.at[h], full_send, full_recv.at[h], following)

    def pass_on(h, state):
        both = jnp.concatenate(split(map_ref[h]), axis=1)
        grown = add_ref[h] + mm(both, jnp.concatenate([state, state], axis=0))
        full_out[h] = grown.astype(bf16)
        send_full(h).start()

    def forward(h):
        if direct:
            take_own(h).wait_recv()
            pass_on(h, own_in[h])
        else:
            @pl.when(seq_here == 1)
            def _():
                take_own(h).wait_recv()
                pass_on(h, own_in[h])

            @pl.when(seq_here > 1)
            def _():
                send_full(h).wait_recv()
                pass_on(h, full_in[h])

    def near(s, b):
        def keys(h):
            return kflat_ref[s, b * sub : (b + 1) * sub, cols(h)]

        def row(kind, h):
            return rows_ref[b, kind, pl.ds(s * HEADS_STEP + h, 1), :]

        return keys, row

    def states_step(s, carry):
        load(s, 0).wait()
        load(s, 1).wait()
        keys = lambda h, b: near(s, b)[0](h)
        row = lambda kind, h, b: near(s, b)[1](kind, h)
        geo = []
        for b in range(blocks):
            start, seg_row, before, last_seg = geometry(b)
            seg_col = segment(start + lax.broadcasted_iota(jnp.int32, (sub, 1), 0) // refl)
            incl = (row_i > col_i) & (seg_col == seg_row)
            geo.append((incl, seg_row == before, seg_row == last_seg, last_seg == before))

        for h, b in pairs:
            kflat_ref[s, b * sub : (b + 1) * sub, cols(h)] = k_ref[s, toks(b), :, cols(h)].reshape(sub, width)

        def scales(h, b):
            gram = mm_nt(keys(h, b), keys(h, b))
            square = jnp.sum(jnp.where(eye, gram, 0.0), axis=0, keepdims=True) + epsilon
            n_log, n_row = -0.5 * jnp.log2(square), lax.rsqrt(square)
            scale_ref[b, pl.ds(s * HEADS_STEP + h, 1), :] = n_row
            factor = jnp.exp2(column(row(2, h, b) + n_log) + (n_log - row(0, h, b)))
            return jnp.where(geo[b][0], factor * gram, 0.0), n_row

        lows, n_rows = zip(*over(scales))
        invs = [eye_f - jnp.where(row_i // refl == col_i // refl, low, 0.0) for low in lows]
        for mask in levels:
            heads_b = [inv.astype(bf16) for inv in invs]
            nils = [
                mm(inv, jnp.where(mask, low, 0.0).astype(bf16)).astype(bf16)
                for inv, low in zip(heads_b, lows)
            ]
            both = [mm(nil, jnp.concatenate([nil, inv], axis=1)) for nil, inv in zip(nils, heads_b)]
            halves = [inv - pair[:, sub:] for inv, pair in zip(invs, both)]
            invs = [
                half + mm(pair[:, :sub].astype(bf16), half.astype(bf16))
                for half, pair in zip(halves, both)
            ]

        if shared:
            @pl.when(s > 0)
            def _():
                for j in range(RELAYS[0], RELAYS[1]):
                    relay(j)

        @pl.when((s == 0) & (seq_here < seq_count - 1))
        def _():
            pl.semaphore_wait(ready_sem, 1)

        @pl.when((s > 0) & inner & (direct | (seq_here == 1)))
        def _():
            for h in range(HEADS_STEP):
                forward((s - 1) * HEADS_STEP + h)

        def residual(h, b, inv, low):
            inv_b = inv.astype(bf16)
            low_2 = jnp.concatenate(split(low), axis=1)
            return eye_f - inv_b.astype(f32) - mm(low_2, jnp.concatenate([inv_b, inv_b], axis=0))

        def refine(h, b, inv, resid):
            inv_b = inv.astype(bf16)
            return inv_b.astype(f32) + mm(inv_b, resid.astype(bf16))

        def write(h, b, inv, n_row):
            carry_row = jnp.where(geo[b][1], jnp.exp2(row(0, h, b)), 0.0)
            by_beta = inv * row(1, h, b)
            tv = jnp.concatenate(split(by_beta), axis=1)
            tk = jnp.concatenate(split(by_beta * (carry_row * n_row)), axis=1)
            vb, kb = v_ref[s, toks(b), :, cols(h)].reshape(sub, width), keys(h, b)
            return jnp.concatenate(
                [mm(tv, jnp.concatenate([vb, vb], axis=0)), mm(tk, jnp.concatenate([kb, kb], axis=0))],
                axis=1,
            )

        def block_step(h, b, wrote, n_row):
            wrote_ref[s * HEADS_STEP + h, b] = wrote.astype(bf16)
            c_row = row(0, h, b)
            c_end = c_row[:, sub - 1 : sub]
            e_row = jnp.where(geo[b][2], jnp.exp2(jnp.minimum(c_end - c_row, 0.0)), 0.0) * n_row
            kb = keys(h, b)
            moved = mm_tn(
                jnp.concatenate([kb, kb], axis=0), jnp.concatenate(split(wrote * column(e_row)), axis=0)
            )
            carry_end = jnp.where(geo[b][3], jnp.exp2(c_end), 0.0)
            return moved[:, :width], carry_end * eye_f - moved[:, width:]

        made, states = {}, {}

        def some(heads_now, stage, *lists):
            return {(h, b): stage(h, b, *[l[h, b] for l in lists]) for h in heads_now for b in range(blocks)}

        def scan(heads_now, b):
            for h in heads_now:
                if b == 0:
                    states[h] = jnp.concatenate(made[h, 0], axis=1)
                    continue
                block_add, block_map = made[h, b]
                s_hi = states[h].astype(bf16)
                prefix_ref[s * HEADS_STEP + h, b - 1] = s_hi
                grown = mm(
                    jnp.concatenate(split(block_map), axis=1), jnp.concatenate([s_hi, s_hi], axis=0)
                )
                states[h] = jnp.concatenate([grown[:, :width] + block_add, grown[:, width:]], axis=1)

        def finish(heads_now):
            for h in heads_now:
                at = s * HEADS_STEP + h
                own_out[at] = states[h][:, :width].astype(bf16)
                send_own(at).start()
                add_ref[at] = states[h][:, :width]
                map_ref[at] = states[h][:, width:]

        named = lambda values: dict(zip(pairs, values))
        lows, invs, n_rows = map(named, (lows, invs, n_rows))
        teams = [list(range(h, min(h + TEAM, HEADS_STEP))) for h in range(0, HEADS_STEP, TEAM)]
        pending = []

        def catch_up(count):
            for _ in range(count):
                if pending:
                    pending.pop(0)()

        for team in teams:
            resids = some(team, residual, invs, lows)
            catch_up(2)
            better = some(team, refine, invs, resids)
            catch_up(1)
            writes = some(team, write, better, n_rows)
            catch_up(1)
            made.update(some(team, block_step, writes, n_rows))
            catch_up(len(pending))
            pending = [functools.partial(scan, team, b) for b in range(blocks)]
            pending.append(functools.partial(finish, team))
        catch_up(len(pending))

        if shared:
            @pl.when(s == 0)
            def _():
                for j in range(RELAYS[0]):
                    relay(j)

        return carry

    lax.fori_loop(0, steps, states_step, 0)
    relayed = RELAYS[1] if steps > 1 else RELAYS[0]
    if shared:
        while relayed < RELAYS[2]:
            relay(relayed)
            relayed += 1

    @pl.when(first)
    def _():
        state_in[...] = jnp.zeros_like(state_in)

    done = (steps - 1) * HEADS_STEP
    if done and not direct:
        @pl.when(inner & (seq_here > 1))
        def _():
            for h in range(done):
                forward(h)

    def reads_step(s, carry):
        load(s, 2).wait()
        geo = []
        for b in range(blocks):
            start, seg_row, before, _ = geometry(b)
            seg_tok = segment(start + lax.broadcasted_iota(jnp.int32, (BLOCK, 1), 0))
            geo.append(((tok_j // refl <= tok_i) & (seg_tok == seg_row), seg_tok == before))

        def read_weights(h, b):
            keys, row = near(s, b)
            qb, c_row = q_ref[s, toks(b), cols(h)], row(0, h)
            n_row = scale_ref[b, pl.ds(s * HEADS_STEP + h, 1), :]
            qf = qb.astype(f32)
            nq = lax.rsqrt(jnp.sum(qf * qf, axis=1, keepdims=True) + epsilon) * width ** (-0.5)
            ct = jnp.sum(jnp.where(pick_tok, c_row, 0.0), axis=1, keepdims=True)
            ratio = jnp.where(geo[b][0], jnp.exp2(jnp.minimum(ct - c_row, 0.0)), 0.0)
            carried = (jnp.where(geo[b][1], jnp.exp2(ct), 0.0) * nq) * qf
            return (ratio * mm_nt(qb, keys(h)) * nq * n_row).astype(bf16), carried

        weights = over(read_weights)

        def read(h, b, weight):
            got = mm(weight[0], wrote_ref[s * HEADS_STEP + h, b])
            return got[:, :width], (weight[1] - got[:, width:]).astype(bf16)

        for (h, b), (own, back) in zip(pairs, over(read, weights)):
            if b:
                moved = mm(back, prefix_ref[s * HEADS_STEP + h, b - 1])
                own, back = own + moved[:, :width], moved[:, width:].astype(bf16)
            oloc_ref[s * HEADS_STEP + h, toks(b), :] = own
            read_ref[s * HEADS_STEP + h, toks(b), :] = back
        return carry

    lax.fori_loop(0, steps, reads_step, 0)
    if shared:
        while relayed < RELAYS[3]:
            relay(relayed)
            relayed += 1

    @pl.when(inner)
    def _():
        for h in range(done, heads):
            forward(h)

    if shared:
        while relayed < RELAYS[4]:
            relay(relayed)
            relayed += 1

    load_gain.wait()
    for g in range(0, heads, FINISH_GROUP):
        if shared and g >= done:
            while relayed < SHARE_PARTS:
                relay(relayed)
                relayed += 1
        group = range(g, min(g + FINISH_GROUP, heads))

        for h in group:
            @pl.when(last & (seq_here == 1))
            def _():
                take_own(h).wait_recv()

            @pl.when((seq_here > 1) & (direct | last))
            def _():
                send_full(h).wait_recv()

            @pl.when(seq_here == 1)
            def _():
                state_in[h] = own_in[h]

            @pl.when(seq_here > 1)
            def _():
                state_in[h] = full_in[h]

        for h in group:
            out = oloc_ref[h] + mm(read_ref[h], state_in[h])
            scale = lax.rsqrt(jnp.mean(out * out, axis=-1, keepdims=True) + epsilon)
            normed_ref[:, cols(h)] = (out * scale * gain_ref[...]).astype(bf16)

        if shared:
            for h in group:
                send_normed(h).start()

    load_weight.wait()
    piece, pieces = PIECE, (weight_ref.shape[1] - shared) // PIECE
    copies = []
    for slot, other in enumerate(others):
        rows = normed_ref[pl.ds(pl.multiple_of(other * chunk, chunk), chunk), :]
        for p in range(pieces):
            part = pl.ds(p * piece, piece)
            part_out[slot, :, part] = mm(rows, weight_ref[:, pl.ds(shared + p * piece, piece)]).astype(bf16)
            copies.append(
                pltpu.make_async_remote_copy(
                    src_ref=part_out.at[slot, :, part],
                    dst_ref=part_in.at[slot, :, part],
                    send_sem=part_send.at[slot],
                    recv_sem=part_recv.at[slot, p],
                    device_id={"head": other},
                    device_id_type=MESH,
                )
            )
            copies[-1].start()
    rows = normed_ref[pl.ds(pl.multiple_of(head_here * chunk, chunk), chunk), :]
    if shared:
        for j in range(SHARE_PARTS):
            over_parts(j, 1 - parts_here).wait_recv()
            over_cores(SHARE_PARTS + j, rep_here).start()
    for p in range(pieces):
        part = pl.ds(shared + p * piece, piece)
        own_ref[:, part] = mm(rows, weight_ref[:, part])
    if shared:
        for p in range(shared // piece):
            part = pl.ds(p * piece, piece)
            own_ref[:, part] = mm(rows, weight_ref[:, part])
        all_cores(1 - rep_here).wait_recv()
        all_normed().wait_recv()
        for p in range(shared // piece):
            part = pl.ds(p * piece, piece)
            peer = mm(rows_in[...], peer_ref[:, part])
            total = own_ref[:, part].astype(bf16).astype(f32) + peer.astype(bf16).astype(f32)
            out_ref[:, part] = total.astype(bf16)
    for p in range(pieces):
        part = pl.ds(p * piece, piece)
        spot = pl.ds(shared + p * piece, piece)
        total = own_ref[:, spot].astype(bf16).astype(f32)
        for slot in range(len(others)):
            copies[slot * pieces + p].wait_recv()
            total += part_in[slot, :, part].astype(f32)
        out_ref[:, spot] = total.astype(bf16)
    for slot, other in enumerate(others):
        remote(
            part_out.at[slot], part_in.at[slot], part_send.at[slot], part_recv.at[slot, 0], {"head": other}
        ).wait_send()
    if shared:
        all_x().wait_send()
        all_y().wait_send()
        all_cores(rep_here).wait_send()
        all_normed().wait_send()

    @pl.when((seq_here > 1) & (last | (not direct)))
    def _():
        for h in range(heads):
            take_own(h).wait_recv()

    @pl.when(seq_here == seq_count - 2)
    def _():
        remote(own_out, own_in.at[pl.ds(heads, heads)], own_send, own_recv.at[heads], following).wait_recv()

    remote(own_out, own_in.at[pl.ds(0, heads)], own_send, own_recv.at[0], following).wait_send()

    @pl.when(inner)
    def _():
        remote(full_out, full_in, full_send, full_recv.at[0], following).wait_send()


def body(queries, reflect_keys, reflect_values, reflect_beta, log_decay, prompt_lengths, norm_gain, out_weight):
    tokens, refl, wide = reflect_keys.shape[1:]
    heads = log_decay.shape[2]
    width = wide // heads
    blocks = tokens // BLOCK
    sub = refl * BLOCK
    head_count = lax.axis_size("head")
    chunk, model = tokens // head_count, out_weight.shape[1]
    steps, slots = heads // HEADS_STEP, max(head_count - 1, 1)
    wide_step = HEADS_STEP * width
    shared = model * SHARE // PIECE // 100 * PIECE if sharing() else 0
    peer_shape = (out_weight.shape[0], shared) if shared else (32, 128)
    rest = model - shared
    pieces = rest // PIECE
    beta, gate = reflect_beta[0].transpose(1, 2, 0), log_decay[0].T
    dma = pltpu.SemaphoreType.DMA
    anywhere, vmem = pl.BlockSpec(memory_space=pl.ANY), pl.BlockSpec(memory_space=pltpu.VMEM)
    out = pl.pallas_call(
        functools.partial(mixer_kernel, refl, blocks),
        in_specs=[anywhere] * 8,
        out_specs=vmem,
        out_shape=pltpu.VMEM((chunk, model), bf16),
        scratch_shapes=[
            pltpu.SMEM(prompt_lengths.shape, jnp.int32),
            pltpu.VMEM((steps, tokens, wide_step), bf16),
            pltpu.VMEM((steps, tokens, refl, wide_step), bf16),
            pltpu.VMEM((steps, tokens, refl, wide_step), bf16),
            pltpu.VMEM(beta.shape, f32),
            pltpu.VMEM(gate.shape, f32),
            pltpu.VMEM((1, width), f32),
            dma((steps, 3)),
            pltpu.SemaphoreType.REGULAR,
            pltpu.VMEM((blocks, 3, heads, sub), f32),
            pltpu.VMEM((blocks, heads, sub), f32),
            pltpu.VMEM((steps, tokens * refl, wide_step), bf16),
            pltpu.VMEM((heads, blocks, sub, 2 * width), bf16),
            pltpu.VMEM((heads, max(blocks - 1, 1), width, 2 * width), bf16),
            pltpu.VMEM((heads, tokens, width), f32),
            pltpu.VMEM((heads, tokens, width), bf16),
            pltpu.VMEM((heads, width, width), f32),
            pltpu.VMEM((heads, width, width), f32),
            pltpu.VMEM(out_weight.shape, bf16),
            dma((5,)),
            *[pltpu.VMEM((heads, width, width), bf16)] * 3,
            pltpu.VMEM((2 * heads, width, width), bf16),
            pltpu.VMEM((heads, width, width), bf16),
            pltpu.VMEM((tokens, wide), bf16),
            pltpu.VMEM((chunk, model), f32),
            pltpu.VMEM((slots, chunk, rest), bf16),
            pltpu.VMEM((slots, chunk, rest), bf16),
            dma, dma((heads + 1,)), dma, dma((heads,)), dma((slots,)), dma((slots, pieces)),
            pltpu.VMEM(peer_shape, bf16),
            pltpu.VMEM((chunk, wide), bf16),
            dma, dma((SHARE_PARTS,)), dma, dma((SHARE_PARTS,)), dma, dma, dma, dma,
        ],
        compiler_params=pltpu.CompilerParams(
            collective_id=0, has_side_effects=True, vmem_limit_bytes=56 * 2**20
        ),
    )(
        prompt_lengths,
        queries[0],
        reflect_keys[0],
        reflect_values[0],
        beta,
        gate,
        norm_gain[None],
        out_weight,
    )
    return out[None]


def solution(mesh):
    in_specs = (
        P(("parts", "rep"), "seq", "head"),
        P(("parts", "rep"), "seq", None, "head"),
        P(("parts", "rep"), "seq", None, "head"),
        P(("parts", "rep"), "seq", None, "head"),
        P(("parts", "rep"), "seq", "head"),
        P(("parts", "rep"), None),
        P(),
        P("head", None),
    )
    out_specs = P(("parts", "rep"), ("seq", "head"), None)
    return jax.shard_map(body, mesh=mesh, in_specs=in_specs, out_specs=out_specs, check_vma=False)
```

```python
import functools
import math

import jax
import jax.numpy as jnp
from jax import lax
from jax.experimental import pallas as pl
from jax.experimental.pallas import tpu as pltpu
from jax.sharding import PartitionSpec as P

BLOCK = 64
HEADS_STEP = 4
FINISH_GROUP = 2
PIECE = 256
SHARE = 63
SHARE_PARTS = 8
SWAP = 2
ORDER = (0, 1, 2, 6, 3, 7, 4, 5)
RELAYS = (1, 3, 5, 7, 8)
TEAM = 2
MESH = pl.DeviceIdType.MESH

epsilon = 1e-06
f32 = jnp.float32
bf16 = jnp.bfloat16
highest = lax.Precision.HIGHEST


def mm(a, b, precision=None):
    return jnp.dot(a, b, preferred_element_type=f32, precision=precision)


def mm_nt(a, b):
    return lax.dot_general(a, b, (((1,), (1,)), ((), ())), preferred_element_type=f32)


def mm_tn(a, b):
    return lax.dot_general(a, b, (((0,), (0,)), ((), ())), preferred_element_type=f32)


def split(x):
    hi = x.astype(bf16)
    return hi, (x - hi.astype(f32)).astype(bf16)


def split3(x):
    hi = x.astype(bf16).astype(f32)
    mid = (x - hi).astype(bf16).astype(f32)
    return [hi, mid, x - hi - mid]


def sub_rows(x, pattern, blocks):
    rows = x.shape[0]
    zero = jnp.zeros_like(pattern)
    table = jnp.concatenate(
        [jnp.concatenate([pattern if c == r else zero for c in range(blocks)], axis=1) for r in range(blocks)],
        axis=0,
    )
    got = mm(jnp.concatenate(split3(x), axis=0).astype(bf16), table)
    return got[:rows] + got[rows : 2 * rows] + got[2 * rows :]


def sharing():
    pairs = all(lax.axis_size(name) == 2 for name in ("head", "parts", "rep"))
    return pairs and lax.axis_size("seq") % 2 == 0


def mixer_kernel(
    refl, blocks, len_hbm, q_hbm, k_hbm, v_hbm, beta_hbm, gate_hbm, gain_hbm, weight_hbm, out_ref,
    len_ref, q_ref, k_ref, v_ref, beta_ref, gate_ref, gain_ref, in_sem, ready_sem,
    rows_ref, scale_ref, kflat_ref, wrote_ref, prefix_ref, oloc_ref, read_ref, add_ref, map_ref,
    weight_ref, weight_sem, state_in, own_out, full_out, own_in, full_in, normed_ref, own_ref, part_out, part_in,
    own_send, own_recv, full_send, full_recv, part_send, part_recv,
    peer_ref, rows_in, x_send, x_recv, y_send, y_recv, z_send, z_recv, core_send, core_recv, norm_send, norm_recv,
):
    heads, width = add_ref.shape[:2]
    steps = heads // HEADS_STEP
    wide = HEADS_STEP * width
    sub = refl * BLOCK
    tokens = blocks * BLOCK
    seq_count, head_count = lax.axis_size("seq"), lax.axis_size("head")
    seq_here, head_here = lax.axis_index("seq"), lax.axis_index("head")
    chunk = out_ref.shape[0]
    first, last = seq_here == 0, seq_here == seq_count - 1
    others = [lax.rem(head_here + d, head_count) for d in range(1, head_count)]
    shared = peer_ref.shape[1] if sharing() else 0
    parts_here, rep_here = lax.axis_index("parts"), lax.axis_index("rep")
    quarter = peer_ref.shape[0] // 4
    slab = quarter // SHARE_PARTS

    odd = lax.rem(seq_here, 2)
    twin = {"seq": seq_here + 1 - 2 * odd}
    direct_slots = SHARE_PARTS - SWAP

    def slab_rows(rep, parts, j):
        if j < SWAP:
            j = odd * SWAP + j
        elif j < direct_slots:
            j = j + SWAP
        else:
            j = (1 - odd) * SWAP + j - direct_slots
        return pl.ds(pl.multiple_of((rep * 2 + parts) * quarter + j * slab, slab), slab)

    def to_twin(k, slot):
        rows = slab_rows(rep_here, parts_here, slot)
        return remote(peer_ref.at[rows], peer_ref.at[rows], z_send, z_recv.at[k], twin)

    def remote(src, dst, send, recv, device):
        return pltpu.make_async_remote_copy(
            src_ref=src, dst_ref=dst, send_sem=send, recv_sem=recv, device_id=device, device_id_type=MESH
        )

    def from_head(j):
        rows = slab_rows(rep_here, parts_here, j)
        return remote(
            weight_hbm.at[rows, pl.ds(0, shared)], peer_ref.at[rows],
            x_send, x_recv.at[j], {"head": 1 - head_here},
        )

    def over_parts(j, parts):
        rows = slab_rows(rep_here, parts, j)
        return remote(
            peer_ref.at[rows], peer_ref.at[rows], y_send, y_recv.at[j], {"parts": 1 - parts_here}
        )

    def over_cores(j, rep):
        parts = parts_here if j < SHARE_PARTS else 1 - parts_here
        rows = slab_rows(rep, parts, j % SHARE_PARTS)
        return remote(
            peer_ref.at[rows], peer_ref.at[rows], core_send, core_recv, {"rep": 1 - rep_here}
        )

    def quarter_rows(rep, parts, count=1):
        return pl.ds(pl.multiple_of((rep * 2 + parts) * quarter, quarter), count * quarter)

    def all_x():
        rows = pl.ds(pl.multiple_of((rep_here * 2 + parts_here) * quarter, quarter), direct_slots * slab)
        return remote(
            weight_hbm.at[rows, pl.ds(0, shared)], peer_ref.at[rows],
            x_send, x_recv.at[0], {"head": 1 - head_here},
        )

    def all_y():
        rows = quarter_rows(rep_here, parts_here)
        return remote(peer_ref.at[rows], peer_ref.at[rows], y_send, y_recv.at[0], {"parts": 1 - parts_here})

    def all_cores(rep):
        rows = quarter_rows(rep, 0, 2)
        return remote(peer_ref.at[rows], peer_ref.at[rows], core_send, core_recv, {"rep": 1 - rep_here})

    def all_normed():
        rows = pl.ds(pl.multiple_of(others[0] * chunk, chunk), chunk)
        return remote(normed_ref.at[rows], rows_in, norm_send, norm_recv, {"head": 1 - head_here})

    def all_z():
        rows = pl.ds(pl.multiple_of((rep_here * 2 + parts_here) * quarter, quarter), SWAP * slab)
        return remote(peer_ref.at[rows], peer_ref.at[rows], z_send, z_recv.at[0], twin)

    def relay(place):
        j = ORDER[place]
        if j < direct_slots:
            from_head(j).wait_recv()
        else:
            to_twin(j - direct_slots, j).wait_recv()
        if j < SWAP:
            to_twin(j, j).start()
        over_parts(j, parts_here).start()
        over_cores(j, rep_here).start()

    def send_normed(h):
        span = cols(h)
        rows = pl.ds(pl.multiple_of(others[0] * chunk, chunk), chunk)
        return remote(
            normed_ref.at[rows, span], rows_in.at[:, span],
            norm_send, norm_recv, {"head": 1 - head_here},
        )

    barrier = pltpu.get_barrier_semaphore()

    @pl.when(seq_here < seq_count - 1)
    def _():
        pl.semaphore_signal(barrier, inc=1, device_id={"seq": seq_here + 1}, device_id_type=MESH)

    for other in others:
        pl.semaphore_signal(barrier, inc=1, device_id={"head": other}, device_id_type=MESH)
    if shared:
        pl.semaphore_signal(barrier, inc=1, device_id={"parts": 1 - parts_here}, device_id_type=MESH)
    pl.semaphore_signal(barrier, inc=1, device_id={"rep": 1 - rep_here}, device_id_type=MESH)

    def load(s, kind):
        span = pl.ds(pl.multiple_of(s * wide, wide), wide)
        src, dst = [
            (k_hbm.at[:, :, span], k_ref), (v_hbm.at[:, :, span], v_ref), (q_hbm.at[:, span], q_ref)
        ][kind]
        return pltpu.make_async_copy(src, dst.at[s], in_sem.at[s, kind])

    load_beta = pltpu.make_async_copy(beta_hbm, beta_ref, weight_sem.at[1])
    load_gate = pltpu.make_async_copy(gate_hbm, gate_ref, weight_sem.at[2])
    load_weight = pltpu.make_async_copy(weight_hbm, weight_ref, weight_sem.at[0])
    load_len = pltpu.make_async_copy(len_hbm, len_ref, weight_sem.at[3])
    load_gain = pltpu.make_async_copy(gain_hbm, gain_ref, weight_sem.at[4])
    load_len.start()
    load_gate.start()
    load_beta.start()
    for s in range(steps):
        load(s, 0).start()
        load(s, 1).start()
    for s in range(steps):
        load(s, 2).start()
    load_gain.start()
    load_weight.start()
    pl.semaphore_wait(barrier, jnp.where(first, 0, 1) + head_count + (1 if shared else 0))
    if shared:
        for j in range(direct_slots):
            from_head(j).start()

    @pl.when(seq_here > 0)
    def _():
        pl.semaphore_signal(ready_sem, inc=1, device_id={"seq": seq_here - 1}, device_id_type=MESH)

    load_len.wait()

    offset = seq_here * tokens
    ends = []
    running = 0
    for d in range(len_ref.shape[1]):
        running = running + len_ref[0, d]
        ends.append(running)

    def segment(pos):
        total = jnp.zeros(pos.shape, jnp.int32)
        for end in ends:
            total += jnp.where(pos >= end, 1, 0)
        return total

    row_i = lax.broadcasted_iota(jnp.int32, (sub, sub), 0)
    col_i = lax.broadcasted_iota(jnp.int32, (sub, sub), 1)
    eye = row_i == col_i
    eye_f = jnp.where(eye, 1.0, 0.0).astype(f32)
    tok_i = lax.broadcasted_iota(jnp.int32, (BLOCK, sub), 0)
    tok_j = lax.broadcasted_iota(jnp.int32, (BLOCK, sub), 1)
    pick_tok = tok_j == tok_i * refl + refl - 1
    levels = []
    size = refl
    while size < sub:
        big = min(4 * size, sub)
        levels.append((row_i // big == col_i // big) & (row_i // size > col_i // size))
        size = big

    load_gate.wait()
    load_beta.wait()
    table = sub_rows(gate_ref[...], jnp.where(tok_i <= tok_j // refl, 1.0, 0.0).astype(bf16), blocks)
    total = 0.0
    for j in range(refl):
        pick = jnp.where(tok_i * refl + j == tok_j, 1.0, 0.0).astype(bf16)
        total += sub_rows(beta_ref[j], pick, blocks)
    for b in range(blocks):
        rows_ref[b, 0] = table[:, b * sub : (b + 1) * sub] * math.log2(math.e)
        rows_ref[b, 1] = total[:, b * sub : (b + 1) * sub]
        rows_ref[b, 2] = rows_ref[b, 0] + jnp.log2(rows_ref[b, 1])

    def geometry(b):
        start = offset + b * BLOCK
        seg_row = segment(start + lax.broadcasted_iota(jnp.int32, (1, sub), 1) // refl)
        before = jnp.where(start == 0, -1, 0)
        last_seg = 0
        for end in ends:
            before += jnp.where(start - 1 >= end, 1, 0)
            last_seg += jnp.where(start + BLOCK - 1 >= end, 1, 0)
        return start, seg_row, before, last_seg

    pairs = [(h, b) for h in range(HEADS_STEP) for b in range(blocks)]

    def over(stage, *lists):
        return [stage(h, b, *args) for (h, b), *args in zip(pairs, *lists)]

    def cols(h):
        return slice(h * width, (h + 1) * width)

    def toks(b):
        return slice(b * BLOCK, (b + 1) * BLOCK)

    def column(values):
        return jnp.sum(jnp.where(eye, values, 0.0), axis=1, keepdims=True)

    reach = (seq_count * tokens // 2 - 2) // tokens
    direct = reach <= 1
    inner = (seq_here > 0) & (seq_here < seq_count - 1)
    following = {"seq": lax.rem(seq_here + 1, seq_count)}
    back = seq_here >= (seq_count - 2 if direct and seq_count > 2 else seq_count - 1)
    beside = {"seq": jnp.where(back, seq_here, seq_here + 1), "rep": jnp.where(back, 1 - rep_here, rep_here)}
    spare = jnp.where(back, heads, 0)

    def send_own(h):
        arrival = own_recv.at[jnp.where(back, heads, h)]
        return remote(own_out.at[h], own_in.at[h + spare], own_send, arrival, beside)

    def take_own(h):
        return remote(own_out.at[h], own_in.at[h], own_send, own_recv.at[h], following)

    def send_full(h):
        return remote(full_out.at[h], full_in.at[h], full_send, full_recv.at[h], following)

    def pass_on(h, state):
        both = jnp.concatenate(split(map_ref[h]), axis=1)
        grown = add_ref[h] + mm(both, jnp.concatenate([state, state], axis=0))
        full_out[h] = grown.astype(bf16)
        send_full(h).start()

    def forward(h):
        if direct:
            take_own(h).wait_recv()
            pass_on(h, own_in[h])
        else:
            @pl.when(seq_here == 1)
            def _():
                take_own(h).wait_recv()
                pass_on(h, own_in[h])

            @pl.when(seq_here > 1)
            def _():
                send_full(h).wait_recv()
                pass_on(h, full_in[h])

    def near(s, b):
        def keys(h):
            return kflat_ref[s, b * sub : (b + 1) * sub, cols(h)]

        def row(kind, h):
            return rows_ref[b, kind, pl.ds(s * HEADS_STEP + h, 1), :]

        return keys, row

    def states_step(s, carry):
        load(s, 0).wait()
        load(s, 1).wait()
        keys = lambda h, b: near(s, b)[0](h)
        row = lambda kind, h, b: near(s, b)[1](kind, h)
        geo = []
        for b in range(blocks):
            start, seg_row, before, last_seg = geometry(b)
            seg_col = segment(start + lax.broadcasted_iota(jnp.int32, (sub, 1), 0) // refl)
            incl = (row_i > col_i) & (seg_col == seg_row)
            geo.append((incl, seg_row == before, seg_row == last_seg, last_seg == before))

        for h, b in pairs:
            kflat_ref[s, b * sub : (b + 1) * sub, cols(h)] = k_ref[s, toks(b), :, cols(h)].reshape(sub, width)

        def scales(h, b):
            gram = mm_nt(keys(h, b), keys(h, b))
            square = jnp.sum(jnp.where(eye, gram, 0.0), axis=0, keepdims=True) + epsilon
            n_log, n_row = -0.5 * jnp.log2(square), lax.rsqrt(square)
            scale_ref[b, pl.ds(s * HEADS_STEP + h, 1), :] = n_row
            factor = jnp.exp2(column(row(2, h, b) + n_log) + (n_log - row(0, h, b)))
            return jnp.where(geo[b][0], factor * gram, 0.0), n_row

        lows, n_rows = zip(*over(scales))
        invs = [eye_f - jnp.where(row_i // refl == col_i // refl, low, 0.0) for low in lows]
        for mask in levels:
            heads_b = [inv.astype(bf16) for inv in invs]
            nils = [
                mm(inv, jnp.where(mask, low, 0.0).astype(bf16)).astype(bf16)
                for inv, low in zip(heads_b, lows)
            ]
            both = [mm(nil, jnp.concatenate([nil, inv], axis=1)) for nil, inv in zip(nils, heads_b)]
            halves = [inv - pair[:, sub:] for inv, pair in zip(invs, both)]
            invs = [
                half + mm(pair[:, :sub].astype(bf16), half.astype(bf16))
                for half, pair in zip(halves, both)
            ]

        if shared:
            @pl.when(s > 0)
            def _():
                for j in range(RELAYS[0], RELAYS[1]):
                    relay(j)

        @pl.when((s == 0) & (seq_here < seq_count - 1))
        def _():
            pl.semaphore_wait(ready_sem, 1)

        @pl.when((s > 0) & inner & (direct | (seq_here == 1)))
        def _():
            for h in range(HEADS_STEP):
                forward((s - 1) * HEADS_STEP + h)

        def residual(h, b, inv, low):
            inv_b = inv.astype(bf16)
            low_2 = jnp.concatenate(split(low), axis=1)
            return eye_f - inv_b.astype(f32) - mm(low_2, jnp.concatenate([inv_b, inv_b], axis=0))

        def refine(h, b, inv, resid):
            inv_b = inv.astype(bf16)
            return inv_b.astype(f32) + mm(inv_b, resid.astype(bf16))

        def write(h, b, inv, n_row):
            carry_row = jnp.where(geo[b][1], jnp.exp2(row(0, h, b)), 0.0)
            by_beta = inv * row(1, h, b)
            tv = jnp.concatenate(split(by_beta), axis=1)
            tk = jnp.concatenate(split(by_beta * (carry_row * n_row)), axis=1)
            vb, kb = v_ref[s, toks(b), :, cols(h)].reshape(sub, width), keys(h, b)
            return jnp.concatenate(
                [mm(tv, jnp.concatenate([vb, vb], axis=0)), mm(tk, jnp.concatenate([kb, kb], axis=0))],
                axis=1,
            )

        def block_step(h, b, wrote, n_row):
            wrote_ref[s * HEADS_STEP + h, b] = wrote.astype(bf16)
            c_row = row(0, h, b)
            c_end = c_row[:, sub - 1 : sub]
            e_row = jnp.where(geo[b][2], jnp.exp2(jnp.minimum(c_end - c_row, 0.0)), 0.0) * n_row
            kb = keys(h, b)
            moved = mm_tn(
                jnp.concatenate([kb, kb], axis=0), jnp.concatenate(split(wrote * column(e_row)), axis=0)
            )
            carry_end = jnp.where(geo[b][3], jnp.exp2(c_end), 0.0)
            return moved[:, :width], carry_end * eye_f - moved[:, width:]

        made, states = {}, {}

        def some(heads_now, stage, *lists):
            return {(h, b): stage(h, b, *[l[h, b] for l in lists]) for h in heads_now for b in range(blocks)}

        def scan(heads_now, b):
            for h in heads_now:
                if b == 0:
                    states[h] = jnp.concatenate(made[h, 0], axis=1)
                    continue
                block_add, block_map = made[h, b]
                s_hi = states[h].astype(bf16)
                prefix_ref[s * HEADS_STEP + h, b - 1] = s_hi
                grown = mm(
                    jnp.concatenate(split(block_map), axis=1), jnp.concatenate([s_hi, s_hi], axis=0)
                )
                states[h] = jnp.concatenate([grown[:, :width] + block_add, grown[:, width:]], axis=1)

        def finish(heads_now):
            for h in heads_now:
                at = s * HEADS_STEP + h
                own_out[at] = states[h][:, :width].astype(bf16)
                send_own(at).start()
                add_ref[at] = states[h][:, :width]
                map_ref[at] = states[h][:, width:]

        named = lambda values: dict(zip(pairs, values))
        lows, invs, n_rows = map(named, (lows, invs, n_rows))
        teams = [list(range(h, min(h + TEAM, HEADS_STEP))) for h in range(0, HEADS_STEP, TEAM)]
        pending = []

        def catch_up(count):
            for _ in range(count):
                if pending:
                    pending.pop(0)()

        for team in teams:
            resids = some(team, residual, invs, lows)
            catch_up(2)
            better = some(team, refine, invs, resids)
            catch_up(1)
            writes = some(team, write, better, n_rows)
            catch_up(1)
            made.update(some(team, block_step, writes, n_rows))
            catch_up(len(pending))
            pending = [functools.partial(scan, team, b) for b in range(blocks)]
            pending.append(functools.partial(finish, team))
        catch_up(len(pending))

        if shared:
            @pl.when(s == 0)
            def _():
                for j in range(RELAYS[0]):
                    relay(j)

        return carry

    lax.fori_loop(0, steps, states_step, 0)
    relayed = RELAYS[1] if steps > 1 else RELAYS[0]
    if shared:
        while relayed < RELAYS[2]:
            relay(relayed)
            relayed += 1

    @pl.when(first)
    def _():
        state_in[...] = jnp.zeros_like(state_in)

    done = (steps - 1) * HEADS_STEP
    if done and not direct:
        @pl.when(inner & (seq_here > 1))
        def _():
            for h in range(done):
                forward(h)

    def reads_step(s, carry):
        load(s, 2).wait()
        geo = []
        for b in range(blocks):
            start, seg_row, before, _ = geometry(b)
            seg_tok = segment(start + lax.broadcasted_iota(jnp.int32, (BLOCK, 1), 0))
            geo.append(((tok_j // refl <= tok_i) & (seg_tok == seg_row), seg_tok == before))

        def read_weights(h, b):
            keys, row = near(s, b)
            qb, c_row = q_ref[s, toks(b), cols(h)], row(0, h)
            n_row = scale_ref[b, pl.ds(s * HEADS_STEP + h, 1), :]
            qf = qb.astype(f32)
            nq = lax.rsqrt(jnp.sum(qf * qf, axis=1, keepdims=True) + epsilon) * width ** (-0.5)
            ct = jnp.sum(jnp.where(pick_tok, c_row, 0.0), axis=1, keepdims=True)
            ratio = jnp.where(geo[b][0], jnp.exp2(jnp.minimum(ct - c_row, 0.0)), 0.0)
            carried = (jnp.where(geo[b][1], jnp.exp2(ct), 0.0) * nq) * qf
            return (ratio * mm_nt(qb, keys(h)) * nq * n_row).astype(bf16), carried

        weights = over(read_weights)

        def read(h, b, weight):
            got = mm(weight[0], wrote_ref[s * HEADS_STEP + h, b])
            return got[:, :width], (weight[1] - got[:, width:]).astype(bf16)

        for (h, b), (own, back) in zip(pairs, over(read, weights)):
            if b:
                moved = mm(back, prefix_ref[s * HEADS_STEP + h, b - 1])
                own, back = own + moved[:, :width], moved[:, width:].astype(bf16)
            oloc_ref[s * HEADS_STEP + h, toks(b), :] = own
            read_ref[s * HEADS_STEP + h, toks(b), :] = back
        return carry

    def relay_until(count):
        nonlocal relayed
        if shared:
            while relayed < count:
                relay(relayed)
                relayed += 1

    def finish_heads(start, stop):
        for g in range(start, stop, FINISH_GROUP):
            finish_group(g, stop)

    def finish_group(g, stop):
        group = range(g, min(g + FINISH_GROUP, stop))

        for h in group:
            @pl.when(last & (seq_here == 1))
            def _():
                take_own(h).wait_recv()

            @pl.when((seq_here > 1) & (direct | last))
            def _():
                send_full(h).wait_recv()

            @pl.when(seq_here == 1)
            def _():
                state_in[h] = own_in[h]

            @pl.when(seq_here > 1)
            def _():
                state_in[h] = full_in[h]

        for h in group:
            out = oloc_ref[h] + mm(read_ref[h], state_in[h])
            scale = lax.rsqrt(jnp.mean(out * out, axis=-1, keepdims=True) + epsilon)
            normed_ref[:, cols(h)] = (out * scale * gain_ref[...]).astype(bf16)

        if shared:
            for h in group:
                send_normed(h).start()

    load_gain.wait()
    for s in range(steps - 1):
        reads_step(s, 0)
        finish_heads(s * HEADS_STEP, (s + 1) * HEADS_STEP)
    relay_until(RELAYS[3])

    @pl.when(inner)
    def _():
        for h in range(done, heads):
            forward(h)

    relay_until(RELAYS[4])
    reads_step(steps - 1, 0)
    relay_until(SHARE_PARTS)
    finish_heads(done, heads)
    load_weight.wait()
    piece, pieces = PIECE, (weight_ref.shape[1] - shared) // PIECE
    copies = []
    for slot, other in enumerate(others):
        rows = normed_ref[pl.ds(pl.multiple_of(other * chunk, chunk), chunk), :]
        for p in range(pieces):
            part = pl.ds(p * piece, piece)
            part_out[slot, :, part] = mm(rows, weight_ref[:, pl.ds(shared + p * piece, piece)]).astype(bf16)
            copies.append(
                pltpu.make_async_remote_copy(
                    src_ref=part_out.at[slot, :, part],
                    dst_ref=part_in.at[slot, :, part],
                    send_sem=part_send.at[slot],
                    recv_sem=part_recv.at[slot, p],
                    device_id={"head": other},
                    device_id_type=MESH,
                )
            )
            copies[-1].start()
    rows = normed_ref[pl.ds(pl.multiple_of(head_here * chunk, chunk), chunk), :]
    if shared:
        for j in range(SHARE_PARTS):
            over_parts(j, 1 - parts_here).wait_recv()
            over_cores(SHARE_PARTS + j, rep_here).start()
    for p in range(pieces):
        part = pl.ds(shared + p * piece, piece)
        own_ref[:, part] = mm(rows, weight_ref[:, part])
    if shared:
        for p in range(shared // piece):
            part = pl.ds(p * piece, piece)
            own_ref[:, part] = mm(rows, weight_ref[:, part])
        all_cores(1 - rep_here).wait_recv()
        all_normed().wait_recv()
        for p in range(shared // piece):
            part = pl.ds(p * piece, piece)
            peer = mm(rows_in[...], peer_ref[:, part])
            total = own_ref[:, part].astype(bf16).astype(f32) + peer.astype(bf16).astype(f32)
            out_ref[:, part] = total.astype(bf16)
    for p in range(pieces):
        part = pl.ds(p * piece, piece)
        spot = pl.ds(shared + p * piece, piece)
        total = own_ref[:, spot].astype(bf16).astype(f32)
        for slot in range(len(others)):
            copies[slot * pieces + p].wait_recv()
            total += part_in[slot, :, part].astype(f32)
        out_ref[:, spot] = total.astype(bf16)
    for slot, other in enumerate(others):
        remote(
            part_out.at[slot], part_in.at[slot], part_send.at[slot], part_recv.at[slot, 0], {"head": other}
        ).wait_send()
    if shared:
        all_x().wait_send()
        all_y().wait_send()
        if SWAP:
            all_z().wait_send()
        all_cores(rep_here).wait_send()
        all_normed().wait_send()

    if not direct:
        @pl.when(seq_here > 1)
        def _():
            for h in range(heads):
                take_own(h).wait_recv()

    @pl.when(back)
    def _():
        remote(own_out, own_in.at[pl.ds(heads, heads)], own_send, own_recv.at[heads], following).wait_recv()

    remote(own_out, own_in.at[pl.ds(0, heads)], own_send, own_recv.at[0], following).wait_send()

    @pl.when(inner)
    def _():
        remote(full_out, full_in, full_send, full_recv.at[0], following).wait_send()


def body(queries, reflect_keys, reflect_values, reflect_beta, log_decay, prompt_lengths, norm_gain, out_weight):
    tokens, refl, wide = reflect_keys.shape[1:]
    heads = log_decay.shape[2]
    width = wide // heads
    blocks = tokens // BLOCK
    sub = refl * BLOCK
    head_count = lax.axis_size("head")
    chunk, model = tokens // head_count, out_weight.shape[1]
    steps, slots = heads // HEADS_STEP, max(head_count - 1, 1)
    wide_step = HEADS_STEP * width
    shared = model * SHARE // PIECE // 100 * PIECE if sharing() else 0
    peer_shape = (out_weight.shape[0], shared) if shared else (32, 128)
    rest = model - shared
    pieces = rest // PIECE
    beta, gate = reflect_beta[0].transpose(1, 2, 0), log_decay[0].T
    dma = pltpu.SemaphoreType.DMA
    anywhere, vmem = pl.BlockSpec(memory_space=pl.ANY), pl.BlockSpec(memory_space=pltpu.VMEM)
    out = pl.pallas_call(
        functools.partial(mixer_kernel, refl, blocks),
        in_specs=[anywhere] * 8,
        out_specs=vmem,
        out_shape=pltpu.VMEM((chunk, model), bf16),
        scratch_shapes=[
            pltpu.SMEM(prompt_lengths.shape, jnp.int32),
            pltpu.VMEM((steps, tokens, wide_step), bf16),
            pltpu.VMEM((steps, tokens, refl, wide_step), bf16),
            pltpu.VMEM((steps, tokens, refl, wide_step), bf16),
            pltpu.VMEM(beta.shape, f32),
            pltpu.VMEM(gate.shape, f32),
            pltpu.VMEM((1, width), f32),
            dma((steps, 3)),
            pltpu.SemaphoreType.REGULAR,
            pltpu.VMEM((blocks, 3, heads, sub), f32),
            pltpu.VMEM((blocks, heads, sub), f32),
            pltpu.VMEM((steps, tokens * refl, wide_step), bf16),
            pltpu.VMEM((heads, blocks, sub, 2 * width), bf16),
            pltpu.VMEM((heads, max(blocks - 1, 1), width, 2 * width), bf16),
            pltpu.VMEM((heads, tokens, width), f32),
            pltpu.VMEM((heads, tokens, width), bf16),
            pltpu.VMEM((heads, width, width), f32),
            pltpu.VMEM((heads, width, width), f32),
            pltpu.VMEM(out_weight.shape, bf16),
            dma((5,)),
            *[pltpu.VMEM((heads, width, width), bf16)] * 3,
            pltpu.VMEM((2 * heads, width, width), bf16),
            pltpu.VMEM((heads, width, width), bf16),
            pltpu.VMEM((tokens, wide), bf16),
            pltpu.VMEM((chunk, model), f32),
            pltpu.VMEM((slots, chunk, rest), bf16),
            pltpu.VMEM((slots, chunk, rest), bf16),
            dma, dma((heads + 1,)), dma, dma((heads,)), dma((slots,)), dma((slots, pieces)),
            pltpu.VMEM(peer_shape, bf16),
            pltpu.VMEM((chunk, wide), bf16),
            dma, dma((SHARE_PARTS - SWAP,)), dma, dma((SHARE_PARTS,)), dma, dma((max(SWAP, 1),)), dma, dma, dma, dma,
        ],
        compiler_params=pltpu.CompilerParams(
            collective_id=0, has_side_effects=True, vmem_limit_bytes=56 * 2**20
        ),
    )(
        prompt_lengths,
        queries[0],
        reflect_keys[0],
        reflect_values[0],
        beta,
        gate,
        norm_gain[None],
        out_weight,
    )
    return out[None]


def solution(mesh):
    in_specs = (
        P(("parts", "rep"), "seq", "head"),
        P(("parts", "rep"), "seq", None, "head"),
        P(("parts", "rep"), "seq", None, "head"),
        P(("parts", "rep"), "seq", None, "head"),
        P(("parts", "rep"), "seq", "head"),
        P(("parts", "rep"), None),
        P(),
        P("head", None),
    )
    out_specs = P(("parts", "rep"), ("seq", "head"), None)
    return jax.shard_map(body, mesh=mesh, in_specs=in_specs, out_specs=out_specs, check_vma=False)
```
